1024 devices in a mesh: gx: 4 (over y), gy: 8 (over x, core), gz: 32 (over z).
Axes of the slice: x: 4, y: 4, z: 32, core: 2. Of those that a mesh axis runs over, the one named last changes fastest.
Arguments:
- loads: float32 [16, 8, 32, 8192], P(None, 'gx', 'gy', 'gz'), may hold values from -60 to 60
- moduli: float32 [8], replicated, may hold values from 0.5 to 4
- material: int32 [8, 32, 8192], P('gx', 'gy', 'gz'), may hold values from 0 to 7
Outputs:
- solution: float32 [16, 8, 32, 8192], P(None, 'gx', 'gy', 'gz')
- residual: float32 [16, 8, 32, 8192], P(None, 'gx', 'gy', 'gz')
The draws below stay inside these ranges and needn't reach their ends.
All inputs are finite; a program needn't handle non-finite values.
Results may differ from the reference program's by a relative error of at most 0.005.
The reference program's roundings to bfloat16 on the way (of `kernel`) count: a program that leaves them out, or rounds other values in their place, can miss the bound.
Values may be sent and summed in bfloat16 or wider, within the bound.
No kernel may reach another device: no remote copies, remote signals or barrier semaphores. Data moves between devices by JAX's collectives and lax.ppermute only.
A program may use at most 32 MiB of HBM per device.

```python
import math
import jax
import jax.numpy as jnp
import numpy as np
from jax import lax

COLS = 16
MATS = 8
ITERS = 2
NX = 8
NY = 32
NZ = 8192


def draw_loads(key, part):
    key_base = jax.random.fold_in(jax.random.fold_in(key, 11), 0)
    key_scale = jax.random.fold_in(jax.random.fold_in(key, 11), 1)
    key_modes = jax.random.fold_in(jax.random.fold_in(key, 11), 3)
    shape = (COLS, NX, NY, NZ)
    pos_x = jnp.arange(NX, dtype=jnp.float32).reshape(1, NX, 1, 1)
    pos_y = jnp.arange(NY, dtype=jnp.float32).reshape(1, 1, NY, 1)
    pos_z = jnp.arange(NZ, dtype=jnp.float32).reshape(1, 1, 1, NZ)
    depth = pos_z / max(NZ - 1, 1)
    across = pos_x / max(NX - 1, 1)
    upper = (pos_y >= NY // 2).astype(jnp.float32)
    ramp = (1.0 + 2.0 * depth) * 0.5
    roughness = jnp.exp(-math.log(10.0) * (1.2 * upper + 0.4 * across + 0.6 * depth))
    scales = jnp.exp(jax.random.uniform(key_scale, (COLS, 1, 1, 1), jnp.float32, 0.0, math.log(10.0))) / 3.0
    key_my, key_mz, key_coef = jax.random.split(key_modes, 3)
    wave_y = jax.random.randint(key_my, (COLS, 3), 1, 3).astype(jnp.float32)
    wave_z = jax.random.randint(key_mz, (COLS, 3), 1, 5).astype(jnp.float32)
    coefs = jax.random.normal(key_coef, (COLS, 3), jnp.float32)
    shape_x = jnp.sin(math.pi * (pos_x + 1.0) / (NX + 1.0))
    smooth = jnp.zeros(shape, jnp.float32)
    for mode in range(3):
        my = wave_y[:, mode].reshape(COLS, 1, 1, 1)
        mz = wave_z[:, mode].reshape(COLS, 1, 1, 1)
        amp = coefs[:, mode].reshape(COLS, 1, 1, 1)
        term = shape_x * jnp.sin(math.pi * my * (pos_y + 1.0) / (NY + 1.0)) * jnp.sin(math.pi * mz * (pos_z + 1.0) / (NZ + 1.0))
        smooth = smooth + amp * term
    smooth = smooth * math.sqrt(8.0 / 3.0)
    rough = jax.random.normal(key_base, shape, jnp.float32)
    field = roughness * rough + 0.7 * smooth
    return jnp.clip(field * scales * ramp, -60.0, 60.0)


def touch_ends(result, stream_key, least, top_value):
    spot = [jax.random.randint(jax.random.fold_in(stream_key, axis), (), 0, length) for axis, length in enumerate(result.shape)]
    widest = result.shape.index(max(result.shape))
    beside = spot[:widest] + [(spot[widest] + 1) % result.shape[widest]] + spot[widest + 1:]
    return result.at[tuple(spot)].set(least).at[tuple(beside)].set(top_value)


def setup_inputs(seed: int = 0) -> dict:
    arg_keys = jax.random.split(jax.random.key(seed), 4)
    loads = draw_loads(jax.random.fold_in(arg_keys[3], 71), 0)
    moduli = jnp.clip(jnp.exp(jax.random.uniform(arg_keys[1], (MATS,), jnp.float32, math.log(0.5), math.log(4.0))), 0.5, 4.0)
    material = touch_ends(jax.random.randint(arg_keys[2], (NX, NY, NZ), 0, MATS), jax.random.fold_in(arg_keys[2], 1), 0, MATS - 1).astype(jnp.int32)
    return dict(loads=loads, moduli=moduli, material=material)


SIGMA = 0.25

def stiffness_table():
    line_mass = np.array([[1.0 / 3.0, 1.0 / 6.0], [1.0 / 6.0, 1.0 / 3.0]])
    line_stiff = np.array([[1.0, -1.0], [-1.0, 1.0]])
    table = np.zeros((8, 8))
    for target in range(8):
        for source in range(8):
            target_bits = [target >> 2 & 1, target >> 1 & 1, target & 1]
            source_bits = [source >> 2 & 1, source >> 1 & 1, source & 1]
            total = 0.0
            for stiff_dim in range(3):
                factor = 1.0
                for other in range(3):
                    if other == stiff_dim:
                        factor = factor * line_stiff[target_bits[other], source_bits[other]]
                    else:
                        factor = factor * line_mass[target_bits[other], source_bits[other]]
                total = total + factor
            table[target, source] = total
    return table

def corner_bits(corner):
    return (corner >> 2 & 1, corner >> 1 & 1, corner & 1)

def apply_column(column, weights, kernel):
    size_x, size_y, size_z = column.shape
    padded = jnp.pad(column.astype(jnp.bfloat16), 1)
    pieces = []
    for corner in range(8):
        bit_x, bit_y, bit_z = corner_bits(corner)
        pieces.append(padded[bit_x:bit_x + size_x + 1, bit_y:bit_y + size_y + 1, bit_z:bit_z + size_z + 1])
    stacked = jnp.stack(pieces).astype(jnp.float32)
    total = SIGMA * column
    for corner in range(8):
        bit_x, bit_y, bit_z = corner_bits(corner)
        part = jnp.einsum('b,bxyz->xyz', kernel[corner], stacked, precision=lax.Precision.HIGHEST) * weights
        total = total + part[1 - bit_x:1 - bit_x + size_x, 1 - bit_y:1 - bit_y + size_y, 1 - bit_z:1 - bit_z + size_z]
    return total

def gram(left, right):
    return jnp.einsum('cxyz,dxyz->cd', left, right, precision=lax.Precision.HIGHEST)

def combine(block, coeffs):
    return jnp.einsum('cxyz,cd->dxyz', block, coeffs, precision=lax.Precision.HIGHEST)

def solve_small(matrix, rhs_small):
    factor = jnp.linalg.cholesky(matrix)
    return jax.scipy.linalg.cho_solve((factor, True), rhs_small)

def reference(loads, moduli, material):
    kernel = jnp.asarray(stiffness_table(), jnp.float32).astype(jnp.bfloat16).astype(jnp.float32)
    node_modulus = jnp.take(moduli, material, axis=0)
    padded_mod = jnp.pad(node_modulus, 1)
    size_x, size_y, size_z = material.shape
    weights = jnp.zeros((size_x + 1, size_y + 1, size_z + 1), jnp.float32)
    for corner in range(8):
        bit_x, bit_y, bit_z = corner_bits(corner)
        weights = weights + padded_mod[bit_x:bit_x + size_x + 1, bit_y:bit_y + size_y + 1, bit_z:bit_z + size_z + 1]
    weights = weights * 0.125

    def operator(block):
        return lax.map(lambda column: apply_column(column, weights, kernel), block)
    solution = jnp.zeros_like(loads)
    residual = loads
    direction = loads
    current = gram(residual, residual)
    for iteration in range(ITERS):
        image = operator(direction)
        alpha = solve_small(gram(direction, image), current)
        solution = solution + combine(direction, alpha)
        residual = residual - combine(image, alpha)
        if iteration + 1 < ITERS:
            updated = gram(residual, residual)
            beta = solve_small(current, updated)
            direction = residual + combine(direction, beta)
            current = updated
    return (solution, residual)
```

```python
import functools

import jax
import jax.numpy as jnp
import numpy as np
from jax import lax
from jax.experimental import pallas as pl
from jax.experimental.pallas import tpu as pltpu
from jax.sharding import Mesh
from jax.sharding import PartitionSpec as P

PLANE = ("gx", "gy_0", "gy_1")
GY = ("gy_0", "gy_1")
SIGMA = 0.25
COLS = 16
LANES = 128
HIGH = lax.Precision.HIGHEST


def stiffness_table():
    line_mass = np.array([[1.0 / 3.0, 1.0 / 6.0], [1.0 / 6.0, 1.0 / 3.0]])
    line_stiff = np.array([[1.0, -1.0], [-1.0, 1.0]])
    table = np.zeros((8, 8))
    for target in range(8):
        for source in range(8):
            target_bits = [target >> 2 & 1, target >> 1 & 1, target & 1]
            source_bits = [source >> 2 & 1, source >> 1 & 1, source & 1]
            total = 0.0
            for stiff_dim in range(3):
                factor = 1.0
                for other in range(3):
                    if other == stiff_dim:
                        factor = factor * line_stiff[target_bits[other], source_bits[other]]
                    else:
                        factor = factor * line_mass[target_bits[other], source_bits[other]]
                total = total + factor
            table[target, source] = total
    return table


def kernel_scale():
    table = np.asarray(jnp.asarray(stiffness_table(), jnp.bfloat16).astype(jnp.float32))
    unit = -float(table[0, 7])
    for target in range(8):
        for source in range(8):
            bits = bin(target ^ source).count("1")
            want = (4.0, 0.0, -1.0, -1.0)[bits] * unit
            assert abs(float(table[target, source]) - want) < 1e-12
    return unit


UNIT = kernel_scale()


def lowered(value):
    return value.astype(jnp.bfloat16).astype(jnp.float32)


def shifted(tiles, step):
    lane = lax.broadcasted_iota(jnp.int32, tiles[0].shape, 1)
    turned = [pltpu.roll(t, (-step) % LANES, 1) for t in tiles]
    count = len(tiles)
    edge = lane < LANES - 1 if step == 1 else lane > 0
    return [jnp.where(edge, turned[i], turned[(i + step) % count]) for i in range(count)]


def operator(field, low, above, below, both, x, y, wx, wy):
    plane, up, down = [], [], []
    for tile in range(3):
        around = {
            (i, j): low(x + i, y + j, tile) for i in (-1, 0, 1) for j in (-1, 0, 1)
        }
        centre = 4.0 * around[0, 0]
        in_plane, from_above, from_below = None, None, None
        for i in (-1, 1):
            for j in (-1, 1):
                ex, ey = wx + (i - 1) // 2, wy + (j - 1) // 2
                others = around[i, 0] + around[0, j] + around[i, j]
                terms = (
                    both(ex, ey, tile) * (centre - around[i, j]),
                    below(ex, ey, tile) * others,
                    above(ex, ey, tile) * others,
                )
                if in_plane is None:
                    in_plane, from_above, from_below = terms
                else:
                    in_plane = in_plane + terms[0]
                    from_above = from_above + terms[1]
                    from_below = from_below + terms[2]
        plane.append(in_plane)
        up.append(from_above)
        down.append(from_below)
    up, down = shifted(up, 1), shifted(down, -1)
    return [SIGMA * field(t) + (plane[t] - up[t] - down[t]) for t in range(3)]


def tile_of(tile):
    return slice(tile * LANES, (tile + 1) * LANES)


def moments_kernel(v_ref, e_ref, q_ref, above_ref, below_ref, both_ref, g_ref, low_ref, qlow_ref, w_ref):
    ext_x, ext_y = v_ref.shape[0], v_ref.shape[1]
    for ex in range(ext_x - 1):
        for tile in range(3):
            pass
        flat = []
        for tile in range(3):
            ours = e_ref[ex * ext_y : ex * ext_y + ext_y, tile_of(tile)]
            next_x = e_ref[(ex + 1) * ext_y : (ex + 1) * ext_y + ext_y, tile_of(tile)]
            both_x = ours + next_x
            flat.append(both_x + pltpu.roll(both_x, ext_y - 1, 0))
        ahead = shifted(flat, 1)
        weights = [(0.125 * UNIT) * (flat[t] + ahead[t]) for t in range(3)]
        behind = shifted(weights, -1)
        for t in range(3):
            above_ref[ex, :, tile_of(t)] = weights[t]
            below_ref[ex, :, tile_of(t)] = behind[t]
            both_ref[ex, :, tile_of(t)] = weights[t] + behind[t]
    for x in range(ext_x):
        for y in range(ext_y):
            low_ref[x, y] = lowered(v_ref[x, y])

    def weight(ref):
        return lambda ex, ey, t: ref[ex, ey : ey + 1, tile_of(t)]

    sides = (weight(above_ref), weight(below_ref), weight(both_ref))
    for x in range(1, ext_x - 1):
        for y in range(1, ext_y - 1):
            image = operator(
                lambda t: v_ref[x, y, :, tile_of(t)],
                lambda i, j, t: low_ref[i, j, :, tile_of(t)],
                *sides,
                x,
                y,
                x,
                y,
            )
            for t in range(3):
                inside = e_ref[x * ext_y + y : x * ext_y + y + 1, tile_of(t)] > 0.0
                value = jnp.where(inside, image[t], 0.0)
                q_ref[x - 1, y - 1, :, tile_of(t)] = value
                qlow_ref[x - 1, y - 1, :, tile_of(t)] = lowered(value)
    total = jnp.zeros((2 * COLS, LANES), jnp.float32)
    pad = jnp.zeros((LANES - 3 * COLS, 2 * LANES), jnp.float32)
    for x in range(2, ext_x - 2):
        for y in range(2, ext_y - 2):
            image = operator(
                lambda t: q_ref[x - 1, y - 1, :, tile_of(t)],
                lambda i, j, t: qlow_ref[i, j, :, tile_of(t)],
                *sides,
                x - 1,
                y - 1,
                x,
                y,
            )
            b = v_ref[x, y, :, : 2 * LANES]
            q = q_ref[x - 1, y - 1, :, : 2 * LANES]
            w = jnp.concatenate(image[:2], axis=1)
            left = jnp.concatenate([b, q], axis=0)
            right = jnp.concatenate([b, q, w, pad], axis=0)
            total = total + lax.dot_general(
                left, right, (((1,), (1,)), ((), ())), precision=HIGH, preferred_element_type=jnp.float32
            )
    lane = lax.broadcasted_iota(jnp.int32, (8, LANES), 1)
    first, second = total[:COLS], total[COLS:]
    crossed = 0.5 * (first + pltpu.roll(second, COLS, 1))
    lane16 = lax.broadcasted_iota(jnp.int32, (COLS, LANES), 1)
    low_pair = jnp.where(lane16 < COLS, first, crossed)
    high_pair = pltpu.roll(second, LANES - COLS, 1)
    quarters = (low_pair[:8], low_pair[8:], high_pair[:8], high_pair[8:])
    packed = jnp.where(lane < 2 * COLS, quarters[0], 0.0)
    for n in range(1, 4):
        moved = pltpu.roll(quarters[n], 2 * COLS * n, 1)
        packed = jnp.where((lane >= 2 * COLS * n) & (lane < 2 * COLS * (n + 1)), moved, packed)
    g_ref[...] = packed


def dot(left, right, dims=((1,), (0,))):
    return lax.dot_general(left, right, (dims, ((), ())), precision=HIGH, preferred_element_type=jnp.float32)


def inverse(matrix):
    size = COLS
    sub = lax.broadcasted_iota(jnp.int32, (size, LANES), 0)
    rows = [jnp.broadcast_to(matrix[:, i : i + 1], (size, LANES)) for i in range(size)]
    for k in range(size):
        scale = 1.0 / rows[k][k : k + 1, :]
        pivot_row = rows[k] * scale
        for i in range(size):
            if i != k:
                factor = rows[i][k : k + 1, :]
                moved = rows[i] - factor * pivot_row
                rows[i] = jnp.where(sub == k, factor * scale, moved)
        rows[k] = jnp.where(sub == k, -scale, pivot_row)
    lane = lax.broadcasted_iota(jnp.int32, (size, LANES), 1)
    out = jnp.zeros((size, LANES), jnp.float32)
    for i in range(size):
        out = jnp.where(lane == i, -rows[i], out)
    return out[:, :size]


def solve(matrix, right):
    inv = inverse(matrix)
    guess = dot(inv, right)
    return guess + dot(inv, right - dot(matrix, guess))


def finish_kernel(g_ref, v_ref, e_ref, q_ref, above_ref, below_ref, both_ref, sol_ref, res_ref, d_ref, dlow_ref):
    ext_x, ext_y = v_ref.shape[0], v_ref.shape[1]
    packed = g_ref[...]
    turned = [packed] + [pltpu.roll(packed, LANES - 2 * COLS * n, 1) for n in range(1, 4)]
    low_pair = jnp.concatenate(turned[:2], axis=0)
    high_pair = jnp.concatenate(turned[2:], axis=0)
    m0 = low_pair[:, :COLS]
    m1 = pltpu.roll(low_pair, LANES - COLS, 1)[:, :COLS]
    m2 = high_pair[:, :COLS]
    m3 = pltpu.roll(high_pair, LANES - COLS, 1)[:, :COLS]
    first = ((0,), (0,))
    alpha = solve(m1, m0)
    m1a, m2a, m3a = dot(m1, alpha), dot(m2, alpha), dot(m3, alpha)
    updated = m0 - m1a - dot(alpha, m1, first) + dot(alpha, m2a, first)
    beta = solve(m0, updated)
    row = lax.broadcasted_iota(jnp.int32, (COLS, COLS), 0)
    col = lax.broadcasted_iota(jnp.int32, (COLS, COLS), 1)
    mix = beta + jnp.where(row == col, 1.0, 0.0)
    curved = dot(mix, dot(m1, mix) - m2a, first) + dot(alpha, m3a - dot(m2, mix), first)
    curved = 0.5 * (curved + curved.T)
    gamma = solve(curved, updated)
    both = jnp.concatenate([mix, -alpha], axis=0)
    for x in range(1, ext_x - 1):
        for y in range(1, ext_y - 1):
            block = jnp.concatenate([v_ref[x, y], q_ref[x - 1, y - 1]], axis=0)
            value = dot(both, block, first)
            inside = e_ref[x * ext_y + y : x * ext_y + y + 1, :] > 0.0
            value = jnp.where(inside, value, 0.0)
            d_ref[x - 1, y - 1] = value
            dlow_ref[x - 1, y - 1] = lowered(value)

    def weight(ref):
        return lambda ex, ey, t: ref[ex, ey : ey + 1, tile_of(t)]

    sides = (weight(above_ref), weight(below_ref), weight(both_ref))
    zero = jnp.zeros((COLS, COLS), jnp.float32)
    to_sol = jnp.concatenate([alpha, gamma, zero], axis=0)
    to_res = jnp.concatenate([-alpha, -gamma], axis=0)
    for x in range(2, ext_x - 2):
        for y in range(2, ext_y - 2):
            image = operator(
                lambda t: d_ref[x - 1, y - 1, :, tile_of(t)],
                lambda i, j, t: dlow_ref[i, j, :, tile_of(t)],
                *sides,
                x - 1,
                y - 1,
                x,
                y,
            )
            b = v_ref[x, y, :, : 2 * LANES]
            q = q_ref[x - 1, y - 1, :, : 2 * LANES]
            d = d_ref[x - 1, y - 1, :, : 2 * LANES]
            i2 = jnp.concatenate(image[:2], axis=1)
            sol_ref[x - 2, y - 2] = dot(to_sol[: 2 * COLS], jnp.concatenate([b, d], axis=0), first)
            res_ref[x - 2, y - 2] = b + dot(to_res, jnp.concatenate([q, i2], axis=0), first)


def ring(axis, step):
    count = lax.axis_size(axis)
    ends = range(count - 1)
    return [(i, i + 1) for i in ends] if step > 0 else [(i + 1, i) for i in ends]


def both_ways(axis, to_next, to_last):
    return lax.ppermute(to_next, axis, ring(axis, 1)), lax.ppermute(to_last, axis, ring(axis, -1))


def spread(value, axes):
    count = lax.axis_size(axes)
    copies = jnp.broadcast_to(value[None], (count, *value.shape))
    return jnp.sum(lax.all_to_all(copies, axes, 0, 0), axis=0)


def on_device(loads, moduli, material):
    levels = jnp.arange(moduli.shape[0], dtype=jnp.int32)
    modulus = jnp.sum(jnp.where(material[..., None] == levels, moduli, 0.0), axis=-1)
    own = jnp.concatenate([loads, modulus[None]], axis=0)
    before, after = both_ways("gz", own[..., LANES:], own[..., :LANES])
    lane = lax.broadcasted_iota(jnp.int32, before.shape, 3)
    own = jnp.concatenate([own, jnp.where(lane < LANES // 2, after, before)], axis=3)
    before, after = both_ways("gx", own, own)
    own = jnp.concatenate([before, own, after], axis=1)
    before, after = both_ways(GY, own[:, :, 2:], own[:, :, :2])
    own = jnp.concatenate([before, own, after], axis=2)
    ext_x, ext_y = own.shape[1], own.shape[2]
    block = jnp.transpose(own[:COLS], (1, 2, 0, 3))
    modulus = own[COLS].reshape(ext_x * ext_y, 3 * LANES)
    f32 = jnp.float32
    wide = 3 * LANES
    weights = jax.ShapeDtypeStruct((ext_x - 1, ext_y, wide), f32)
    image, above, below, both, moments = pl.pallas_call(
        moments_kernel,
        out_shape=(
            jax.ShapeDtypeStruct((ext_x - 2, ext_y - 2, COLS, wide), f32),
            weights,
            weights,
            weights,
            jax.ShapeDtypeStruct((8, LANES), f32),
        ),
        scratch_shapes=[
            pltpu.VMEM((ext_x, ext_y, COLS, wide), f32),
            pltpu.VMEM((ext_x - 2, ext_y - 2, COLS, wide), f32),
            pltpu.VMEM((8, 128), f32),
        ],
        name="moments",
    )(block, modulus)
    moments = spread(spread(moments, PLANE), "gz")
    out = jax.ShapeDtypeStruct((ext_x - 4, ext_y - 4, COLS, 2 * LANES), f32)
    solution, residual = pl.pallas_call(
        finish_kernel,
        out_shape=(out, out),
        scratch_shapes=[pltpu.VMEM((ext_x - 2, ext_y - 2, COLS, wide), f32)] * 2,
        name="finish",
    )(moments, block, modulus, image, above, below, both)
    return jnp.transpose(solution, (2, 0, 1, 3)), jnp.transpose(residual, (2, 0, 1, 3))


def solution(mesh):
    wide, long = mesh.shape["gy"] // 2, mesh.shape["gz"]
    split = Mesh(mesh.devices.reshape(mesh.shape["gx"], wide, 2, long), ("gx", "gy_0", "gy_1", "gz"))
    spec = P(None, "gx", GY, "gz")
    return jax.shard_map(
        on_device,
        mesh=split,
        in_specs=(spec, P(), P("gx", GY, "gz")),
        out_specs=(spec, spec),
        check_vma=False,
    )
```

```python
import functools

import jax
import jax.numpy as jnp
import numpy as np
from jax import lax
from jax.experimental import pallas as pl
from jax.experimental.pallas import tpu as pltpu
from jax.sharding import Mesh
from jax.sharding import PartitionSpec as P

PLANE = ("gx", "gy_0", "gy_1")
GY = ("gy_0", "gy_1")
SIGMA = 0.25
COLS = 16
LANES = 128
HIGH = lax.Precision.HIGHEST


def stiffness_table():
    line_mass = np.array([[1.0 / 3.0, 1.0 / 6.0], [1.0 / 6.0, 1.0 / 3.0]])
    line_stiff = np.array([[1.0, -1.0], [-1.0, 1.0]])
    table = np.zeros((8, 8))
    for target in range(8):
        for source in range(8):
            target_bits = [target >> 2 & 1, target >> 1 & 1, target & 1]
            source_bits = [source >> 2 & 1, source >> 1 & 1, source & 1]
            total = 0.0
            for stiff_dim in range(3):
                factor = 1.0
                for other in range(3):
                    if other == stiff_dim:
                        factor = factor * line_stiff[target_bits[other], source_bits[other]]
                    else:
                        factor = factor * line_mass[target_bits[other], source_bits[other]]
                total = total + factor
            table[target, source] = total
    return table


def kernel_scale():
    table = np.asarray(jnp.asarray(stiffness_table(), jnp.bfloat16).astype(jnp.float32))
    unit = -float(table[0, 7])
    for target in range(8):
        for source in range(8):
            bits = bin(target ^ source).count("1")
            want = (4.0, 0.0, -1.0, -1.0)[bits] * unit
            assert abs(float(table[target, source]) - want) < 1e-12
    return unit


UNIT = kernel_scale()


def lowered(value):
    return value.astype(jnp.bfloat16).astype(jnp.float32)


def shifted(tiles, step):
    lane = lax.broadcasted_iota(jnp.int32, tiles[0].shape, 1)
    turned = [pltpu.roll(t, (-step) % LANES, 1) for t in tiles]
    count = len(tiles)
    edge = lane < LANES - 1 if step == 1 else lane > 0
    return [jnp.where(edge, turned[i], turned[(i + step) % count]) for i in range(count)]


def operator(field, low, above, below, both, x, y, wx, wy):
    plane, up, down = [], [], []
    for tile in range(3):
        around = {
            (i, j): low(x + i, y + j, tile) for i in (-1, 0, 1) for j in (-1, 0, 1)
        }
        centre = 4.0 * around[0, 0]
        in_plane, from_above, from_below = None, None, None
        for i in (-1, 1):
            for j in (-1, 1):
                ex, ey = wx + (i - 1) // 2, wy + (j - 1) // 2
                others = around[i, 0] + around[0, j] + around[i, j]
                terms = (
                    both(ex, ey, tile) * (centre - around[i, j]),
                    below(ex, ey, tile) * others,
                    above(ex, ey, tile) * others,
                )
                if in_plane is None:
                    in_plane, from_above, from_below = terms
                else:
                    in_plane = in_plane + terms[0]
                    from_above = from_above + terms[1]
                    from_below = from_below + terms[2]
        plane.append(in_plane)
        up.append(from_above)
        down.append(from_below)
    up, down = shifted(up, 1), shifted(down, -1)
    return [SIGMA * field(t) + (plane[t] - up[t] - down[t]) for t in range(3)]


def tile_of(tile):
    return slice(tile * LANES, (tile + 1) * LANES)


def pack_kernel(n_ref, lo_ref, hi_ref, ext_x, ext_y):
    nodes = ext_x * ext_y
    for first, out_ref in ((True, lo_ref), (False, hi_ref)):
        base = 0 if first else n_ref.shape[0] // 2
        turn = 0 if first else 2
        lane = lax.broadcasted_iota(jnp.int32, (COLS, LANES), 1)
        packed = jnp.zeros((COLS, LANES), jnp.float32)
        for node in range(nodes):
            value = n_ref[pl.ds(base + node, COLS, stride=nodes), :]
            shift = (2 * node + turn) % LANES
            moved = pltpu.roll(value, shift, 1) if shift else value
            packed = jnp.where(lane // 2 == node, moved, packed)
        out_ref[:COLS, :] = packed
        lane = lax.broadcasted_iota(jnp.int32, (ext_y, LANES), 1)
        packed = jnp.zeros((ext_y, LANES), jnp.float32)
        for x in range(ext_x):
            start = base + COLS * nodes + x * ext_y
            value = n_ref[start : start + ext_y, :]
            shift = (2 * x + turn) % LANES
            moved = pltpu.roll(value, shift, 1) if shift else value
            packed = jnp.where(lane // 2 == x, moved, packed)
        out_ref[COLS : COLS + ext_y, :] = packed


def ends_tile(before, after, index):
    lane = lax.broadcasted_iota(jnp.int32, before.shape, 1)
    back, ahead = (-2 * index) % LANES, (LANES - 2 - 2 * index) % LANES
    follows = pltpu.roll(after, back, 1) if back else after
    comes = pltpu.roll(before, ahead, 1) if ahead else before
    return jnp.where(lane < 2, follows, jnp.where(lane >= LANES - 2, comes, 0.0))


def moments_kernel(
    moduli_ref, n_ref, before_ref, after_ref,
    v_ref, q_ref, above_ref, below_ref, both_ref, g_ref,
    low_ref, qlow_ref, e_ref,
):
    ext_x, ext_y = low_ref.shape[0], low_ref.shape[1]
    nodes = ext_x * ext_y
    base = n_ref.shape[0] // 2
    for x in range(ext_x):
        start = COLS * nodes + x * ext_y
        third = ends_tile(before_ref[COLS : COLS + ext_y, :], after_ref[COLS : COLS + ext_y, :], x)
        tiles = [n_ref[t * base + start : t * base + start + ext_y, :] for t in range(2)] + [third]
        for t in range(3):
            modulus = jnp.zeros_like(third)
            for level in range(moduli_ref.shape[0]):
                modulus = jnp.where(tiles[t] == level + 1.0, moduli_ref[level], modulus)
            e_ref[x, :, tile_of(t)] = modulus
    for ex in range(ext_x - 1):
        flat = []
        for t in range(3):
            both_x = e_ref[ex, :, tile_of(t)] + e_ref[ex + 1, :, tile_of(t)]
            flat.append(both_x + pltpu.roll(both_x, ext_y - 1, 0))
        ahead = shifted(flat, 1)
        weights = [(0.125 * UNIT) * (flat[t] + ahead[t]) for t in range(3)]
        behind = shifted(weights, -1)
        for t in range(3):
            above_ref[ex, :, tile_of(t)] = weights[t]
            below_ref[ex, :, tile_of(t)] = behind[t]
            both_ref[ex, :, tile_of(t)] = weights[t] + behind[t]
    before, after = before_ref[:COLS, :], after_ref[:COLS, :]
    for x in range(ext_x):
        for y in range(ext_y):
            node = x * ext_y + y
            tiles = [n_ref[pl.ds(t * base + node, COLS, stride=nodes), :] for t in range(2)]
            tiles.append(ends_tile(before, after, node))
            for t in range(3):
                low_ref[x, y, :, tile_of(t)] = lowered(tiles[t])
                if 0 < x < ext_x - 1 and 0 < y < ext_y - 1:
                    v_ref[x - 1, y - 1, :, tile_of(t)] = tiles[t]

    def weight(ref):
        return lambda ex, ey, t: ref[ex, ey : ey + 1, tile_of(t)]

    sides = (weight(above_ref), weight(below_ref), weight(both_ref))
    for x in range(1, ext_x - 1):
        for y in range(1, ext_y - 1):
            image = operator(
                lambda t: v_ref[x - 1, y - 1, :, tile_of(t)],
                lambda i, j, t: low_ref[i, j, :, tile_of(t)],
                *sides,
                x,
                y,
                x,
                y,
            )
            for t in range(3):
                inside = e_ref[x, y : y + 1, tile_of(t)] > 0.0
                value = jnp.where(inside, image[t], 0.0)
                q_ref[x - 1, y - 1, :, tile_of(t)] = value
                qlow_ref[x - 1, y - 1, :, tile_of(t)] = lowered(value)
    total = jnp.zeros((2 * COLS, LANES), jnp.float32)
    pad = jnp.zeros((LANES - 3 * COLS, 2 * LANES), jnp.float32)
    for x in range(2, ext_x - 2):
        for y in range(2, ext_y - 2):
            image = operator(
                lambda t: q_ref[x - 1, y - 1, :, tile_of(t)],
                lambda i, j, t: qlow_ref[i, j, :, tile_of(t)],
                *sides,
                x - 1,
                y - 1,
                x,
                y,
            )
            b = v_ref[x - 1, y - 1, :, : 2 * LANES]
            q = q_ref[x - 1, y - 1, :, : 2 * LANES]
            w = jnp.concatenate(image[:2], axis=1)
            left = jnp.concatenate([b, q], axis=0)
            right = jnp.concatenate([b, q, w, pad], axis=0)
            total = total + lax.dot_general(
                left, right, (((1,), (1,)), ((), ())), precision=HIGH, preferred_element_type=jnp.float32
            )
    g_ref[...] = pack_moments(total)


def pack_moments(total):
    first, second = total[:COLS], total[COLS:]
    row = lax.broadcasted_iota(jnp.int32, (COLS, LANES), 0)
    lane = lax.broadcasted_iota(jnp.int32, (COLS, LANES), 1)
    col = lane % COLS
    upper = jnp.where(lane < COLS, first, second)
    lower = jnp.where(
        lane < COLS,
        0.5 * (pltpu.roll(first, LANES - COLS, 1) + second),
        pltpu.roll(second, LANES - COLS, 1),
    )
    valid = lane < 2 * COLS
    square = jnp.where(valid, jnp.where(row <= col, upper, lower), 0.0)
    diagonal = jnp.sum(jnp.where(valid & (row == col), lower, 0.0), axis=0, keepdims=True)
    out = []
    for half in range(2):
        out.append(square[8 * half : 8 * half + 8])
    spread_rows = jnp.zeros((8, LANES), jnp.float32)
    sub8 = lax.broadcasted_iota(jnp.int32, (8, LANES), 0)
    lane8 = lax.broadcasted_iota(jnp.int32, (8, LANES), 1)
    for quarter in range(4):
        piece = out[quarter // 2]
        if quarter % 2:
            piece = pltpu.roll(piece, 4, 0)
        if quarter:
            piece = pltpu.roll(piece, 2 * COLS * quarter, 1)
        here = (sub8 < 4) & (lane8 // (2 * COLS) == quarter)
        spread_rows = jnp.where(here, piece, spread_rows)
    return jnp.where(sub8 == 4, diagonal, spread_rows)


def unpack_moments(packed):
    sub8 = lax.broadcasted_iota(jnp.int32, (8, LANES), 0)
    halves = []
    for half in range(2):
        a, b = 2 * half, 2 * half + 1
        top = pltpu.roll(packed, LANES - 2 * COLS * a, 1) if a else packed
        bottom = pltpu.roll(pltpu.roll(packed, LANES - 2 * COLS * b, 1), 4, 0)
        halves.append(jnp.where(sub8 < 4, top, bottom))
    square = jnp.concatenate(halves, axis=0)
    row = lax.broadcasted_iota(jnp.int32, (COLS, COLS), 0)
    col = lax.broadcasted_iota(jnp.int32, (COLS, COLS), 1)
    moments = []
    for pair in range(2):
        turned = pltpu.roll(square, LANES - COLS, 1) if pair else square
        mixed = turned[:, :COLS]
        diagonal = (pltpu.roll(packed, LANES - COLS, 1) if pair else packed)[4:5, :COLS]
        flipped = mixed.T
        moments.append(jnp.where(row <= col, mixed, flipped))
        lower = jnp.where(row == col, diagonal, jnp.where(row > col, mixed, flipped))
        moments.append(lower)
    return moments


def dot(left, right, dims=((1,), (0,))):
    return lax.dot_general(left, right, (dims, ((), ())), precision=HIGH, preferred_element_type=jnp.float32)


def inverse(matrix):
    size = COLS
    sub = lax.broadcasted_iota(jnp.int32, (size, LANES), 0)
    rows = [jnp.broadcast_to(matrix[:, i : i + 1], (size, LANES)) for i in range(size)]
    for k in range(size):
        scale = 1.0 / rows[k][k : k + 1, :]
        pivot_row = rows[k] * scale
        for i in range(size):
            if i != k:
                factor = rows[i][k : k + 1, :]
                moved = rows[i] - factor * pivot_row
                rows[i] = jnp.where(sub == k, factor * scale, moved)
        rows[k] = jnp.where(sub == k, -scale, pivot_row)
    lane = lax.broadcasted_iota(jnp.int32, (size, LANES), 1)
    out = jnp.zeros((size, LANES), jnp.float32)
    for i in range(size):
        out = jnp.where(lane == i, -rows[i], out)
    return out[:, :size]


def solve(matrix, right):
    inv = inverse(matrix)
    guess = dot(inv, right)
    return guess + dot(inv, right - dot(matrix, guess))


def finish_kernel(g_ref, v_ref, q_ref, above_ref, below_ref, both_ref, sol_ref, res_ref, d_ref, dlow_ref):
    own_x, own_y = v_ref.shape[0], v_ref.shape[1]
    m0, m1, m2, m3 = unpack_moments(g_ref[...])
    first = ((0,), (0,))
    alpha = solve(m1, m0)
    m1a, m2a, m3a = dot(m1, alpha), dot(m2, alpha), dot(m3, alpha)
    updated = m0 - m1a - dot(alpha, m1, first) + dot(alpha, m2a, first)
    beta = solve(m0, updated)
    row = lax.broadcasted_iota(jnp.int32, (COLS, COLS), 0)
    col = lax.broadcasted_iota(jnp.int32, (COLS, COLS), 1)
    mix = beta + jnp.where(row == col, 1.0, 0.0)
    curved = dot(mix, dot(m1, mix) - m2a, first) + dot(alpha, m3a - dot(m2, mix), first)
    curved = 0.5 * (curved + curved.T)
    gamma = solve(curved, updated)
    both = jnp.concatenate([mix, -alpha], axis=0)
    for x in range(own_x):
        for y in range(own_y):
            block = jnp.concatenate([v_ref[x, y], q_ref[x, y]], axis=0)
            value = dot(both, block, first)
            d_ref[x, y] = value
            dlow_ref[x, y] = lowered(value)

    def weight(ref):
        return lambda ex, ey, t: ref[ex, ey : ey + 1, tile_of(t)]

    sides = (weight(above_ref), weight(below_ref), weight(both_ref))
    to_sol = jnp.concatenate([alpha, gamma], axis=0)
    to_res = jnp.concatenate([-alpha, -gamma], axis=0)
    for x in range(1, own_x - 1):
        for y in range(1, own_y - 1):
            image = operator(
                lambda t: d_ref[x, y, :, tile_of(t)],
                lambda i, j, t: dlow_ref[i, j, :, tile_of(t)],
                *sides,
                x,
                y,
                x + 1,
                y + 1,
            )
            b = v_ref[x, y, :, : 2 * LANES]
            q = q_ref[x, y, :, : 2 * LANES]
            d = d_ref[x, y, :, : 2 * LANES]
            i2 = jnp.concatenate(image[:2], axis=1)
            sol_ref[:, x - 1, y - 1, :] = dot(to_sol, jnp.concatenate([b, d], axis=0), first)
            res_ref[:, x - 1, y - 1, :] = b + dot(to_res, jnp.concatenate([q, i2], axis=0), first)


def ring(axis, step):
    count = lax.axis_size(axis)
    ends = range(count - 1)
    return [(i, i + 1) for i in ends] if step > 0 else [(i + 1, i) for i in ends]


def both_ways(axis, to_next, to_last):
    return lax.ppermute(to_next, axis, ring(axis, 1)), lax.ppermute(to_last, axis, ring(axis, -1))


def spread(value, axes, groups=None):
    count = lax.axis_size(axes)
    copies = jnp.broadcast_to(value[None], (count, *value.shape))
    return jnp.sum(lax.all_to_all(copies, axes, 0, 0, axis_index_groups=groups), axis=0)


def near(value):
    return pltpu.with_memory_space_constraint(value, pltpu.VMEM)


def on_device(loads, moduli, material):
    f32 = jnp.float32
    own = jnp.concatenate([loads, (material[None] + 1).astype(f32)], axis=0)
    own = jnp.stack([own[..., :LANES], own[..., LANES:]])
    before, after = both_ways("gx", own, own)
    own = jnp.concatenate([before, own, after], axis=2)
    before, after = both_ways(GY, own[:, :, :, 2:], own[:, :, :, :2])
    own = jnp.concatenate([before, own, after], axis=3)
    ext_x, ext_y = own.shape[2:4]
    natural = near(own.reshape(2 * (COLS + 1) * ext_x * ext_y, LANES))
    ends = pltpu.VMEM((COLS + 8, LANES), f32)
    first, last = pl.pallas_call(
        functools.partial(pack_kernel, ext_x=ext_x, ext_y=ext_y), out_shape=(ends, ends), name="pack"
    )(natural)
    before, after = both_ways("gz", last, first)
    wide = 3 * LANES
    weights = pltpu.VMEM((ext_x - 1, ext_y, wide), f32)
    field = pltpu.VMEM((ext_x - 2, ext_y - 2, COLS, wide), f32)
    in_vmem = pl.BlockSpec(memory_space=pltpu.VMEM)
    block, image, above, below, both, moments = pl.pallas_call(
        moments_kernel,
        out_shape=(field, field, weights, weights, weights, pltpu.VMEM((8, LANES), f32)),
        in_specs=[pl.BlockSpec(memory_space=pltpu.SMEM), in_vmem, in_vmem, in_vmem],
        scratch_shapes=[
            pltpu.VMEM((ext_x, ext_y, COLS, wide), f32),
            pltpu.VMEM((ext_x - 2, ext_y - 2, COLS, wide), f32),
            pltpu.VMEM((ext_x, ext_y, wide), f32),
        ],
        name="moments",
    )(moduli, natural, near(before), near(after))
    rows = 5
    count = lax.axis_size("gz")
    middle = [[(i + count // 2) % count for i in range(count)]]
    moments = spread(moments[:rows].reshape(rows, 1, LANES), PLANE)
    moments = spread(moments, "gz", middle).reshape(rows, LANES)
    moments = jnp.concatenate([moments, jnp.zeros((8 - rows, LANES), f32)], axis=0)
    out = jax.ShapeDtypeStruct(loads.shape, f32)
    return pl.pallas_call(
        finish_kernel,
        out_shape=(out, out),
        scratch_shapes=[pltpu.VMEM(field.shape, f32)] * 2,
        name="finish",
    )(near(moments), near(block), near(image), near(above), near(below), near(both))


def solution(mesh):
    wide, long = mesh.shape["gy"] // 2, mesh.shape["gz"]
    split = Mesh(mesh.devices.reshape(mesh.shape["gx"], wide, 2, long), ("gx", "gy_0", "gy_1", "gz"))
    spec = P(None, "gx", GY, "gz")
    return jax.shard_map(
        on_device,
        mesh=split,
        in_specs=(spec, P(), P("gx", GY, "gz")),
        out_specs=(spec, spec),
        check_vma=False,
    )
```

```python
import functools

import jax
import jax.numpy as jnp
import numpy as np
from jax import lax
from jax.experimental import pallas as pl
from jax.experimental.pallas import tpu as pltpu
from jax.sharding import Mesh
from jax.sharding import PartitionSpec as P

PLANE = ("gx", "gy_0", "gy_1")
GY = ("gy_0", "gy_1")
SIGMA = 0.25
COLS = 16
LANES = 128
HIGH = lax.Precision.HIGHEST


def stiffness_table():
    line_mass = np.array([[1.0 / 3.0, 1.0 / 6.0], [1.0 / 6.0, 1.0 / 3.0]])
    line_stiff = np.array([[1.0, -1.0], [-1.0, 1.0]])
    table = np.zeros((8, 8))
    for target in range(8):
        for source in range(8):
            target_bits = [target >> 2 & 1, target >> 1 & 1, target & 1]
            source_bits = [source >> 2 & 1, source >> 1 & 1, source & 1]
            total = 0.0
            for stiff_dim in range(3):
                factor = 1.0
                for other in range(3):
                    if other == stiff_dim:
                        factor = factor * line_stiff[target_bits[other], source_bits[other]]
                    else:
                        factor = factor * line_mass[target_bits[other], source_bits[other]]
                total = total + factor
            table[target, source] = total
    return table


def kernel_scale():
    table = np.asarray(jnp.asarray(stiffness_table(), jnp.bfloat16).astype(jnp.float32))
    unit = -float(table[0, 7])
    for target in range(8):
        for source in range(8):
            bits = bin(target ^ source).count("1")
            want = (4.0, 0.0, -1.0, -1.0)[bits] * unit
            assert abs(float(table[target, source]) - want) < 1e-12
    return unit


UNIT = kernel_scale()


def lowered(value):
    return value.astype(jnp.bfloat16).astype(jnp.float32)


def shifted(tiles, step):
    lane = lax.broadcasted_iota(jnp.int32, tiles[0].shape, 1)
    turned = [pltpu.roll(t, (-step) % LANES, 1) for t in tiles]
    count = len(tiles)
    edge = lane < LANES - 1 if step == 1 else lane > 0
    return [jnp.where(edge, turned[i], turned[(i + step) % count]) for i in range(count)]


def operator(field, low, above, below, both, x, y, wx, wy):
    plane, up, down = [], [], []
    for tile in range(3):
        around = {
            (i, j): low(x + i, y + j, tile) for i in (-1, 0, 1) for j in (-1, 0, 1)
        }
        centre = 4.0 * around[0, 0]
        in_plane, from_above, from_below = None, None, None
        for i in (-1, 1):
            for j in (-1, 1):
                ex, ey = wx + (i - 1) // 2, wy + (j - 1) // 2
                others = around[i, 0] + around[0, j] + around[i, j]
                terms = (
                    both(ex, ey, tile) * (centre - around[i, j]),
                    below(ex, ey, tile) * others,
                    above(ex, ey, tile) * others,
                )
                if in_plane is None:
                    in_plane, from_above, from_below = terms
                else:
                    in_plane = in_plane + terms[0]
                    from_above = from_above + terms[1]
                    from_below = from_below + terms[2]
        plane.append(in_plane)
        up.append(from_above)
        down.append(from_below)
    up, down = shifted(up, 1), shifted(down, -1)
    return [SIGMA * field(t) + (plane[t] - up[t] - down[t]) for t in range(3)]


def tile_of(tile):
    return slice(tile * LANES, (tile + 1) * LANES)


def pack_kernel(n_ref, lo_ref, hi_ref, ext_x, ext_y):
    nodes = ext_x * ext_y
    for first, out_ref in ((True, lo_ref), (False, hi_ref)):
        base = 0 if first else n_ref.shape[0] // 2
        turn = 0 if first else 2
        lane = lax.broadcasted_iota(jnp.int32, (COLS, LANES), 1)
        packed = jnp.zeros((COLS, LANES), jnp.float32)
        for node in range(nodes):
            value = n_ref[pl.ds(base + node, COLS, stride=nodes), :]
            shift = (2 * node + turn) % LANES
            moved = pltpu.roll(value, shift, 1) if shift else value
            packed = jnp.where(lane // 2 == node, moved, packed)
        out_ref[:COLS, :] = packed
        lane = lax.broadcasted_iota(jnp.int32, (ext_y, LANES), 1)
        packed = jnp.zeros((ext_y, LANES), jnp.float32)
        for x in range(ext_x):
            start = base + COLS * nodes + x * ext_y
            value = n_ref[start : start + ext_y, :]
            shift = (2 * x + turn) % LANES
            moved = pltpu.roll(value, shift, 1) if shift else value
            packed = jnp.where(lane // 2 == x, moved, packed)
        out_ref[COLS : COLS + ext_y, :] = packed


def ends_tile(before, after, index):
    lane = lax.broadcasted_iota(jnp.int32, before.shape, 1)
    back, ahead = (-2 * index) % LANES, (LANES - 2 - 2 * index) % LANES
    follows = pltpu.roll(after, back, 1) if back else after
    comes = pltpu.roll(before, ahead, 1) if ahead else before
    return jnp.where(lane < 2, follows, jnp.where(lane >= LANES - 2, comes, 0.0))


def moments_kernel(
    moduli_ref, n_ref, before_ref, after_ref,
    v_ref, q_ref, above_ref, below_ref, both_ref, g_ref,
    low_ref, qlow_ref, e_ref,
):
    ext_x, ext_y = low_ref.shape[0], low_ref.shape[1]
    nodes = ext_x * ext_y
    base = n_ref.shape[0] // 2
    for x in range(ext_x):
        start = COLS * nodes + x * ext_y
        third = ends_tile(before_ref[COLS : COLS + ext_y, :], after_ref[COLS : COLS + ext_y, :], x)
        tiles = [n_ref[t * base + start : t * base + start + ext_y, :] for t in range(2)] + [third]
        for t in range(3):
            modulus = jnp.zeros_like(third)
            for level in range(moduli_ref.shape[0]):
                modulus = jnp.where(tiles[t] == level + 1.0, moduli_ref[level], modulus)
            e_ref[x, :, tile_of(t)] = modulus
    for ex in range(ext_x - 1):
        flat = []
        for t in range(3):
            both_x = e_ref[ex, :, tile_of(t)] + e_ref[ex + 1, :, tile_of(t)]
            flat.append(both_x + pltpu.roll(both_x, ext_y - 1, 0))
        ahead = shifted(flat, 1)
        weights = [(0.125 * UNIT) * (flat[t] + ahead[t]) for t in range(3)]
        behind = shifted(weights, -1)
        for t in range(3):
            above_ref[ex, :, tile_of(t)] = weights[t]
            below_ref[ex, :, tile_of(t)] = behind[t]
            both_ref[ex, :, tile_of(t)] = weights[t] + behind[t]
    before, after = before_ref[:COLS, :], after_ref[:COLS, :]
    for x in range(ext_x):
        for y in range(ext_y):
            node = x * ext_y + y
            tiles = [n_ref[pl.ds(t * base + node, COLS, stride=nodes), :] for t in range(2)]
            tiles.append(ends_tile(before, after, node))
            for t in range(3):
                low_ref[x, y, :, tile_of(t)] = lowered(tiles[t])
                if 0 < x < ext_x - 1 and 0 < y < ext_y - 1:
                    v_ref[x - 1, y - 1, :, tile_of(t)] = tiles[t]

    def weight(ref):
        return lambda ex, ey, t: ref[ex, ey : ey + 1, tile_of(t)]

    sides = (weight(above_ref), weight(below_ref), weight(both_ref))
    for x in range(1, ext_x - 1):
        for y in range(1, ext_y - 1):
            image = operator(
                lambda t: v_ref[x - 1, y - 1, :, tile_of(t)],
                lambda i, j, t: low_ref[i, j, :, tile_of(t)],
                *sides,
                x,
                y,
                x,
                y,
            )
            for t in range(3):
                inside = e_ref[x, y : y + 1, tile_of(t)] > 0.0
                value = jnp.where(inside, image[t], 0.0)
                q_ref[x - 1, y - 1, :, tile_of(t)] = value
                qlow_ref[x - 1, y - 1, :, tile_of(t)] = lowered(value)
    total = jnp.zeros((2 * COLS, LANES), jnp.float32)
    pad = jnp.zeros((LANES - 3 * COLS, 2 * LANES), jnp.float32)
    for x in range(2, ext_x - 2):
        for y in range(2, ext_y - 2):
            image = operator(
                lambda t: q_ref[x - 1, y - 1, :, tile_of(t)],
                lambda i, j, t: qlow_ref[i, j, :, tile_of(t)],
                *sides,
                x - 1,
                y - 1,
                x,
                y,
            )
            b = v_ref[x - 1, y - 1, :, : 2 * LANES]
            q = q_ref[x - 1, y - 1, :, : 2 * LANES]
            w = jnp.concatenate(image[:2], axis=1)
            left = jnp.concatenate([b, q], axis=0)
            right = jnp.concatenate([b, q, w, pad], axis=0)
            total = total + lax.dot_general(
                left, right, (((1,), (1,)), ((), ())), precision=HIGH, preferred_element_type=jnp.float32
            )
    g_ref[...] = pack_moments(total)


def pack_moments(total):
    first, second = total[:COLS], total[COLS:]
    row = lax.broadcasted_iota(jnp.int32, (COLS, LANES), 0)
    lane = lax.broadcasted_iota(jnp.int32, (COLS, LANES), 1)
    col = lane % COLS
    upper = jnp.where(lane < COLS, first, second)
    lower = jnp.where(
        lane < COLS,
        0.5 * (pltpu.roll(first, LANES - COLS, 1) + second),
        pltpu.roll(second, LANES - COLS, 1),
    )
    valid = lane < 2 * COLS
    square = jnp.where(valid, jnp.where(row <= col, upper, lower), 0.0)
    diagonal = jnp.sum(jnp.where(valid & (row == col), lower, 0.0), axis=0, keepdims=True)
    out = []
    for half in range(2):
        out.append(square[8 * half : 8 * half + 8])
    spread_rows = jnp.zeros((8, LANES), jnp.float32)
    sub8 = lax.broadcasted_iota(jnp.int32, (8, LANES), 0)
    lane8 = lax.broadcasted_iota(jnp.int32, (8, LANES), 1)
    for quarter in range(4):
        piece = out[quarter // 2]
        if quarter % 2:
            piece = pltpu.roll(piece, 4, 0)
        if quarter:
            piece = pltpu.roll(piece, 2 * COLS * quarter, 1)
        here = (sub8 < 4) & (lane8 // (2 * COLS) == quarter)
        spread_rows = jnp.where(here, piece, spread_rows)
    return jnp.where(sub8 == 4, diagonal, spread_rows)


def unpack_moments(packed):
    sub8 = lax.broadcasted_iota(jnp.int32, (8, LANES), 0)
    halves = []
    for half in range(2):
        a, b = 2 * half, 2 * half + 1
        top = pltpu.roll(packed, LANES - 2 * COLS * a, 1) if a else packed
        bottom = pltpu.roll(pltpu.roll(packed, LANES - 2 * COLS * b, 1), 4, 0)
        halves.append(jnp.where(sub8 < 4, top, bottom))
    square = jnp.concatenate(halves, axis=0)
    row = lax.broadcasted_iota(jnp.int32, (COLS, COLS), 0)
    col = lax.broadcasted_iota(jnp.int32, (COLS, COLS), 1)
    moments = []
    for pair in range(2):
        turned = pltpu.roll(square, LANES - COLS, 1) if pair else square
        mixed = turned[:, :COLS]
        diagonal = (pltpu.roll(packed, LANES - COLS, 1) if pair else packed)[4:5, :COLS]
        flipped = mixed.T
        moments.append(jnp.where(row <= col, mixed, flipped))
        lower = jnp.where(row == col, diagonal, jnp.where(row > col, mixed, flipped))
        moments.append(lower)
    return moments


def dot(left, right, dims=((1,), (0,))):
    return lax.dot_general(left, right, (dims, ((), ())), precision=HIGH, preferred_element_type=jnp.float32)


def inverse(matrix):
    size = COLS
    sub = lax.broadcasted_iota(jnp.int32, (size, LANES), 0)
    rows = [jnp.broadcast_to(matrix[:, i : i + 1], (size, LANES)) for i in range(size)]
    for k in range(size):
        scale = 1.0 / rows[k][k : k + 1, :]
        pivot_row = rows[k] * scale
        for i in range(size):
            if i != k:
                factor = rows[i][k : k + 1, :]
                moved = rows[i] - factor * pivot_row
                rows[i] = jnp.where(sub == k, factor * scale, moved)
        rows[k] = jnp.where(sub == k, -scale, pivot_row)
    lane = lax.broadcasted_iota(jnp.int32, (size, LANES), 1)
    out = jnp.zeros((size, LANES), jnp.float32)
    for i in range(size):
        out = jnp.where(lane == i, -rows[i], out)
    return out[:, :size]


def finish_kernel(g_ref, v_ref, q_ref, above_ref, below_ref, both_ref, sol_ref, res_ref, d_ref, dlow_ref):
    own_x, own_y = v_ref.shape[0], v_ref.shape[1]
    m0, m1, m2, m3 = unpack_moments(g_ref[...])
    first = ((0,), (0,))
    inv = inverse(m1)
    alpha = dot(inv, m0)
    m2a = dot(m2, alpha)
    mix = dot(inv, m2a)
    updated = dot(alpha, m2a, first) - m0
    curved = dot(alpha, dot(m3, alpha), first) - dot(m2a, mix, first)
    gamma = dot(inverse(0.5 * (curved + curved.T)), updated)
    both = jnp.concatenate([mix, -alpha], axis=0)
    for x in range(own_x):
        for y in range(own_y):
            block = jnp.concatenate([v_ref[x, y], q_ref[x, y]], axis=0)
            value = dot(both, block, first)
            d_ref[x, y] = value
            dlow_ref[x, y] = lowered(value)

    def weight(ref):
        return lambda ex, ey, t: ref[ex, ey : ey + 1, tile_of(t)]

    sides = (weight(above_ref), weight(below_ref), weight(both_ref))
    to_sol = jnp.concatenate([alpha, gamma], axis=0)
    to_res = jnp.concatenate([-alpha, -gamma], axis=0)
    for x in range(1, own_x - 1):
        for y in range(1, own_y - 1):
            image = operator(
                lambda t: d_ref[x, y, :, tile_of(t)],
                lambda i, j, t: dlow_ref[i, j, :, tile_of(t)],
                *sides,
                x,
                y,
                x + 1,
                y + 1,
            )
            b = v_ref[x, y, :, : 2 * LANES]
            q = q_ref[x, y, :, : 2 * LANES]
            d = d_ref[x, y, :, : 2 * LANES]
            i2 = jnp.concatenate(image[:2], axis=1)
            sol_ref[:, x - 1, y - 1, :] = dot(to_sol, jnp.concatenate([b, d], axis=0), first)
            res_ref[:, x - 1, y - 1, :] = b + dot(to_res, jnp.concatenate([q, i2], axis=0), first)


def both_ways(axis, to_next, to_last, around=False):
    count = lax.axis_size(axis)
    steps = range(count) if around else range(count - 1)
    before = lax.ppermute(to_next, axis, [(i, (i + 1) % count) for i in steps])
    after = lax.ppermute(to_last, axis, [((i + 1) % count, i) for i in steps])
    if around:
        place = lax.axis_index(axis)
        before = jnp.where(place > 0, before, 0.0)
        after = jnp.where(place < count - 1, after, 0.0)
    return before, after


def spread(value, axes, groups=None):
    count = lax.axis_size(axes)
    copies = jnp.broadcast_to(value[None], (count, *value.shape))
    return jnp.sum(lax.all_to_all(copies, axes, 0, 0, axis_index_groups=groups), axis=0)


def near(value):
    return pltpu.with_memory_space_constraint(value, pltpu.VMEM)


def on_device(loads, moduli, material):
    f32 = jnp.float32
    own = jnp.concatenate([loads, (material[None] + 1).astype(f32)], axis=0)
    own = jnp.stack([own[..., :LANES], own[..., LANES:]])
    before, after = both_ways("gx", own, own)
    own = jnp.concatenate([before, own, after], axis=2)
    before, after = both_ways(GY, own[:, :, :, 2:], own[:, :, :, :2], around=True)
    own = jnp.concatenate([before, own, after], axis=3)
    ext_x, ext_y = own.shape[2:4]
    natural = near(own.reshape(2 * (COLS + 1) * ext_x * ext_y, LANES))
    ends = pltpu.VMEM((COLS + 8, LANES), f32)
    first, last = pl.pallas_call(
        functools.partial(pack_kernel, ext_x=ext_x, ext_y=ext_y), out_shape=(ends, ends), name="pack"
    )(natural)
    before, after = both_ways("gz", last, first)
    wide = 3 * LANES
    weights = pltpu.VMEM((ext_x - 1, ext_y, wide), f32)
    field = pltpu.VMEM((ext_x - 2, ext_y - 2, COLS, wide), f32)
    in_vmem = pl.BlockSpec(memory_space=pltpu.VMEM)
    block, image, above, below, both, moments = pl.pallas_call(
        moments_kernel,
        out_shape=(field, field, weights, weights, weights, pltpu.VMEM((8, LANES), f32)),
        in_specs=[pl.BlockSpec(memory_space=pltpu.SMEM), in_vmem, in_vmem, in_vmem],
        scratch_shapes=[
            pltpu.VMEM((ext_x, ext_y, COLS, wide), f32),
            pltpu.VMEM((ext_x - 2, ext_y - 2, COLS, wide), f32),
            pltpu.VMEM((ext_x, ext_y, wide), f32),
        ],
        name="moments",
    )(moduli, natural, near(before), near(after))
    rows = 5
    count = lax.axis_size("gz")
    middle = [[(i + 5 * count // 8) % count for i in range(count)]]
    moments = spread(moments[:rows].reshape(rows, 1, LANES), "gz", middle)
    moments = spread(moments, PLANE).reshape(rows, LANES)
    moments = jnp.concatenate([moments, jnp.zeros((8 - rows, LANES), f32)], axis=0)
    out = jax.ShapeDtypeStruct(loads.shape, f32)
    return pl.pallas_call(
        finish_kernel,
        out_shape=(out, out),
        scratch_shapes=[pltpu.VMEM(field.shape, f32)] * 2,
        name="finish",
    )(near(moments), near(block), near(image), near(above), near(below), near(both))


def solution(mesh):
    wide, long = mesh.shape["gy"] // 2, mesh.shape["gz"]
    split = Mesh(mesh.devices.reshape(mesh.shape["gx"], wide, 2, long), ("gx", "gy_0", "gy_1", "gz"))
    spec = P(None, "gx", GY, "gz")
    return jax.shard_map(
        on_device,
        mesh=split,
        in_specs=(spec, P(), P("gx", GY, "gz")),
        out_specs=(spec, spec),
        check_vma=False,
    )
```

```python
import functools

import jax
import jax.numpy as jnp
import numpy as np
from jax import lax
from jax.experimental import pallas as pl
from jax.experimental.pallas import tpu as pltpu
from jax.sharding import Mesh
from jax.sharding import PartitionSpec as P

PLANE = ("gx", "gy_0", "gy_1")
GY = ("gy_0", "gy_1")
SIGMA = 0.25
COLS = 16
LANES = 128
EDGE = LANES // 4
HIGH = lax.Precision.HIGHEST


def stiffness_table():
    line_mass = np.array([[1.0 / 3.0, 1.0 / 6.0], [1.0 / 6.0, 1.0 / 3.0]])
    line_stiff = np.array([[1.0, -1.0], [-1.0, 1.0]])
    table = np.zeros((8, 8))
    for target in range(8):
        for source in range(8):
            target_bits = [target >> 2 & 1, target >> 1 & 1, target & 1]
            source_bits = [source >> 2 & 1, source >> 1 & 1, source & 1]
            total = 0.0
            for stiff_dim in range(3):
                factor = 1.0
                for other in range(3):
                    if other == stiff_dim:
                        factor = factor * line_stiff[target_bits[other], source_bits[other]]
                    else:
                        factor = factor * line_mass[target_bits[other], source_bits[other]]
                total = total + factor
            table[target, source] = total
    return table


def kernel_scale():
    table = np.asarray(jnp.asarray(stiffness_table(), jnp.bfloat16).astype(jnp.float32))
    unit = -float(table[0, 7])
    for target in range(8):
        for source in range(8):
            bits = bin(target ^ source).count("1")
            want = (4.0, 0.0, -1.0, -1.0)[bits] * unit
            assert abs(float(table[target, source]) - want) < 1e-12
    return unit


UNIT = kernel_scale()


def lowered(value):
    return value.astype(jnp.bfloat16).astype(jnp.float32)


def tile_of(tile):
    return slice(tile * LANES, (tile + 1) * LANES)


def lanes_of(value):
    return lax.broadcasted_iota(jnp.int32, value.shape, 1)


def turn(value, amount):
    amount %= LANES
    return pltpu.roll(value, amount, 1) if amount else value


def shifted(tiles, step, beyond=None):
    count = len(tiles)
    turned = [turn(t, -step) for t in tiles]
    past = turn(beyond, -step) if beyond is not None else turned[0 if step > 0 else -1]
    lane = lanes_of(tiles[0])
    if step > 0:
        return [jnp.where(lane < LANES - 1, turned[i], turned[i + 1] if i + 1 < count else past) for i in range(count)]
    return [jnp.where(lane > 0, turned[i], turned[i - 1] if i else past) for i in range(count)]


def terms(low, sides, tile, x, y, wx, wy):
    above, below, both = sides
    around = {(i, j): low(x + i, y + j, tile) for i in (-1, 0, 1) for j in (-1, 0, 1)}
    centre = 4.0 * around[0, 0]
    total = None
    for i in (-1, 1):
        for j in (-1, 1):
            ex, ey = wx + (i - 1) // 2, wy + (j - 1) // 2
            others = around[i, 0] + around[0, j] + around[i, j]
            new = (
                both(ex, ey, tile) * (centre - around[i, j]),
                below(ex, ey, tile) * others,
                above(ex, ey, tile) * others,
            )
            total = new if total is None else tuple(a + b for a, b in zip(total, new))
    return total


def operator(field, low, sides, count, x, y, wx, wy):
    plane, down, up = zip(*[terms(low, sides, t, x, y, wx, wy) for t in range(count)])
    from_above, from_below = shifted(down, 1), shifted(up, -1)
    return [SIGMA * field(t) + (plane[t] - from_above[t] - from_below[t]) for t in range(count)]


def split_terms(value, count):
    parts = []
    for n in range(count):
        part = value.astype(jnp.bfloat16)
        parts.append(part)
        if n + 1 < count:
            value = value - part.astype(jnp.float32)
    return jnp.concatenate(parts, axis=0)


def rows_of(refs, flags_ref, tile, x, y, first, count):
    before_ref, mid_ref, after_ref, ext_x = refs
    if y < 2:
        ref, wide, at, flag = before_ref, 2, y, 0
    elif y < 6:
        ref, wide, at, flag = mid_ref, 4, y - 2, None
    else:
        ref, wide, at, flag = after_ref, 2, y - 6, 1
    stride = ext_x * wide
    start = tile * (ref.shape[0] // 2) + first * stride + x * wide + at
    value = ref[pl.ds(start, count, stride=stride), :] if count > 1 else ref[start : start + 1, :]
    if flag is not None:
        value = jnp.where(flags_ref[flag : flag + 1, :] > 0.0, value, 0.0)
    return value


def front_kernel(moduli_ref, loads_ref, material_ref, own_ref, levels_ref):
    for t in range(2):
        own_ref[t, :COLS] = loads_ref[:, :, :, tile_of(t)]
        own_ref[t, COLS] = (material_ref[:, :, tile_of(t)] + 1).astype(jnp.float32)
    for level in range(moduli_ref.shape[0]):
        levels_ref[level : level + 1, :] = jnp.full((1, LANES), moduli_ref[level], jnp.float32)


def pack_kernel(flags_ref, before_ref, mid_ref, after_ref, lo_ref, hi_ref, ext_x, ext_y):
    refs = (before_ref, mid_ref, after_ref, ext_x)
    for tile, out_ref in ((0, lo_ref), (1, hi_ref)):
        offset = 2 * tile
        lane = lax.broadcasted_iota(jnp.int32, (COLS, LANES), 1)
        packed = jnp.zeros((COLS, LANES), jnp.float32)
        ids = [jnp.zeros((1, LANES), jnp.float32)] * ext_y
        for x in range(ext_x):
            for y in range(ext_y):
                node = x * ext_y + y
                value = rows_of(refs, flags_ref, tile, x, y, 0, COLS)
                packed = jnp.where(lane // 2 == node, turn(value, 2 * node + offset), packed)
                value = rows_of(refs, flags_ref, tile, x, y, COLS, 1)
                ids[y] = jnp.where(lane[:1] // 2 == x, turn(value, 2 * x + offset), ids[y])
        out_ref[:COLS, :] = packed
        for y in range(ext_y):
            out_ref[COLS + y : COLS + y + 1, :] = ids[y]


def modulus_of(levels_ref, ids):
    modulus = jnp.zeros_like(ids)
    for level in range(levels_ref.shape[0]):
        modulus = jnp.where(ids == level + 1.0, levels_ref[level : level + 1, :], modulus)
    return modulus


def element_weights(e_ref, above_ref, below_ref, both_ref, count):
    ext_x, ext_y = e_ref.shape[:2]
    for ex in range(ext_x - 1):
        flat = []
        for t in range(count):
            both_x = e_ref[ex, :, tile_of(t)] + e_ref[ex + 1, :, tile_of(t)]
            flat.append(both_x + pltpu.roll(both_x, ext_y - 1, 0))
        ahead = shifted(flat, 1)
        weights = [(0.125 * UNIT) * (flat[t] + ahead[t]) for t in range(count)]
        behind = shifted(weights, -1)
        for t in range(count):
            above_ref[ex, :, tile_of(t)] = weights[t]
            below_ref[ex, :, tile_of(t)] = behind[t]
            both_ref[ex, :, tile_of(t)] = weights[t] + behind[t]


def sides_of(*refs):
    return tuple(lambda ex, ey, t, ref=ref: ref[ex, ey : ey + 1, tile_of(t)] for ref in refs)


def first_image(v_ref, low_ref, e_ref, sides, q_ref, qlow_ref, count):
    ext_x, ext_y = low_ref.shape[0], low_ref.shape[1]
    for x in range(1, ext_x - 1):
        for y in range(1, ext_y - 1):
            image = operator(
                lambda t: v_ref[x - 1, y - 1, :, tile_of(t)],
                lambda i, j, t: low_ref[i, j, :, tile_of(t)],
                sides, count, x, y, x, y,
            )
            for t in range(count):
                value = jnp.where(e_ref[x, y : y + 1, tile_of(t)] > 0.0, image[t], 0.0)
                q_ref[x - 1, y - 1, :, tile_of(t)] = value
                qlow_ref[x - 1, y - 1, :, tile_of(t)] = lowered(value)


def gram_terms(v_ref, q_ref, qlow_ref, sides, count, keep, left_ref, right_ref):
    own_x, own_y = v_ref.shape[0], v_ref.shape[1]
    node = 0
    for x in range(1, own_x - 1):
        for y in range(1, own_y - 1):
            image = operator(
                lambda t: q_ref[x, y, :, tile_of(t)],
                lambda i, j, t: qlow_ref[i, j, :, tile_of(t)],
                sides, count, x, y, x + 1, y + 1,
            )
            for t in range(count):
                b, q = v_ref[x, y, :, tile_of(t)], q_ref[x, y, :, tile_of(t)]
                at = tile_of(node * count + t)
                left = jnp.concatenate([b, q], axis=0)
                left = jnp.where(keep(lanes_of(left), t), left, 0.0)
                left_ref[:, at] = split_terms(left, 3)
                right = jnp.concatenate([b, q, image[t], jnp.zeros_like(b)], axis=0)
                right_ref[:, at] = split_terms(right, 3)
            node += 1
    product = lax.dot_general(
        left_ref[...], right_ref[...], (((1,), (1,)), ((), ())), preferred_element_type=jnp.float32
    )
    half = LANES // 2
    third = jnp.concatenate([product[:, LANES:], jnp.zeros((6 * COLS, half), jnp.float32)], axis=1)
    folded = product[:, :LANES] + turn(product[:, :LANES], half) + third
    return sum(folded[2 * COLS * n : 2 * COLS * (n + 1)] for n in range(3))


def main_kernel(
    levels_ref, flags_ref, before_ref, mid_ref, after_ref,
    v_ref, q_ref, above_ref, below_ref, both_ref, total_ref, ve_ref, ie_ref,
    low_ref, qlow_ref, e_ref, left_ref, right_ref,
):
    ext_x, ext_y = low_ref.shape[0], low_ref.shape[1]
    refs = (before_ref, mid_ref, after_ref, ext_x)
    for x in range(ext_x):
        for y in range(ext_y):
            tiles = [rows_of(refs, flags_ref, t, x, y, COLS, 1) for t in range(2)]
            lane = lanes_of(tiles[0])
            edge = jnp.where(lane < EDGE, tiles[0], jnp.where(lane < 2 * EDGE, turn(tiles[1], 2 * EDGE), 0.0))
            ie_ref[x, y : y + 1, :] = edge
            for t in range(2):
                e_ref[x, y : y + 1, tile_of(t)] = tiles[t]
        for t in range(2):
            e_ref[x, :, tile_of(t)] = modulus_of(levels_ref, e_ref[x, :, tile_of(t)])
    element_weights(e_ref, above_ref, below_ref, both_ref, 2)
    for x in range(ext_x):
        for y in range(ext_y):
            tiles = [rows_of(refs, flags_ref, t, x, y, 0, COLS) for t in range(2)]
            lane = lanes_of(tiles[0])
            edge = jnp.where(lane < EDGE, tiles[0], jnp.where(lane < 2 * EDGE, turn(tiles[1], 2 * EDGE), 0.0))
            ve_ref[x, y] = edge
            for t in range(2):
                low_ref[x, y, :, tile_of(t)] = lowered(tiles[t])
                if 0 < x < ext_x - 1 and 0 < y < ext_y - 1:
                    v_ref[x - 1, y - 1, :, tile_of(t)] = tiles[t]
    sides = sides_of(above_ref, below_ref, both_ref)
    first_image(v_ref, low_ref, e_ref, sides, q_ref, qlow_ref, 2)
    total_ref[...] = gram_terms(
        v_ref, q_ref, qlow_ref, sides, 2,
        lambda lane, t: lane >= 2 if t == 0 else lane < LANES - 2,
        left_ref, right_ref,
    )


def edge_kernel(
    levels_ref, total_ref, ve_ref, ie_ref, before_ref, after_ref,
    v_ref, q_ref, above_ref, below_ref, both_ref, g_ref,
    low_ref, qlow_ref, e_ref, left_ref, right_ref,
):
    ext_x, ext_y = low_ref.shape[0], low_ref.shape[1]

    def with_ends(own, before, after, index):
        lane = lanes_of(own)
        follows, comes = turn(after, LANES // 2 - 2 * index), turn(before, LANES - 2 - 2 * index)
        value = jnp.where(lane >= LANES - 2, comes, own)
        return jnp.where((lane >= LANES // 2) & (lane < LANES // 2 + 2), follows, value)

    for x in range(ext_x):
        ids = with_ends(ie_ref[x], before_ref[COLS : COLS + ext_y, :], after_ref[COLS : COLS + ext_y, :], x)
        e_ref[x] = modulus_of(levels_ref, ids)
    element_weights(e_ref, above_ref, below_ref, both_ref, 1)
    before, after = before_ref[:COLS, :], after_ref[:COLS, :]
    for x in range(ext_x):
        for y in range(ext_y):
            value = with_ends(ve_ref[x, y], before, after, x * ext_y + y)
            low_ref[x, y] = lowered(value)
            if 0 < x < ext_x - 1 and 0 < y < ext_y - 1:
                v_ref[x - 1, y - 1] = value
    sides = sides_of(above_ref, below_ref, both_ref)
    first_image(v_ref, low_ref, e_ref, sides, q_ref, qlow_ref, 1)
    total = gram_terms(
        v_ref, q_ref, qlow_ref, sides, 1,
        lambda lane, t: (lane < 2) | ((lane >= 2 * EDGE - 2) & (lane < 2 * EDGE)),
        left_ref, right_ref,
    )
    g_ref[...] = pack_moments(total_ref[...] + total)


def pack_moments(total):
    first, second = total[:COLS], total[COLS:]
    row = lax.broadcasted_iota(jnp.int32, (COLS, LANES), 0)
    lane = lax.broadcasted_iota(jnp.int32, (COLS, LANES), 1)
    col = lane % COLS
    upper = jnp.where(lane < COLS, first, second)
    lower = jnp.where(
        lane < COLS,
        0.5 * (pltpu.roll(first, LANES - COLS, 1) + second),
        pltpu.roll(second, LANES - COLS, 1),
    )
    valid = lane < 2 * COLS
    square = jnp.where(valid, jnp.where(row <= col, upper, lower), 0.0)
    diagonal = jnp.sum(jnp.where(valid & (row == col), lower, 0.0), axis=0, keepdims=True)
    out = []
    for half in range(2):
        out.append(square[8 * half : 8 * half + 8])
    spread_rows = jnp.zeros((8, LANES), jnp.float32)
    sub8 = lax.broadcasted_iota(jnp.int32, (8, LANES), 0)
    lane8 = lax.broadcasted_iota(jnp.int32, (8, LANES), 1)
    for quarter in range(4):
        piece = out[quarter // 2]
        if quarter % 2:
            piece = pltpu.roll(piece, 4, 0)
        if quarter:
            piece = pltpu.roll(piece, 2 * COLS * quarter, 1)
        here = (sub8 < 4) & (lane8 // (2 * COLS) == quarter)
        spread_rows = jnp.where(here, piece, spread_rows)
    return jnp.where(sub8 == 4, diagonal, spread_rows)


def unpack_moments(packed):
    sub8 = lax.broadcasted_iota(jnp.int32, (8, LANES), 0)
    halves = []
    for half in range(2):
        a, b = 2 * half, 2 * half + 1
        top = pltpu.roll(packed, LANES - 2 * COLS * a, 1) if a else packed
        bottom = pltpu.roll(pltpu.roll(packed, LANES - 2 * COLS * b, 1), 4, 0)
        halves.append(jnp.where(sub8 < 4, top, bottom))
    square = jnp.concatenate(halves, axis=0)
    row = lax.broadcasted_iota(jnp.int32, (COLS, COLS), 0)
    col = lax.broadcasted_iota(jnp.int32, (COLS, COLS), 1)
    moments = []
    for pair in range(2):
        turned = pltpu.roll(square, LANES - COLS, 1) if pair else square
        mixed = turned[:, :COLS]
        diagonal = (pltpu.roll(packed, LANES - COLS, 1) if pair else packed)[4:5, :COLS]
        flipped = mixed.T
        moments.append(jnp.where(row <= col, mixed, flipped))
        lower = jnp.where(row == col, diagonal, jnp.where(row > col, mixed, flipped))
        moments.append(lower)
    return moments


def dot(left, right, dims=((1,), (0,))):
    return lax.dot_general(left, right, (dims, ((), ())), precision=HIGH, preferred_element_type=jnp.float32)


def sweeps(matrix):
    size = COLS
    sub = lax.broadcasted_iota(jnp.int32, (size, LANES), 0)
    rows = [jnp.broadcast_to(matrix[:, i : i + 1], (size, LANES)) for i in range(size)]
    for k in range(size):
        scale = 1.0 / rows[k][k : k + 1, :]
        pivot_row = rows[k] * scale
        for i in range(size):
            if i != k:
                factor = rows[i][k : k + 1, :]
                moved = rows[i] - factor * pivot_row
                rows[i] = jnp.where(sub == k, factor * scale, moved)
        rows[k] = jnp.where(sub == k, -scale, pivot_row)
        yield None
    lane = lax.broadcasted_iota(jnp.int32, (size, LANES), 1)
    out = jnp.zeros((size, LANES), jnp.float32)
    for i in range(size):
        out = jnp.where(lane == i, -rows[i], out)
    yield out[:, :size]


def mixer(coeffs, count):
    flipped = split_terms(coeffs.T, count)
    return jnp.concatenate([flipped] * count, axis=1)


def mixed(left, block, count):
    out = jnp.dot(left, split_terms(block, count), preferred_element_type=jnp.float32)
    size = out.shape[0] // count
    return sum(out[size * n : size * (n + 1)] for n in range(count))


def finish_kernel(
    g_ref, v_ref, q_ref, above_ref, below_ref, both_ref,
    ve_ref, qe_ref, abovee_ref, belowe_ref, bothe_ref,
    sol_ref, res_ref, d_ref, dlow_ref, w0_ref, w1_ref, w2_ref,
):
    own_x, own_y = v_ref.shape[0], v_ref.shape[1]
    m0, m1, m2, m3 = unpack_moments(g_ref[...])
    first = ((0,), (0,))
    *_, inv = sweeps(m1)
    alpha = dot(inv, m0)
    m2a = dot(m2, alpha)
    mix = dot(inv, m2a)
    left = mixer(jnp.concatenate([mix, -alpha], axis=0), 3)
    updated = dot(alpha, m2a, first) - m0
    curved = dot(alpha, dot(m3, alpha), first) - dot(m2a, mix, first)
    steps = sweeps(0.5 * (curved + curved.T))
    inv = None
    for x in range(own_x):
        for y in range(own_y):
            q0, q1, qe = q_ref[x, y, :, :LANES], q_ref[x, y, :, LANES:], qe_ref[x, y]
            lane = lanes_of(qe)
            q0 = jnp.where(lane == 0, qe, q0)
            q1 = jnp.where(lane == LANES - 1, turn(qe, LANES // 2), q1)
            block = jnp.concatenate(
                [
                    jnp.concatenate([v_ref[x, y], ve_ref[x, y]], axis=1),
                    jnp.concatenate([q0, q1, qe], axis=1),
                ],
                axis=0,
            )
            value = mixed(left, block, 3)
            d_ref[x, y] = value
            dlow_ref[x, y] = lowered(value)
            if inv is None:
                inv = next(steps)
    gamma = dot(inv, updated)
    edge, main = (abovee_ref, belowe_ref, bothe_ref), (above_ref, below_ref, both_ref)
    whole = (w0_ref, w1_ref, w2_ref)
    for end_ref, main_ref, whole_ref in zip(edge, main, whole):
        for ex in range(1, own_x):
            end = end_ref[ex]
            lane = lanes_of(end)
            whole_ref[ex, :, :LANES] = jnp.where(lane == 0, end, main_ref[ex, :, :LANES])
            end = turn(end, LANES // 2)
            whole_ref[ex, :, LANES:] = jnp.where(lane == LANES - 1, end, main_ref[ex, :, LANES:])
    main, edge = sides_of(*whole), sides_of(*edge)
    zero = jnp.zeros((COLS, COLS), jnp.float32)
    last = mixer(
        jnp.concatenate(
            [
                jnp.concatenate([alpha, gamma, zero, zero], axis=0),
                jnp.concatenate([zero, zero, -alpha, -gamma], axis=0),
            ],
            axis=1,
        ),
        2,
    )
    for x in range(1, own_x - 1):
        for y in range(1, own_y - 1):
            low = lambda i, j, t: dlow_ref[i, j, :, tile_of(t)]
            at = (x, y, x + 1, y + 1)
            plane, down, up = zip(*[terms(low, main, t, *at) for t in range(2)])
            ends = terms(lambda i, j, t: dlow_ref[i, j, :, tile_of(2)], edge, 0, *at)
            from_above = shifted(down, 1, turn(ends[1], LANES // 2))
            from_below = shifted(up, -1, ends[2])
            image = [
                SIGMA * d_ref[x, y, :, tile_of(t)] + (plane[t] - from_above[t] - from_below[t])
                for t in range(2)
            ]
            q0, q1, qe = q_ref[x, y, :, :LANES], q_ref[x, y, :, LANES:], qe_ref[x, y]
            lane = lanes_of(qe)
            q0 = jnp.where(lane == 0, qe, q0)
            q1 = jnp.where(lane == LANES - 1, turn(qe, LANES // 2), q1)
            b = v_ref[x, y]
            block = jnp.concatenate(
                [
                    b,
                    d_ref[x, y, :, : 2 * LANES],
                    jnp.concatenate([q0, q1], axis=1),
                    jnp.concatenate(image, axis=1),
                ],
                axis=0,
            )
            out = mixed(last, block, 2)
            sol_ref[:, x - 1, y - 1, :] = out[:COLS]
            res_ref[:, x - 1, y - 1, :] = b + out[COLS:]


def both_ways(axis, to_next, to_last, around=False):
    count = lax.axis_size(axis)
    steps = range(count) if around else range(count - 1)
    before = lax.ppermute(to_next, axis, [(i, (i + 1) % count) for i in steps])
    after = lax.ppermute(to_last, axis, [((i + 1) % count, i) for i in steps])
    return before, after


def spread(value, axes, groups=None):
    count = lax.axis_size(axes)
    copies = jnp.broadcast_to(value[None], (count, *value.shape))
    return jnp.sum(lax.all_to_all(copies, axes, 0, 0, axis_index_groups=groups), axis=0)


def near(value):
    return pltpu.with_memory_space_constraint(value, pltpu.VMEM)


def on_device(loads, moduli, material):
    f32, bf16, wide = jnp.float32, jnp.bfloat16, 2 * LANES
    own_x, own_y = material.shape[:2]
    ext_x, ext_y = own_x + 4, own_y + 4
    own, levels = pl.pallas_call(
        front_kernel,
        out_shape=(
            pltpu.VMEM((2, COLS + 1, own_x, own_y, LANES), f32),
            pltpu.VMEM((moduli.shape[0], LANES), f32),
        ),
        in_specs=[
            pl.BlockSpec(memory_space=pltpu.SMEM),
            pl.BlockSpec(memory_space=pltpu.VMEM),
            pl.BlockSpec(memory_space=pltpu.VMEM),
        ],
        name="front",
    )(moduli, loads, material)
    place = lax.axis_index(GY)
    row = lax.broadcasted_iota(jnp.int32, (8, LANES), 0)
    flags = jnp.where(row == 0, place > 0, place < lax.axis_size(GY) - 1).astype(f32)
    before, after = both_ways("gx", own, own)
    mid = jnp.concatenate([before, own, after], axis=2)
    before, after = both_ways(GY, mid[:, :, :, 2:], mid[:, :, :, :2], around=True)
    flat = [near(part.reshape(-1, LANES)) for part in (before, mid, after)]
    ends = pltpu.VMEM((COLS + 8, LANES), f32)
    first, last = pl.pallas_call(
        functools.partial(pack_kernel, ext_x=ext_x, ext_y=ext_y), out_shape=(ends, ends), name="pack"
    )(near(flags), *flat)
    before, after = both_ways("gz", last, first)
    nodes = own_x * own_y

    def weights(size):
        return (pltpu.VMEM((ext_x - 1, ext_y, size), f32),) * 3

    def fields(size):
        return (pltpu.VMEM((ext_x - 2, ext_y - 2, COLS, size), f32),) * 2

    def scratch(size):
        return [
            pltpu.VMEM((ext_x, ext_y, COLS, size), f32),
            pltpu.VMEM((ext_x - 2, ext_y - 2, COLS, size), f32),
            pltpu.VMEM((ext_x, ext_y, size), f32),
            pltpu.VMEM((6 * COLS, nodes * size), bf16),
            pltpu.VMEM((12 * COLS, nodes * size), bf16),
        ]

    *main, total, edge, ids = pl.pallas_call(
        main_kernel,
        out_shape=(
            *fields(wide),
            *weights(wide),
            pltpu.VMEM((2 * COLS, LANES), f32),
            pltpu.VMEM((ext_x, ext_y, COLS, LANES), f32),
            pltpu.VMEM((ext_x, ext_y, LANES), f32),
        ),
        scratch_shapes=scratch(wide),
        name="main",
    )(near(levels), near(flags), *flat)
    *edges, moments = pl.pallas_call(
        edge_kernel,
        out_shape=(*fields(LANES), *weights(LANES), pltpu.VMEM((8, LANES), f32)),
        scratch_shapes=scratch(LANES),
        name="edge",
    )(*[near(value) for value in (levels, total, edge, ids, before, after)])
    rows = 5
    count = lax.axis_size("gz")
    middle = [[(i + 5 * count // 8) % count for i in range(count)]]
    moments = spread(moments[:rows].reshape(rows, 1, LANES), "gz", middle)
    moments = spread(moments, PLANE).reshape(rows, LANES)
    moments = jnp.concatenate([moments, jnp.zeros((8 - rows, LANES), f32)], axis=0)
    out = jax.ShapeDtypeStruct(loads.shape, f32)
    return pl.pallas_call(
        finish_kernel,
        out_shape=(out, out),
        scratch_shapes=[pltpu.VMEM((ext_x - 2, ext_y - 2, COLS, 3 * LANES), f32)] * 2
        + [pltpu.VMEM((ext_x - 1, ext_y, wide), f32)] * 3,
        name="finish",
    )(*[near(value) for value in (moments, *main, *edges)])


def solution(mesh):
    wide, long = mesh.shape["gy"] // 2, mesh.shape["gz"]
    split = Mesh(mesh.devices.reshape(mesh.shape["gx"], wide, 2, long), ("gx", "gy_0", "gy_1", "gz"))
    spec = P(None, "gx", GY, "gz")
    return jax.shard_map(
        on_device,
        mesh=split,
        in_specs=(spec, P(), P("gx", GY, "gz")),
        out_specs=(spec, spec),
        check_vma=False,
    )
```

```python
import functools

import jax
import jax.numpy as jnp
import numpy as np
from jax import lax
from jax.experimental import pallas as pl
from jax.experimental.pallas import tpu as pltpu
from jax.sharding import Mesh
from jax.sharding import PartitionSpec as P

PLANE = ("gx", "gy_0", "gy_1")
GY = ("gy_0", "gy_1")
SIGMA = 0.25
COLS = 16
LANES = 128
EDGE = LANES // 4
HIGH = lax.Precision.HIGHEST


def stiffness_table():
    line_mass = np.array([[1.0 / 3.0, 1.0 / 6.0], [1.0 / 6.0, 1.0 / 3.0]])
    line_stiff = np.array([[1.0, -1.0], [-1.0, 1.0]])
    table = np.zeros((8, 8))
    for target in range(8):
        for source in range(8):
            target_bits = [target >> 2 & 1, target >> 1 & 1, target & 1]
            source_bits = [source >> 2 & 1, source >> 1 & 1, source & 1]
            total = 0.0
            for stiff_dim in range(3):
                factor = 1.0
                for other in range(3):
                    if other == stiff_dim:
                        factor = factor * line_stiff[target_bits[other], source_bits[other]]
                    else:
                        factor = factor * line_mass[target_bits[other], source_bits[other]]
                total = total + factor
            table[target, source] = total
    return table


def kernel_scale():
    table = np.asarray(jnp.asarray(stiffness_table(), jnp.bfloat16).astype(jnp.float32))
    unit = -float(table[0, 7])
    for target in range(8):
        for source in range(8):
            bits = bin(target ^ source).count("1")
            want = (4.0, 0.0, -1.0, -1.0)[bits] * unit
            assert abs(float(table[target, source]) - want) < 1e-12
    return unit


UNIT = kernel_scale()


def lowered(value):
    return value.astype(jnp.bfloat16).astype(jnp.float32)


def tile_of(tile):
    return slice(tile * LANES, (tile + 1) * LANES)


def lanes_of(value):
    return lax.broadcasted_iota(jnp.int32, value.shape, 1)


def turn(value, amount):
    amount %= LANES
    return pltpu.roll(value, amount, 1) if amount else value


def shifted(tiles, step, beyond=None):
    count = len(tiles)
    turned = [turn(t, -step) for t in tiles]
    past = turn(beyond, -step) if beyond is not None else turned[0 if step > 0 else -1]
    lane = lanes_of(tiles[0])
    if step > 0:
        return [jnp.where(lane < LANES - 1, turned[i], turned[i + 1] if i + 1 < count else past) for i in range(count)]
    return [jnp.where(lane > 0, turned[i], turned[i - 1] if i else past) for i in range(count)]


def terms(low, sides, tile, x, y, wx, wy):
    above, below, both = sides
    around = {(i, j): low(x + i, y + j, tile) for i in (-1, 0, 1) for j in (-1, 0, 1)}
    centre = 4.0 * around[0, 0]
    total = None
    for i in (-1, 1):
        for j in (-1, 1):
            ex, ey = wx + (i - 1) // 2, wy + (j - 1) // 2
            others = around[i, 0] + around[0, j] + around[i, j]
            new = (
                both(ex, ey, tile) * (centre - around[i, j]),
                below(ex, ey, tile) * others,
                above(ex, ey, tile) * others,
            )
            total = new if total is None else tuple(a + b for a, b in zip(total, new))
    return total


def operator(field, low, sides, count, x, y, wx, wy):
    plane, down, up = zip(*[terms(low, sides, t, x, y, wx, wy) for t in range(count)])
    from_above, from_below = shifted(down, 1), shifted(up, -1)
    return [SIGMA * field(t) + (plane[t] - from_above[t] - from_below[t]) for t in range(count)]


def split_terms(value, count):
    parts = []
    for n in range(count):
        part = value.astype(jnp.bfloat16)
        parts.append(part)
        if n + 1 < count:
            value = value - part.astype(jnp.float32)
    return jnp.concatenate(parts, axis=0)


def rows_of(refs, flags_ref, tile, x, y, first, count):
    before_ref, mid_ref, after_ref, ext_x = refs
    if y < 2:
        ref, wide, at, flag = before_ref, 2, y, 0
    elif y < 6:
        ref, wide, at, flag = mid_ref, 4, y - 2, None
    else:
        ref, wide, at, flag = after_ref, 2, y - 6, 1
    stride = ext_x * wide
    start = tile * (ref.shape[0] // 2) + first * stride + x * wide + at
    value = ref[pl.ds(start, count, stride=stride), :] if count > 1 else ref[start : start + 1, :]
    if flag is not None:
        value = jnp.where(flags_ref[flag : flag + 1, :] > 0.0, value, 0.0)
    return value


def front_kernel(moduli_ref, loads_ref, material_ref, own_ref, levels_ref):
    for t in range(2):
        own_ref[t, :COLS] = loads_ref[:, :, :, tile_of(t)]
        own_ref[t, COLS] = (material_ref[:, :, tile_of(t)] + 1).astype(jnp.float32)
    for level in range(moduli_ref.shape[0]):
        levels_ref[level : level + 1, :] = jnp.full((1, LANES), moduli_ref[level], jnp.float32)


def pack_kernel(flags_ref, before_ref, mid_ref, after_ref, lo_ref, hi_ref, ext_x, ext_y):
    refs = (before_ref, mid_ref, after_ref, ext_x)
    for tile, out_ref in ((0, lo_ref), (1, hi_ref)):
        offset = 2 * tile
        lane = lax.broadcasted_iota(jnp.int32, (COLS, LANES), 1)
        packed = jnp.zeros((COLS, LANES), jnp.float32)
        ids = [jnp.zeros((1, LANES), jnp.float32)] * ext_y
        for x in range(ext_x):
            for y in range(ext_y):
                node = x * ext_y + y
                value = rows_of(refs, flags_ref, tile, x, y, 0, COLS)
                packed = jnp.where(lane // 2 == node, turn(value, 2 * node + offset), packed)
                value = rows_of(refs, flags_ref, tile, x, y, COLS, 1)
                ids[y] = jnp.where(lane[:1] // 2 == x, turn(value, 2 * x + offset), ids[y])
        out_ref[:COLS, :] = packed
        for y in range(ext_y):
            out_ref[COLS + y : COLS + y + 1, :] = ids[y]


def modulus_of(levels_ref, ids):
    modulus = jnp.zeros_like(ids)
    for level in range(levels_ref.shape[0]):
        modulus = jnp.where(ids == level + 1.0, levels_ref[level : level + 1, :], modulus)
    return modulus


def element_weights(e_ref, above_ref, below_ref, both_ref, count):
    ext_x, ext_y = e_ref.shape[:2]
    for ex in range(ext_x - 1):
        flat = []
        for t in range(count):
            both_x = e_ref[ex, :, tile_of(t)] + e_ref[ex + 1, :, tile_of(t)]
            flat.append(both_x + pltpu.roll(both_x, ext_y - 1, 0))
        ahead = shifted(flat, 1)
        weights = [(0.125 * UNIT) * (flat[t] + ahead[t]) for t in range(count)]
        behind = shifted(weights, -1)
        for t in range(count):
            above_ref[ex, :, tile_of(t)] = weights[t]
            below_ref[ex, :, tile_of(t)] = behind[t]
            both_ref[ex, :, tile_of(t)] = weights[t] + behind[t]


def sides_of(*refs):
    return tuple(lambda ex, ey, t, ref=ref: ref[ex, ey : ey + 1, tile_of(t)] for ref in refs)


def first_image(v_ref, low_ref, e_ref, sides, q_ref, qlow_ref, count):
    ext_x, ext_y = low_ref.shape[0], low_ref.shape[1]
    for x in range(1, ext_x - 1):
        for y in range(1, ext_y - 1):
            image = operator(
                lambda t: v_ref[x - 1, y - 1, :, tile_of(t)],
                lambda i, j, t: low_ref[i, j, :, tile_of(t)],
                sides, count, x, y, x, y,
            )
            for t in range(count):
                value = jnp.where(e_ref[x, y : y + 1, tile_of(t)] > 0.0, image[t], 0.0)
                q_ref[x - 1, y - 1, :, tile_of(t)] = value
                qlow_ref[x - 1, y - 1, :, tile_of(t)] = lowered(value)


def gram_terms(v_ref, q_ref, qlow_ref, sides, count, keep, left_ref, right_ref):
    own_x, own_y = v_ref.shape[0], v_ref.shape[1]
    node = 0
    for x in range(1, own_x - 1):
        for y in range(1, own_y - 1):
            image = operator(
                lambda t: q_ref[x, y, :, tile_of(t)],
                lambda i, j, t: qlow_ref[i, j, :, tile_of(t)],
                sides, count, x, y, x + 1, y + 1,
            )
            for t in range(count):
                b, q = v_ref[x, y, :, tile_of(t)], q_ref[x, y, :, tile_of(t)]
                at = tile_of(node * count + t)
                left = jnp.concatenate([b, q], axis=0)
                left = jnp.where(keep(lanes_of(left), t), left, 0.0)
                left_ref[:, at] = split_terms(left, 3)
                right = jnp.concatenate([b, q, image[t], jnp.zeros_like(b)], axis=0)
                right_ref[:, at] = split_terms(right, 3)
            node += 1
    product = lax.dot_general(
        left_ref[...], right_ref[...], (((1,), (1,)), ((), ())), preferred_element_type=jnp.float32
    )
    half = LANES // 2
    third = jnp.concatenate([product[:, LANES:], jnp.zeros((6 * COLS, half), jnp.float32)], axis=1)
    folded = product[:, :LANES] + turn(product[:, :LANES], half) + third
    return sum(folded[2 * COLS * n : 2 * COLS * (n + 1)] for n in range(3))


def main_kernel(
    levels_ref, flags_ref, before_ref, mid_ref, after_ref,
    v_ref, q_ref, above_ref, below_ref, both_ref, total_ref, ve_ref, ie_ref,
    low_ref, qlow_ref, e_ref, left_ref, right_ref,
):
    ext_x, ext_y = low_ref.shape[0], low_ref.shape[1]
    refs = (before_ref, mid_ref, after_ref, ext_x)
    for x in range(ext_x):
        for y in range(ext_y):
            tiles = [rows_of(refs, flags_ref, t, x, y, COLS, 1) for t in range(2)]
            lane = lanes_of(tiles[0])
            edge = jnp.where(lane < EDGE, tiles[0], jnp.where(lane < 2 * EDGE, turn(tiles[1], 2 * EDGE), 0.0))
            ie_ref[x, y : y + 1, :] = edge
            for t in range(2):
                e_ref[x, y : y + 1, tile_of(t)] = tiles[t]
        for t in range(2):
            e_ref[x, :, tile_of(t)] = modulus_of(levels_ref, e_ref[x, :, tile_of(t)])
    element_weights(e_ref, above_ref, below_ref, both_ref, 2)
    for x in range(ext_x):
        for y in range(ext_y):
            tiles = [rows_of(refs, flags_ref, t, x, y, 0, COLS) for t in range(2)]
            lane = lanes_of(tiles[0])
            edge = jnp.where(lane < EDGE, tiles[0], jnp.where(lane < 2 * EDGE, turn(tiles[1], 2 * EDGE), 0.0))
            ve_ref[x, y] = edge
            for t in range(2):
                low_ref[x, y, :, tile_of(t)] = lowered(tiles[t])
                if 0 < x < ext_x - 1 and 0 < y < ext_y - 1:
                    v_ref[x - 1, y - 1, :, tile_of(t)] = tiles[t]
    sides = sides_of(above_ref, below_ref, both_ref)
    first_image(v_ref, low_ref, e_ref, sides, q_ref, qlow_ref, 2)
    total_ref[...] = gram_terms(
        v_ref, q_ref, qlow_ref, sides, 2,
        lambda lane, t: lane >= 2 if t == 0 else lane < LANES - 2,
        left_ref, right_ref,
    )


def edge_kernel(
    levels_ref, total_ref, ve_ref, ie_ref, before_ref, after_ref,
    v_ref, q_ref, above_ref, below_ref, both_ref, g_ref,
    low_ref, qlow_ref, e_ref, left_ref, right_ref,
):
    ext_x, ext_y = low_ref.shape[0], low_ref.shape[1]

    def with_ends(own, before, after, index):
        lane = lanes_of(own)
        follows, comes = turn(after, LANES // 2 - 2 * index), turn(before, LANES - 2 - 2 * index)
        value = jnp.where(lane >= LANES - 2, comes, own)
        return jnp.where((lane >= LANES // 2) & (lane < LANES // 2 + 2), follows, value)

    for x in range(ext_x):
        ids = with_ends(ie_ref[x], before_ref[COLS : COLS + ext_y, :], after_ref[COLS : COLS + ext_y, :], x)
        e_ref[x] = modulus_of(levels_ref, ids)
    element_weights(e_ref, above_ref, below_ref, both_ref, 1)
    before, after = before_ref[:COLS, :], after_ref[:COLS, :]
    for x in range(ext_x):
        for y in range(ext_y):
            value = with_ends(ve_ref[x, y], before, after, x * ext_y + y)
            low_ref[x, y] = lowered(value)
            if 0 < x < ext_x - 1 and 0 < y < ext_y - 1:
                v_ref[x - 1, y - 1] = value
    sides = sides_of(above_ref, below_ref, both_ref)
    first_image(v_ref, low_ref, e_ref, sides, q_ref, qlow_ref, 1)
    total = gram_terms(
        v_ref, q_ref, qlow_ref, sides, 1,
        lambda lane, t: (lane < 2) | ((lane >= 2 * EDGE - 2) & (lane < 2 * EDGE)),
        left_ref, right_ref,
    )
    g_ref[...] = pack_moments(total_ref[...] + total)


def pack_moments(total):
    first, second = total[:COLS], total[COLS:]
    row = lax.broadcasted_iota(jnp.int32, (COLS, LANES), 0)
    lane = lax.broadcasted_iota(jnp.int32, (COLS, LANES), 1)
    col = lane % COLS
    upper = jnp.where(lane < COLS, first, second)
    lower = jnp.where(
        lane < COLS,
        0.5 * (pltpu.roll(first, LANES - COLS, 1) + second),
        pltpu.roll(second, LANES - COLS, 1),
    )
    valid = lane < 2 * COLS
    square = jnp.where(valid, jnp.where(row <= col, upper, lower), 0.0)
    diagonal = jnp.sum(jnp.where(valid & (row == col), lower, 0.0), axis=0, keepdims=True)
    out = []
    for half in range(2):
        out.append(square[8 * half : 8 * half + 8])
    spread_rows = jnp.zeros((8, LANES), jnp.float32)
    sub8 = lax.broadcasted_iota(jnp.int32, (8, LANES), 0)
    lane8 = lax.broadcasted_iota(jnp.int32, (8, LANES), 1)
    for quarter in range(4):
        piece = out[quarter // 2]
        if quarter % 2:
            piece = pltpu.roll(piece, 4, 0)
        if quarter:
            piece = pltpu.roll(piece, 2 * COLS * quarter, 1)
        here = (sub8 < 4) & (lane8 // (2 * COLS) == quarter)
        spread_rows = jnp.where(here, piece, spread_rows)
    return jnp.where(sub8 == 4, diagonal, spread_rows)


def unpack_moments(packed):
    sub8 = lax.broadcasted_iota(jnp.int32, (8, LANES), 0)
    halves = []
    for half in range(2):
        a, b = 2 * half, 2 * half + 1
        top = pltpu.roll(packed, LANES - 2 * COLS * a, 1) if a else packed
        bottom = pltpu.roll(pltpu.roll(packed, LANES - 2 * COLS * b, 1), 4, 0)
        halves.append(jnp.where(sub8 < 4, top, bottom))
    square = jnp.concatenate(halves, axis=0)
    row = lax.broadcasted_iota(jnp.int32, (COLS, COLS), 0)
    col = lax.broadcasted_iota(jnp.int32, (COLS, COLS), 1)
    moments = []
    for pair in range(2):
        turned = pltpu.roll(square, LANES - COLS, 1) if pair else square
        mixed = turned[:, :COLS]
        diagonal = (pltpu.roll(packed, LANES - COLS, 1) if pair else packed)[4:5, :COLS]
        flipped = mixed.T
        moments.append(jnp.where(row <= col, mixed, flipped))
        lower = jnp.where(row == col, diagonal, jnp.where(row > col, mixed, flipped))
        moments.append(lower)
    return moments


def dot(left, right, dims=((1,), (0,))):
    return lax.dot_general(left, right, (dims, ((), ())), precision=HIGH, preferred_element_type=jnp.float32)


def sweeps(matrix):
    size = COLS
    sub = lax.broadcasted_iota(jnp.int32, (size, LANES), 0)
    rows = [jnp.broadcast_to(matrix[:, i : i + 1], (size, LANES)) for i in range(size)]
    for k in range(size):
        scale = 1.0 / rows[k][k : k + 1, :]
        pivot_row = rows[k] * scale
        for i in range(size):
            if i != k:
                factor = rows[i][k : k + 1, :]
                moved = rows[i] - factor * pivot_row
                rows[i] = jnp.where(sub == k, factor * scale, moved)
        rows[k] = jnp.where(sub == k, -scale, pivot_row)
        yield None
    lane = lax.broadcasted_iota(jnp.int32, (size, LANES), 1)
    out = jnp.zeros((size, LANES), jnp.float32)
    for i in range(size):
        out = jnp.where(lane == i, -rows[i], out)
    yield out[:, :size]


def mixer(coeffs, count):
    flipped = split_terms(coeffs.T, count)
    return jnp.concatenate([flipped] * count, axis=1)


def mixed(left, block, count):
    out = jnp.dot(left, split_terms(block, count), preferred_element_type=jnp.float32)
    size = out.shape[0] // count
    return sum(out[size * n : size * (n + 1)] for n in range(count))


def finish_kernel(
    g_ref, v_ref, q_ref, above_ref, below_ref, both_ref,
    ve_ref, qe_ref, abovee_ref, belowe_ref, bothe_ref,
    sol_ref, res_ref, d_ref, dlow_ref, w0_ref, w1_ref, w2_ref,
):
    own_x, own_y = v_ref.shape[0], v_ref.shape[1]
    m0, m1, m2, m3 = unpack_moments(g_ref[...])
    first = ((0,), (0,))
    *_, inv = sweeps(m1)
    alpha = dot(inv, m0)
    m2a = dot(m2, alpha)
    mix = dot(inv, m2a)
    left = mixer(jnp.concatenate([mix, -alpha], axis=0), 3)
    updated = dot(alpha, m2a, first) - m0
    curved = dot(alpha, dot(m3, alpha), first) - dot(m2a, mix, first)
    steps = sweeps(0.5 * (curved + curved.T))
    inv = None
    for x in range(own_x):
        for y in range(own_y):
            q0, q1, qe = q_ref[x, y, :, :LANES], q_ref[x, y, :, LANES:], qe_ref[x, y]
            lane = lanes_of(qe)
            q0 = jnp.where(lane == 0, qe, q0)
            q1 = jnp.where(lane == LANES - 1, turn(qe, LANES // 2), q1)
            block = jnp.concatenate(
                [
                    jnp.concatenate([v_ref[x, y], ve_ref[x, y]], axis=1),
                    jnp.concatenate([q0, q1, qe], axis=1),
                ],
                axis=0,
            )
            value = mixed(left, block, 3)
            d_ref[x, y] = value
            dlow_ref[x, y] = lowered(value)
            if inv is None:
                inv = next(steps)
    gamma = dot(inv, updated)
    edge, main = (abovee_ref, belowe_ref, bothe_ref), (above_ref, below_ref, both_ref)
    whole = (w0_ref, w1_ref, w2_ref)
    for end_ref, main_ref, whole_ref in zip(edge, main, whole):
        for ex in range(1, own_x):
            end = end_ref[ex]
            lane = lanes_of(end)
            whole_ref[ex, :, :LANES] = jnp.where(lane == 0, end, main_ref[ex, :, :LANES])
            end = turn(end, LANES // 2)
            whole_ref[ex, :, LANES:] = jnp.where(lane == LANES - 1, end, main_ref[ex, :, LANES:])
    main, edge = sides_of(*whole), sides_of(*edge)
    zero = jnp.zeros((COLS, COLS), jnp.float32)
    last = mixer(
        jnp.concatenate(
            [
                jnp.concatenate([alpha, gamma, zero, zero], axis=0),
                jnp.concatenate([zero, zero, -alpha, -gamma], axis=0),
            ],
            axis=1,
        ),
        2,
    )
    for x in range(1, own_x - 1):
        for y in range(1, own_y - 1):
            low = lambda i, j, t: dlow_ref[i, j, :, tile_of(t)]
            at = (x, y, x + 1, y + 1)
            plane, down, up = zip(*[terms(low, main, t, *at) for t in range(2)])
            ends = terms(lambda i, j, t: dlow_ref[i, j, :, tile_of(2)], edge, 0, *at)
            from_above = shifted(down, 1, turn(ends[1], LANES // 2))
            from_below = shifted(up, -1, ends[2])
            image = [
                SIGMA * d_ref[x, y, :, tile_of(t)] + (plane[t] - from_above[t] - from_below[t])
                for t in range(2)
            ]
            q0, q1, qe = q_ref[x, y, :, :LANES], q_ref[x, y, :, LANES:], qe_ref[x, y]
            lane = lanes_of(qe)
            q0 = jnp.where(lane == 0, qe, q0)
            q1 = jnp.where(lane == LANES - 1, turn(qe, LANES // 2), q1)
            b = v_ref[x, y]
            block = jnp.concatenate(
                [
                    b,
                    d_ref[x, y, :, : 2 * LANES],
                    jnp.concatenate([q0, q1], axis=1),
                    jnp.concatenate(image, axis=1),
                ],
                axis=0,
            )
            out = mixed(last, block, 2)
            sol_ref[:, x - 1, y - 1, :] = out[:COLS]
            res_ref[:, x - 1, y - 1, :] = b + out[COLS:]


def both_ways(axis, to_next, to_last, around=False):
    count = lax.axis_size(axis)
    steps = range(count) if around else range(count - 1)
    before = lax.ppermute(to_next, axis, [(i, (i + 1) % count) for i in steps])
    after = lax.ppermute(to_last, axis, [((i + 1) % count, i) for i in steps])
    return before, after


def spread(value, axes, root):
    count = lax.axis_size(axes)
    copies = jnp.broadcast_to(value[None], (count, *value.shape))
    group = [(root + i) % count for i in range(count)]
    return jnp.sum(lax.all_to_all(copies, axes, 0, 0, axis_index_groups=[group]), axis=0)


def near(value):
    return pltpu.with_memory_space_constraint(value, pltpu.VMEM)


def on_device(loads, moduli, material):
    f32, bf16, wide = jnp.float32, jnp.bfloat16, 2 * LANES
    own_x, own_y = material.shape[:2]
    ext_x, ext_y = own_x + 4, own_y + 4
    own, levels = pl.pallas_call(
        front_kernel,
        out_shape=(
            pltpu.VMEM((2, COLS + 1, own_x, own_y, LANES), f32),
            pltpu.VMEM((moduli.shape[0], LANES), f32),
        ),
        in_specs=[
            pl.BlockSpec(memory_space=pltpu.SMEM),
            pl.BlockSpec(memory_space=pltpu.VMEM),
            pl.BlockSpec(memory_space=pltpu.VMEM),
        ],
        name="front",
    )(moduli, loads, material)
    place = lax.axis_index(GY)
    row = lax.broadcasted_iota(jnp.int32, (8, LANES), 0)
    flags = jnp.where(row == 0, place > 0, place < lax.axis_size(GY) - 1).astype(f32)
    before, after = both_ways("gx", own, own)
    mid = jnp.concatenate([before, own, after], axis=2)
    before, after = both_ways(GY, mid[:, :, :, 2:], mid[:, :, :, :2], around=True)
    flat = [near(part.reshape(-1, LANES)) for part in (before, mid, after)]
    ends = pltpu.VMEM((COLS + 8, LANES), f32)
    first, last = pl.pallas_call(
        functools.partial(pack_kernel, ext_x=ext_x, ext_y=ext_y), out_shape=(ends, ends), name="pack"
    )(near(flags), *flat)
    before, after = both_ways("gz", last, first)
    nodes = own_x * own_y

    def weights(size):
        return (pltpu.VMEM((ext_x - 1, ext_y, size), f32),) * 3

    def fields(size):
        return (pltpu.VMEM((ext_x - 2, ext_y - 2, COLS, size), f32),) * 2

    def scratch(size):
        return [
            pltpu.VMEM((ext_x, ext_y, COLS, size), f32),
            pltpu.VMEM((ext_x - 2, ext_y - 2, COLS, size), f32),
            pltpu.VMEM((ext_x, ext_y, size), f32),
            pltpu.VMEM((6 * COLS, nodes * size), bf16),
            pltpu.VMEM((12 * COLS, nodes * size), bf16),
        ]

    *main, total, edge, ids = pl.pallas_call(
        main_kernel,
        out_shape=(
            *fields(wide),
            *weights(wide),
            pltpu.VMEM((2 * COLS, LANES), f32),
            pltpu.VMEM((ext_x, ext_y, COLS, LANES), f32),
            pltpu.VMEM((ext_x, ext_y, LANES), f32),
        ),
        scratch_shapes=scratch(wide),
        name="main",
    )(near(levels), near(flags), *flat)
    *edges, moments = pl.pallas_call(
        edge_kernel,
        out_shape=(*fields(LANES), *weights(LANES), pltpu.VMEM((8, LANES), f32)),
        scratch_shapes=scratch(LANES),
        name="edge",
    )(*[near(value) for value in (levels, total, edge, ids, before, after)])
    rows = 5
    length, chips = lax.axis_size("gz"), lax.axis_size("gy_0")
    moments = spread(moments[:rows].reshape(rows, 1, LANES), "gz", 9 * length // 16)
    middle = (lax.axis_size("gx") // 2 * chips + chips // 2) * 2 + 1
    moments = spread(moments, PLANE, middle).reshape(rows, LANES)
    moments = jnp.concatenate([moments, jnp.zeros((8 - rows, LANES), f32)], axis=0)
    out = jax.ShapeDtypeStruct(loads.shape, f32)
    return pl.pallas_call(
        finish_kernel,
        out_shape=(out, out),
        scratch_shapes=[pltpu.VMEM((ext_x - 2, ext_y - 2, COLS, 3 * LANES), f32)] * 2
        + [pltpu.VMEM((ext_x - 1, ext_y, wide), f32)] * 3,
        name="finish",
    )(*[near(value) for value in (moments, *main, *edges)])


def solution(mesh):
    wide, long = mesh.shape["gy"] // 2, mesh.shape["gz"]
    split = Mesh(mesh.devices.reshape(mesh.shape["gx"], wide, 2, long), ("gx", "gy_0", "gy_1", "gz"))
    spec = P(None, "gx", GY, "gz")
    return jax.shard_map(
        on_device,
        mesh=split,
        in_specs=(spec, P(), P("gx", GY, "gz")),
        out_specs=(spec, spec),
        check_vma=False,
    )
```

```python
import functools

import jax
import jax.numpy as jnp
import numpy as np
from jax import lax
from jax.experimental import pallas as pl
from jax.experimental.pallas import tpu as pltpu
from jax.sharding import Mesh
from jax.sharding import PartitionSpec as P

PLANE = ("gx", "gy_0", "gy_1")
GY = ("gy_0", "gy_1")
SIGMA = 0.25
COLS = 16
LANES = 128
EDGE = LANES // 4
HIGH = lax.Precision.HIGHEST


def stiffness_table():
    line_mass = np.array([[1.0 / 3.0, 1.0 / 6.0], [1.0 / 6.0, 1.0 / 3.0]])
    line_stiff = np.array([[1.0, -1.0], [-1.0, 1.0]])
    table = np.zeros((8, 8))
    for target in range(8):
        for source in range(8):
            target_bits = [target >> 2 & 1, target >> 1 & 1, target & 1]
            source_bits = [source >> 2 & 1, source >> 1 & 1, source & 1]
            total = 0.0
            for stiff_dim in range(3):
                factor = 1.0
                for other in range(3):
                    if other == stiff_dim:
                        factor = factor * line_stiff[target_bits[other], source_bits[other]]
                    else:
                        factor = factor * line_mass[target_bits[other], source_bits[other]]
                total = total + factor
            table[target, source] = total
    return table


def kernel_scale():
    table = np.asarray(jnp.asarray(stiffness_table(), jnp.bfloat16).astype(jnp.float32))
    unit = -float(table[0, 7])
    for target in range(8):
        for source in range(8):
            bits = bin(target ^ source).count("1")
            want = (4.0, 0.0, -1.0, -1.0)[bits] * unit
            assert abs(float(table[target, source]) - want) < 1e-12
    return unit


UNIT = kernel_scale()


def lowered(value):
    return value.astype(jnp.bfloat16).astype(jnp.float32)


def tile_of(tile):
    return slice(tile * LANES, (tile + 1) * LANES)


def lanes_of(value):
    return lax.broadcasted_iota(jnp.int32, value.shape, 1)


def turn(value, amount):
    amount %= LANES
    return pltpu.roll(value, amount, 1) if amount else value


def shifted(tiles, step, beyond=None):
    count = len(tiles)
    turned = [turn(t, -step) for t in tiles]
    past = turn(beyond, -step) if beyond is not None else turned[0 if step > 0 else -1]
    lane = lanes_of(tiles[0])
    if step > 0:
        return [jnp.where(lane < LANES - 1, turned[i], turned[i + 1] if i + 1 < count else past) for i in range(count)]
    return [jnp.where(lane > 0, turned[i], turned[i - 1] if i else past) for i in range(count)]


def terms(low, sides, tile, x, y, wx, wy):
    above, below, both = sides
    around = {(i, j): low(x + i, y + j, tile) for i in (-1, 0, 1) for j in (-1, 0, 1)}
    total = None
    for i in (-1, 1):
        for j in (-1, 1):
            ex, ey = wx + (i - 1) // 2, wy + (j - 1) // 2
            others = around[i, 0] + around[0, j] + around[i, j]
            new = (
                both(ex, ey, tile) * around[i, j],
                below(ex, ey, tile) * others,
                above(ex, ey, tile) * others,
            )
            total = new if total is None else tuple(a + b for a, b in zip(total, new))
    rim = [both(wx + i, wy + j, tile) for i in (-1, 0) for j in (-1, 0)]
    centre = (4.0 * ((rim[0] + rim[1]) + (rim[2] + rim[3]))) * around[0, 0]
    return centre - total[0], total[1], total[2]


def operator(field, low, sides, count, x, y, wx, wy):
    plane, down, up = zip(*[terms(low, sides, t, x, y, wx, wy) for t in range(count)])
    from_above, from_below = shifted(down, 1), shifted(up, -1)
    return [SIGMA * field(t) + (plane[t] - from_above[t] - from_below[t]) for t in range(count)]


def split_terms(value, count):
    parts = []
    for n in range(count):
        part = value.astype(jnp.bfloat16)
        parts.append(part)
        if n + 1 < count:
            value = value - part.astype(jnp.float32)
    return jnp.concatenate(parts, axis=0)


def rows_of(refs, flags_ref, tile, x, y, first, count):
    before_ref, mid_ref, after_ref, ext_x = refs
    if y < 2:
        ref, wide, at, flag = before_ref, 2, y, 0
    elif y < 6:
        ref, wide, at, flag = mid_ref, 4, y - 2, None
    else:
        ref, wide, at, flag = after_ref, 2, y - 6, 1
    stride = ext_x * wide
    start = tile * (ref.shape[0] // 2) + first * stride + x * wide + at
    value = ref[pl.ds(start, count, stride=stride), :] if count > 1 else ref[start : start + 1, :]
    if flag is not None:
        value = jnp.where(flags_ref[flag : flag + 1, :] > 0.0, value, 0.0)
    return value


def front_kernel(moduli_ref, loads_ref, material_ref, own_ref, levels_ref):
    for t in range(2):
        own_ref[t, :COLS] = loads_ref[:, :, :, tile_of(t)]
        own_ref[t, COLS] = (material_ref[:, :, tile_of(t)] + 1).astype(jnp.float32)
    for level in range(moduli_ref.shape[0]):
        levels_ref[level : level + 1, :] = jnp.full((1, LANES), moduli_ref[level], jnp.float32)


def pack_kernel(flags_ref, before_ref, mid_ref, after_ref, lo_ref, hi_ref, ext_x, ext_y):
    refs = (before_ref, mid_ref, after_ref, ext_x)
    for tile, out_ref in ((0, lo_ref), (1, hi_ref)):
        offset = 2 * tile
        lane = lax.broadcasted_iota(jnp.int32, (COLS, LANES), 1)
        packed = jnp.zeros((COLS, LANES), jnp.float32)
        ids = [jnp.zeros((1, LANES), jnp.float32)] * ext_y
        for x in range(ext_x):
            for y in range(ext_y):
                node = x * ext_y + y
                value = rows_of(refs, flags_ref, tile, x, y, 0, COLS)
                packed = jnp.where(lane // 2 == node, turn(value, 2 * node + offset), packed)
                value = rows_of(refs, flags_ref, tile, x, y, COLS, 1)
                ids[y] = jnp.where(lane[:1] // 2 == x, turn(value, 2 * x + offset), ids[y])
        out_ref[:COLS, :] = packed
        for y in range(ext_y):
            out_ref[COLS + y : COLS + y + 1, :] = ids[y]


def modulus_of(levels_ref, ids):
    modulus = jnp.zeros_like(ids)
    for level in range(levels_ref.shape[0]):
        modulus = jnp.where(ids == level + 1.0, levels_ref[level : level + 1, :], modulus)
    return modulus


def element_weights(e_ref, above_ref, below_ref, both_ref, count):
    ext_x, ext_y = e_ref.shape[:2]
    for ex in range(ext_x - 1):
        flat = []
        for t in range(count):
            both_x = e_ref[ex, :, tile_of(t)] + e_ref[ex + 1, :, tile_of(t)]
            flat.append(both_x + pltpu.roll(both_x, ext_y - 1, 0))
        ahead = shifted(flat, 1)
        weights = [(0.125 * UNIT) * (flat[t] + ahead[t]) for t in range(count)]
        behind = shifted(weights, -1)
        for t in range(count):
            above_ref[ex, :, tile_of(t)] = weights[t]
            below_ref[ex, :, tile_of(t)] = behind[t]
            both_ref[ex, :, tile_of(t)] = weights[t] + behind[t]


def sides_of(*refs):
    return tuple(lambda ex, ey, t, ref=ref: ref[ex, ey : ey + 1, tile_of(t)] for ref in refs)


def first_image(v_ref, low_ref, e_ref, sides, q_ref, qlow_ref, count):
    ext_x, ext_y = low_ref.shape[0], low_ref.shape[1]
    for x in range(1, ext_x - 1):
        for y in range(1, ext_y - 1):
            image = operator(
                lambda t: v_ref[x - 1, y - 1, :, tile_of(t)],
                lambda i, j, t: low_ref[i, j, :, tile_of(t)],
                sides, count, x, y, x, y,
            )
            for t in range(count):
                value = image[t]
                if count == 1 or x in (1, ext_x - 2) or y in (1, ext_y - 2):
                    value = jnp.where(e_ref[x, y : y + 1, tile_of(t)] > 0.0, value, 0.0)
                q_ref[x - 1, y - 1, :, tile_of(t)] = value
                qlow_ref[x - 1, y - 1, :, tile_of(t)] = lowered(value)


def own_nodes(v_ref, q_ref, qlow_ref, sides, count):
    own_x, own_y = v_ref.shape[0], v_ref.shape[1]
    for x in range(1, own_x - 1):
        for y in range(1, own_y - 1):
            image = operator(
                lambda t: q_ref[x, y, :, tile_of(t)],
                lambda i, j, t: qlow_ref[i, j, :, tile_of(t)],
                sides, count, x, y, x + 1, y + 1,
            )
            for t in range(count):
                yield t, v_ref[x, y, :, tile_of(t)], q_ref[x, y, :, tile_of(t)], image[t]


def left_terms(right):
    return jnp.concatenate([right[3 * COLS * n : 3 * COLS * n + 2 * COLS] for n in range(3)], axis=0)


def products(left, right):
    product = lax.dot_general(left, right, (((1,), (1,)), ((), ())), preferred_element_type=jnp.float32)
    rows = sum(product[2 * COLS * n : 2 * COLS * (n + 1)] for n in range(3))
    lane = lax.broadcasted_iota(jnp.int32, (2 * COLS, LANES), 1)
    first = rows[:, :LANES]
    rest = jnp.concatenate([rows[:, LANES:], jnp.zeros((2 * COLS, 2 * LANES - 9 * COLS), jnp.float32)], axis=1)
    third = jnp.where(lane < 2 * COLS, turn(first, -6 * COLS), turn(rest, 2 * COLS))
    return first + turn(first, -3 * COLS) + third


def main_kernel(
    levels_ref, flags_ref, before_ref, mid_ref, after_ref,
    v_ref, q_ref, above_ref, below_ref, both_ref, total_ref, ve_ref, ie_ref,
    low_ref, qlow_ref, e_ref, left_ref, right_ref,
):
    ext_x, ext_y = low_ref.shape[0], low_ref.shape[1]
    refs = (before_ref, mid_ref, after_ref, ext_x)
    for x in range(ext_x):
        for y in range(ext_y):
            tiles = [rows_of(refs, flags_ref, t, x, y, COLS, 1) for t in range(2)]
            lane = lanes_of(tiles[0])
            edge = jnp.where(lane < EDGE, tiles[0], jnp.where(lane < 2 * EDGE, turn(tiles[1], 2 * EDGE), 0.0))
            ie_ref[x, y : y + 1, :] = edge
            for t in range(2):
                e_ref[x, y : y + 1, tile_of(t)] = tiles[t]
        for t in range(2):
            e_ref[x, :, tile_of(t)] = modulus_of(levels_ref, e_ref[x, :, tile_of(t)])
    element_weights(e_ref, above_ref, below_ref, both_ref, 2)
    for x in range(ext_x):
        for y in range(ext_y):
            tiles = [rows_of(refs, flags_ref, t, x, y, 0, COLS) for t in range(2)]
            lane = lanes_of(tiles[0])
            edge = jnp.where(lane < EDGE, tiles[0], jnp.where(lane < 2 * EDGE, turn(tiles[1], 2 * EDGE), 0.0))
            ve_ref[x, y] = edge
            for t in range(2):
                low_ref[x, y, :, tile_of(t)] = lowered(tiles[t])
                if 0 < x < ext_x - 1 and 0 < y < ext_y - 1:
                    v_ref[x - 1, y - 1, :, tile_of(t)] = tiles[t]
    sides = sides_of(above_ref, below_ref, both_ref)
    first_image(v_ref, low_ref, e_ref, sides, q_ref, qlow_ref, 2)
    for n, (t, b, q, w) in enumerate(own_nodes(v_ref, q_ref, qlow_ref, sides, 2)):
        right = split_terms(jnp.concatenate([b, q, w], axis=0), 3)
        left = left_terms(right)
        here = lanes_of(left) >= 2 if t == 0 else lanes_of(left) < LANES - 2
        left_ref[:, tile_of(n)] = jnp.where(here, left, jnp.zeros_like(left))
        right_ref[:, tile_of(n)] = right
    total_ref[...] = products(left_ref[...], right_ref[...])


def edge_kernel(
    levels_ref, total_ref, ve_ref, ie_ref, before_ref, after_ref,
    v_ref, q_ref, above_ref, below_ref, both_ref, g_ref,
    low_ref, qlow_ref, e_ref,
):
    ext_x, ext_y = low_ref.shape[0], low_ref.shape[1]

    def with_ends(own, before, after, index):
        lane = lanes_of(own)
        follows, comes = turn(after, LANES // 2 - 2 * index), turn(before, LANES - 2 - 2 * index)
        value = jnp.where(lane >= LANES - 2, comes, own)
        return jnp.where((lane >= LANES // 2) & (lane < LANES // 2 + 2), follows, value)

    for x in range(ext_x):
        ids = with_ends(ie_ref[x], before_ref[COLS : COLS + ext_y, :], after_ref[COLS : COLS + ext_y, :], x)
        e_ref[x] = modulus_of(levels_ref, ids)
    element_weights(e_ref, above_ref, below_ref, both_ref, 1)
    before, after = before_ref[:COLS, :], after_ref[:COLS, :]
    for x in range(ext_x):
        for y in range(ext_y):
            value = with_ends(ve_ref[x, y], before, after, x * ext_y + y)
            low_ref[x, y] = lowered(value)
            if 0 < x < ext_x - 1 and 0 < y < ext_y - 1:
                v_ref[x - 1, y - 1] = value
    sides = sides_of(above_ref, below_ref, both_ref)
    first_image(v_ref, low_ref, e_ref, sides, q_ref, qlow_ref, 1)
    right = jnp.zeros((3 * COLS, LANES), jnp.float32)
    for n, (_, b, q, w) in enumerate(own_nodes(v_ref, q_ref, qlow_ref, sides, 1)):
        three = jnp.concatenate([b, q, w], axis=0)
        at = lanes_of(three) - 2 * n
        here = ((at >= 0) & (at < 2)) | ((at >= 2 * EDGE - 2) & (at < 2 * EDGE))
        right = jnp.where(here, turn(three, 2 * n), right)
    right = split_terms(right, 3)
    total = products(left_terms(right), right)
    g_ref[...] = pack_moments(total_ref[...] + total)


def pack_moments(total):
    first, second = total[:COLS], total[COLS:]
    row = lax.broadcasted_iota(jnp.int32, (COLS, LANES), 0)
    lane = lax.broadcasted_iota(jnp.int32, (COLS, LANES), 1)
    col = lane % COLS
    upper = jnp.where(lane < COLS, first, second)
    lower = jnp.where(
        lane < COLS,
        0.5 * (pltpu.roll(first, LANES - COLS, 1) + second),
        pltpu.roll(second, LANES - COLS, 1),
    )
    valid = lane < 2 * COLS
    square = jnp.where(valid, jnp.where(row <= col, upper, lower), 0.0)
    diagonal = jnp.sum(jnp.where(valid & (row == col), lower, 0.0), axis=0, keepdims=True)
    out = []
    for half in range(2):
        out.append(square[8 * half : 8 * half + 8])
    spread_rows = jnp.zeros((8, LANES), jnp.float32)
    sub8 = lax.broadcasted_iota(jnp.int32, (8, LANES), 0)
    lane8 = lax.broadcasted_iota(jnp.int32, (8, LANES), 1)
    for quarter in range(4):
        piece = out[quarter // 2]
        if quarter % 2:
            piece = pltpu.roll(piece, 4, 0)
        if quarter:
            piece = pltpu.roll(piece, 2 * COLS * quarter, 1)
        here = (sub8 < 4) & (lane8 // (2 * COLS) == quarter)
        spread_rows = jnp.where(here, piece, spread_rows)
    return jnp.where(sub8 == 4, diagonal, spread_rows)


def unpack_moments(packed):
    sub8 = lax.broadcasted_iota(jnp.int32, (8, LANES), 0)
    halves = []
    for half in range(2):
        a, b = 2 * half, 2 * half + 1
        top = pltpu.roll(packed, LANES - 2 * COLS * a, 1) if a else packed
        bottom = pltpu.roll(pltpu.roll(packed, LANES - 2 * COLS * b, 1), 4, 0)
        halves.append(jnp.where(sub8 < 4, top, bottom))
    square = jnp.concatenate(halves, axis=0)
    row = lax.broadcasted_iota(jnp.int32, (COLS, COLS), 0)
    col = lax.broadcasted_iota(jnp.int32, (COLS, COLS), 1)
    moments = []
    for pair in range(2):
        turned = pltpu.roll(square, LANES - COLS, 1) if pair else square
        mixed = turned[:, :COLS]
        diagonal = (pltpu.roll(packed, LANES - COLS, 1) if pair else packed)[4:5, :COLS]
        flipped = mixed.T
        moments.append(jnp.where(row <= col, mixed, flipped))
        lower = jnp.where(row == col, diagonal, jnp.where(row > col, mixed, flipped))
        moments.append(lower)
    return moments


def dot(left, right, dims=((1,), (0,))):
    return lax.dot_general(left, right, (dims, ((), ())), precision=HIGH, preferred_element_type=jnp.float32)


def replicated(matrix):
    return [jnp.broadcast_to(matrix[:, i : i + 1], (COLS, LANES)) for i in range(COLS)]


def sweeps(rows):
    rows = list(rows)
    sub = lax.broadcasted_iota(jnp.int32, (COLS, LANES), 0)
    for k in range(COLS):
        scale = 1.0 / rows[k][k : k + 1, :]
        pivot_row = rows[k] * scale
        for i in range(COLS):
            if i != k:
                factor = rows[i][k : k + 1, :]
                moved = rows[i] - factor * pivot_row
                rows[i] = jnp.where(sub == k, factor * scale, moved)
        rows[k] = jnp.where(sub == k, -scale, pivot_row)
        yield rows


def times(rows, right):
    parts = [rows[i] * right[i : i + 1, :] for i in range(COLS)]
    while len(parts) > 1:
        parts = [a + b for a, b in zip(parts[::2], parts[1::2])]
    return parts[0]


def mixer(coeffs, count):
    flipped = split_terms(coeffs.T, count)
    return jnp.concatenate([flipped] * count, axis=1)


def mixed(left, block, count):
    out = jnp.dot(left, split_terms(block, count), preferred_element_type=jnp.float32)
    size = out.shape[0] // count
    return sum(out[size * n : size * (n + 1)] for n in range(count))


def finish_kernel(
    g_ref, v_ref, q_ref, above_ref, below_ref, both_ref,
    ve_ref, qe_ref, abovee_ref, belowe_ref, bothe_ref,
    sol_ref, res_ref, d_ref, dlow_ref, w0_ref, w1_ref, w2_ref,
):
    own_x, own_y = v_ref.shape[0], v_ref.shape[1]
    m0, m1, m2, m3 = unpack_moments(g_ref[...])
    first = ((0,), (0,))
    padding = jnp.zeros((COLS, LANES - COLS), jnp.float32)
    *_, minus_inv = sweeps(replicated(m1))
    minus_alpha = times(minus_inv, jnp.concatenate([m0, padding], axis=1))
    minus_m2a = times(replicated(m2), minus_alpha)
    mix = times(minus_inv, minus_m2a)[:, :COLS]
    minus_m3a = times(replicated(m3), minus_alpha)[:, :COLS]
    minus_alpha, minus_m2a = minus_alpha[:, :COLS], minus_m2a[:, :COLS]
    alpha = -minus_alpha
    left = mixer(jnp.concatenate([mix, minus_alpha], axis=0), 3)
    updated = dot(minus_alpha, minus_m2a, first) - m0
    curved = dot(minus_alpha, minus_m3a, first) + dot(minus_m2a, mix, first)
    steps = sweeps(replicated(0.5 * (curved + curved.T)))
    minus_inv = None
    for x in range(own_x):
        for y in range(own_y):
            q0, q1, qe = q_ref[x, y, :, :LANES], q_ref[x, y, :, LANES:], qe_ref[x, y]
            lane = lanes_of(qe)
            q0 = jnp.where(lane == 0, qe, q0)
            q1 = jnp.where(lane == LANES - 1, turn(qe, LANES // 2), q1)
            block = jnp.concatenate(
                [
                    jnp.concatenate([v_ref[x, y], ve_ref[x, y]], axis=1),
                    jnp.concatenate([q0, q1, qe], axis=1),
                ],
                axis=0,
            )
            value = mixed(left, block, 3)
            d_ref[x, y] = value
            dlow_ref[x, y] = lowered(value)
            minus_inv = next(steps, minus_inv)
    gamma = -times(minus_inv, jnp.concatenate([updated, padding], axis=1))[:, :COLS]
    edge, main = (abovee_ref, belowe_ref, bothe_ref), (above_ref, below_ref, both_ref)
    whole = (w0_ref, w1_ref, w2_ref)
    for end_ref, main_ref, whole_ref in zip(edge, main, whole):
        for ex in range(1, own_x):
            end = end_ref[ex]
            lane = lanes_of(end)
            whole_ref[ex, :, :LANES] = jnp.where(lane == 0, end, main_ref[ex, :, :LANES])
            end = turn(end, LANES // 2)
            whole_ref[ex, :, LANES:] = jnp.where(lane == LANES - 1, end, main_ref[ex, :, LANES:])
    main, edge = sides_of(*whole), sides_of(*edge)
    zero = jnp.zeros((COLS, COLS), jnp.float32)
    last = mixer(
        jnp.concatenate(
            [
                jnp.concatenate([alpha, gamma, zero, zero], axis=0),
                jnp.concatenate([zero, zero, -alpha, -gamma], axis=0),
            ],
            axis=1,
        ),
        2,
    )
    for x in range(1, own_x - 1):
        for y in range(1, own_y - 1):
            low = lambda i, j, t: dlow_ref[i, j, :, tile_of(t)]
            at = (x, y, x + 1, y + 1)
            plane, down, up = zip(*[terms(low, main, t, *at) for t in range(2)])
            ends = terms(lambda i, j, t: dlow_ref[i, j, :, tile_of(2)], edge, 0, *at)
            from_above = shifted(down, 1, turn(ends[1], LANES // 2))
            from_below = shifted(up, -1, ends[2])
            image = [
                SIGMA * d_ref[x, y, :, tile_of(t)] + (plane[t] - from_above[t] - from_below[t])
                for t in range(2)
            ]
            q0, q1, qe = q_ref[x, y, :, :LANES], q_ref[x, y, :, LANES:], qe_ref[x, y]
            lane = lanes_of(qe)
            q0 = jnp.where(lane == 0, qe, q0)
            q1 = jnp.where(lane == LANES - 1, turn(qe, LANES // 2), q1)
            b = v_ref[x, y]
            block = jnp.concatenate(
                [
                    b,
                    d_ref[x, y, :, : 2 * LANES],
                    jnp.concatenate([q0, q1], axis=1),
                    jnp.concatenate(image, axis=1),
                ],
                axis=0,
            )
            out = mixed(last, block, 2)
            sol_ref[:, x - 1, y - 1, :] = out[:COLS]
            res_ref[:, x - 1, y - 1, :] = b + out[COLS:]


def both_ways(axis, to_next, to_last, around=False):
    count = lax.axis_size(axis)
    steps = range(count) if around else range(count - 1)
    before = lax.ppermute(to_next, axis, [(i, (i + 1) % count) for i in steps])
    after = lax.ppermute(to_last, axis, [((i + 1) % count, i) for i in steps])
    return before, after


def spread(value, axes, root):
    count = lax.axis_size(axes)
    copies = jnp.broadcast_to(value[None], (count, *value.shape))
    group = [(root + i) % count for i in range(count)]
    return jnp.sum(lax.all_to_all(copies, axes, 0, 0, axis_index_groups=[group]), axis=0)


def near(value):
    return pltpu.with_memory_space_constraint(value, pltpu.VMEM)


def on_device(loads, moduli, material):
    f32, bf16, wide = jnp.float32, jnp.bfloat16, 2 * LANES
    own_x, own_y = material.shape[:2]
    ext_x, ext_y = own_x + 4, own_y + 4
    own, levels = pl.pallas_call(
        front_kernel,
        out_shape=(
            pltpu.VMEM((2, COLS + 1, own_x, own_y, LANES), f32),
            pltpu.VMEM((moduli.shape[0], LANES), f32),
        ),
        in_specs=[
            pl.BlockSpec(memory_space=pltpu.SMEM),
            pl.BlockSpec(memory_space=pltpu.VMEM),
            pl.BlockSpec(memory_space=pltpu.VMEM),
        ],
        name="front",
    )(moduli, loads, material)
    place = lax.axis_index(GY)
    row = lax.broadcasted_iota(jnp.int32, (8, LANES), 0)
    flags = jnp.where(row == 0, place > 0, place < lax.axis_size(GY) - 1).astype(f32)
    before, after = both_ways("gx", own, own)
    mid = jnp.concatenate([before, own, after], axis=2)
    before, after = both_ways(GY, mid[:, :, :, 2:], mid[:, :, :, :2], around=True)
    flat = [near(part.reshape(-1, LANES)) for part in (before, mid, after)]
    ends = pltpu.VMEM((COLS + 8, LANES), f32)
    first, last = pl.pallas_call(
        functools.partial(pack_kernel, ext_x=ext_x, ext_y=ext_y), out_shape=(ends, ends), name="pack"
    )(near(flags), *flat)
    before, after = both_ways("gz", last, first)
    nodes = own_x * own_y

    def weights(size):
        return (pltpu.VMEM((ext_x - 1, ext_y, size), f32),) * 3

    def fields(size):
        return (pltpu.VMEM((ext_x - 2, ext_y - 2, COLS, size), f32),) * 2

    def scratch(size):
        return [
            pltpu.VMEM((ext_x, ext_y, COLS, size), f32),
            pltpu.VMEM((ext_x - 2, ext_y - 2, COLS, size), f32),
            pltpu.VMEM((ext_x, ext_y, size), f32),
        ]

    *main, total, edge, ids = pl.pallas_call(
        main_kernel,
        out_shape=(
            *fields(wide),
            *weights(wide),
            pltpu.VMEM((2 * COLS, LANES), f32),
            pltpu.VMEM((ext_x, ext_y, COLS, LANES), f32),
            pltpu.VMEM((ext_x, ext_y, LANES), f32),
        ),
        scratch_shapes=scratch(wide)
        + [pltpu.VMEM((6 * COLS, nodes * wide), bf16), pltpu.VMEM((9 * COLS, nodes * wide), bf16)],
        name="main",
    )(near(levels), near(flags), *flat)
    *edges, moments = pl.pallas_call(
        edge_kernel,
        out_shape=(*fields(LANES), *weights(LANES), pltpu.VMEM((8, LANES), f32)),
        scratch_shapes=scratch(LANES),
        name="edge",
    )(*[near(value) for value in (levels, total, edge, ids, before, after)])
    rows = 5
    length, chips = lax.axis_size("gz"), lax.axis_size("gy_0")
    moments = spread(moments[:rows].reshape(rows, 1, LANES), "gz", 17 * length // 32)
    middle = (lax.axis_size("gx") // 2 * chips + chips // 2) * 2 + 1
    moments = spread(moments, PLANE, middle).reshape(rows, LANES)
    moments = jnp.concatenate([moments, jnp.zeros((8 - rows, LANES), f32)], axis=0)
    out = jax.ShapeDtypeStruct(loads.shape, f32)
    return pl.pallas_call(
        finish_kernel,
        out_shape=(out, out),
        scratch_shapes=[pltpu.VMEM((ext_x - 2, ext_y - 2, COLS, 3 * LANES), f32)] * 2
        + [pltpu.VMEM((ext_x - 1, ext_y, wide), f32)] * 3,
        name="finish",
    )(*[near(value) for value in (moments, *main, *edges)])


def solution(mesh):
    wide, long = mesh.shape["gy"] // 2, mesh.shape["gz"]
    split = Mesh(mesh.devices.reshape(mesh.shape["gx"], wide, 2, long), ("gx", "gy_0", "gy_1", "gz"))
    spec = P(None, "gx", GY, "gz")
    return jax.shard_map(
        on_device,
        mesh=split,
        in_specs=(spec, P(), P("gx", GY, "gz")),
        out_specs=(spec, spec),
        check_vma=False,
    )
```

```python
import functools

import jax
import jax.numpy as jnp
import numpy as np
from jax import lax
from jax.experimental import pallas as pl
from jax.experimental.pallas import tpu as pltpu
from jax.sharding import Mesh
from jax.sharding import PartitionSpec as P

PLANE = ("gx", "gy_0", "gy_1")
GY = ("gy_0", "gy_1")
SIGMA = 0.25
COLS = 16
LANES = 128
EDGE = LANES // 4
HIGH = lax.Precision.HIGHEST


def stiffness_table():
    line_mass = np.array([[1.0 / 3.0, 1.0 / 6.0], [1.0 / 6.0, 1.0 / 3.0]])
    line_stiff = np.array([[1.0, -1.0], [-1.0, 1.0]])
    table = np.zeros((8, 8))
    for target in range(8):
        for source in range(8):
            target_bits = [target >> 2 & 1, target >> 1 & 1, target & 1]
            source_bits = [source >> 2 & 1, source >> 1 & 1, source & 1]
            total = 0.0
            for stiff_dim in range(3):
                factor = 1.0
                for other in range(3):
                    if other == stiff_dim:
                        factor = factor * line_stiff[target_bits[other], source_bits[other]]
                    else:
                        factor = factor * line_mass[target_bits[other], source_bits[other]]
                total = total + factor
            table[target, source] = total
    return table


def kernel_scale():
    table = np.asarray(jnp.asarray(stiffness_table(), jnp.bfloat16).astype(jnp.float32))
    unit = -float(table[0, 7])
    for target in range(8):
        for source in range(8):
            bits = bin(target ^ source).count("1")
            want = (4.0, 0.0, -1.0, -1.0)[bits] * unit
            assert abs(float(table[target, source]) - want) < 1e-12
    return unit


UNIT = kernel_scale()


def lowered(value):
    return value.astype(jnp.bfloat16).astype(jnp.float32)


def tile_of(tile):
    return slice(tile * LANES, (tile + 1) * LANES)


def lanes_of(value):
    return lax.broadcasted_iota(jnp.int32, value.shape, 1)


def turn(value, amount):
    amount %= LANES
    return pltpu.roll(value, amount, 1) if amount else value


def shifted(tiles, step, beyond=None):
    count = len(tiles)
    turned = [turn(t, -step) for t in tiles]
    past = turn(beyond, -step) if beyond is not None else turned[0 if step > 0 else -1]
    lane = lanes_of(tiles[0])
    if step > 0:
        return [jnp.where(lane < LANES - 1, turned[i], turned[i + 1] if i + 1 < count else past) for i in range(count)]
    return [jnp.where(lane > 0, turned[i], turned[i - 1] if i else past) for i in range(count)]


def terms(low, sides, tile, x, y, wx, wy):
    above, below, both = sides
    around = {(i, j): low(x + i, y + j, tile) for i in (-1, 0, 1) for j in (-1, 0, 1)}
    total = None
    for i in (-1, 1):
        for j in (-1, 1):
            ex, ey = wx + (i - 1) // 2, wy + (j - 1) // 2
            others = around[i, 0] + around[0, j] + around[i, j]
            new = (
                both(ex, ey, tile) * around[i, j],
                below(ex, ey, tile) * others,
                above(ex, ey, tile) * others,
            )
            total = new if total is None else tuple(a + b for a, b in zip(total, new))
    rim = [both(wx + i, wy + j, tile) for i in (-1, 0) for j in (-1, 0)]
    centre = (4.0 * ((rim[0] + rim[1]) + (rim[2] + rim[3]))) * around[0, 0]
    return centre - total[0], total[1], total[2]


def operator(field, low, sides, count, x, y, wx, wy):
    plane, down, up = zip(*[terms(low, sides, t, x, y, wx, wy) for t in range(count)])
    from_above, from_below = shifted(down, 1), shifted(up, -1)
    return [SIGMA * field(t) + (plane[t] - from_above[t] - from_below[t]) for t in range(count)]


def split_terms(value, count):
    parts = []
    for n in range(count):
        part = value.astype(jnp.bfloat16)
        parts.append(part)
        if n + 1 < count:
            value = value - part.astype(jnp.float32)
    return jnp.concatenate(parts, axis=0)


def rows_of(refs, flags_ref, tile, x, y, first, count):
    before_x_ref, own_ref, after_x_ref, before_ref, before_last_ref, after_ref, after_last_ref = refs
    flag = None
    if 2 <= y < 6:
        ref, column, wide, tall, at = (before_x_ref, own_ref, after_x_ref)[x // 2], x % 2, 2, 4, y - 2
    else:
        low = y < 2
        flag, at, tall = (0, y, 2) if low else (1, y - 6, 2)
        if x < 4:
            ref, column, wide = before_ref if low else after_ref, x, 4
        else:
            ref, column, wide = before_last_ref if low else after_last_ref, x - 4, 2
    stride = wide * tall
    start = tile * (ref.shape[0] // 2) + first * stride + column * tall + at
    value = ref[pl.ds(start, count, stride=stride), :] if count > 1 else ref[start : start + 1, :]
    if flag is not None:
        value = jnp.where(flags_ref[flag : flag + 1, :] > 0.0, value, 0.0)
    return value


def front_kernel(moduli_ref, loads_ref, material_ref, own_ref, levels_ref):
    for t in range(2):
        own_ref[t, :COLS] = loads_ref[:, :, :, tile_of(t)]
        own_ref[t, COLS] = (material_ref[:, :, tile_of(t)] + 1).astype(jnp.float32)
    for level in range(moduli_ref.shape[0]):
        levels_ref[level : level + 1, :] = jnp.full((1, LANES), moduli_ref[level], jnp.float32)


def pack_kernel(flags_ref, *refs, ext_x, ext_y):
    *refs, lo_ref, hi_ref = refs
    for tile, out_ref in ((0, lo_ref), (1, hi_ref)):
        offset = 2 * tile
        lane = lax.broadcasted_iota(jnp.int32, (COLS, LANES), 1)
        packed = jnp.zeros((COLS, LANES), jnp.float32)
        ids = [jnp.zeros((1, LANES), jnp.float32)] * ext_y
        for x in range(ext_x):
            for y in range(ext_y):
                node = x * ext_y + y
                value = rows_of(refs, flags_ref, tile, x, y, 0, COLS)
                packed = jnp.where(lane // 2 == node, turn(value, 2 * node + offset), packed)
                value = rows_of(refs, flags_ref, tile, x, y, COLS, 1)
                ids[y] = jnp.where(lane[:1] // 2 == x, turn(value, 2 * x + offset), ids[y])
        out_ref[:COLS, :] = packed
        for y in range(ext_y):
            out_ref[COLS + y : COLS + y + 1, :] = ids[y]


def modulus_of(levels_ref, ids):
    modulus = jnp.zeros_like(ids)
    for level in range(levels_ref.shape[0]):
        modulus = jnp.where(ids == level + 1.0, levels_ref[level : level + 1, :], modulus)
    return modulus


def element_weights(e_ref, above_ref, below_ref, both_ref, count):
    ext_x, ext_y = e_ref.shape[:2]
    for ex in range(ext_x - 1):
        flat = []
        for t in range(count):
            both_x = e_ref[ex, :, tile_of(t)] + e_ref[ex + 1, :, tile_of(t)]
            flat.append(both_x + pltpu.roll(both_x, ext_y - 1, 0))
        ahead = shifted(flat, 1)
        weights = [(0.125 * UNIT) * (flat[t] + ahead[t]) for t in range(count)]
        behind = shifted(weights, -1)
        for t in range(count):
            above_ref[ex, :, tile_of(t)] = weights[t]
            below_ref[ex, :, tile_of(t)] = behind[t]
            both_ref[ex, :, tile_of(t)] = weights[t] + behind[t]


def sides_of(*refs):
    return tuple(lambda ex, ey, t, ref=ref: ref[ex, ey : ey + 1, tile_of(t)] for ref in refs)


def first_image(v_ref, low_ref, e_ref, sides, q_ref, qlow_ref, count):
    ext_x, ext_y = low_ref.shape[0], low_ref.shape[1]
    for x in range(1, ext_x - 1):
        for y in range(1, ext_y - 1):
            image = operator(
                lambda t: v_ref[x - 1, y - 1, :, tile_of(t)],
                lambda i, j, t: low_ref[i, j, :, tile_of(t)],
                sides, count, x, y, x, y,
            )
            for t in range(count):
                value = image[t]
                if count == 1 or x in (1, ext_x - 2) or y in (1, ext_y - 2):
                    value = jnp.where(e_ref[x, y : y + 1, tile_of(t)] > 0.0, value, 0.0)
                q_ref[x - 1, y - 1, :, tile_of(t)] = value
                qlow_ref[x - 1, y - 1, :, tile_of(t)] = lowered(value)


def own_nodes(v_ref, q_ref, qlow_ref, sides, count):
    own_x, own_y = v_ref.shape[0], v_ref.shape[1]
    for x in range(1, own_x - 1):
        for y in range(1, own_y - 1):
            image = operator(
                lambda t: q_ref[x, y, :, tile_of(t)],
                lambda i, j, t: qlow_ref[i, j, :, tile_of(t)],
                sides, count, x, y, x + 1, y + 1,
            )
            for t in range(count):
                yield t, v_ref[x, y, :, tile_of(t)], q_ref[x, y, :, tile_of(t)], image[t]


def left_terms(right):
    return jnp.concatenate([right[3 * COLS * n : 3 * COLS * n + 2 * COLS] for n in range(3)], axis=0)


def products(left, right):
    product = lax.dot_general(left, right, (((1,), (1,)), ((), ())), preferred_element_type=jnp.float32)
    rows = sum(product[2 * COLS * n : 2 * COLS * (n + 1)] for n in range(3))
    lane = lax.broadcasted_iota(jnp.int32, (2 * COLS, LANES), 1)
    first = rows[:, :LANES]
    rest = jnp.concatenate([rows[:, LANES:], jnp.zeros((2 * COLS, 2 * LANES - 9 * COLS), jnp.float32)], axis=1)
    third = jnp.where(lane < 2 * COLS, turn(first, -6 * COLS), turn(rest, 2 * COLS))
    return first + turn(first, -3 * COLS) + third


def main_kernel(
    levels_ref, flags_ref, a_ref, b_ref, c_ref, d_ref, e0_ref, f_ref, g_ref,
    v_ref, q_ref, above_ref, below_ref, both_ref, total_ref, ve_ref, ie_ref,
    low_ref, qlow_ref, e_ref, left_ref, right_ref,
):
    ext_x, ext_y = low_ref.shape[0], low_ref.shape[1]
    refs = (a_ref, b_ref, c_ref, d_ref, e0_ref, f_ref, g_ref)
    for x in range(ext_x):
        for y in range(ext_y):
            tiles = [rows_of(refs, flags_ref, t, x, y, COLS, 1) for t in range(2)]
            lane = lanes_of(tiles[0])
            edge = jnp.where(lane < EDGE, tiles[0], jnp.where(lane < 2 * EDGE, turn(tiles[1], 2 * EDGE), 0.0))
            ie_ref[x, y : y + 1, :] = edge
            for t in range(2):
                e_ref[x, y : y + 1, tile_of(t)] = tiles[t]
        for t in range(2):
            e_ref[x, :, tile_of(t)] = modulus_of(levels_ref, e_ref[x, :, tile_of(t)])
    element_weights(e_ref, above_ref, below_ref, both_ref, 2)
    for x in range(ext_x):
        for y in range(ext_y):
            tiles = [rows_of(refs, flags_ref, t, x, y, 0, COLS) for t in range(2)]
            lane = lanes_of(tiles[0])
            edge = jnp.where(lane < EDGE, tiles[0], jnp.where(lane < 2 * EDGE, turn(tiles[1], 2 * EDGE), 0.0))
            ve_ref[x, y] = edge
            for t in range(2):
                low_ref[x, y, :, tile_of(t)] = lowered(tiles[t])
                if 0 < x < ext_x - 1 and 0 < y < ext_y - 1:
                    v_ref[x - 1, y - 1, :, tile_of(t)] = tiles[t]
    sides = sides_of(above_ref, below_ref, both_ref)
    first_image(v_ref, low_ref, e_ref, sides, q_ref, qlow_ref, 2)
    for n, (t, b, q, w) in enumerate(own_nodes(v_ref, q_ref, qlow_ref, sides, 2)):
        right = split_terms(jnp.concatenate([b, q, w], axis=0), 3)
        left = left_terms(right)
        here = lanes_of(left) >= 2 if t == 0 else lanes_of(left) < LANES - 2
        left_ref[:, tile_of(n)] = jnp.where(here, left, jnp.zeros_like(left))
        right_ref[:, tile_of(n)] = right
    total_ref[...] = products(left_ref[...], right_ref[...])


def edge_kernel(
    levels_ref, total_ref, ve_ref, ie_ref, before_ref, after_ref,
    v_ref, q_ref, above_ref, below_ref, both_ref, g_ref,
    low_ref, qlow_ref, e_ref,
):
    ext_x, ext_y = low_ref.shape[0], low_ref.shape[1]

    def with_ends(own, before, after, index):
        lane = lanes_of(own)
        follows, comes = turn(after, LANES // 2 - 2 * index), turn(before, LANES - 2 - 2 * index)
        value = jnp.where(lane >= LANES - 2, comes, own)
        return jnp.where((lane >= LANES // 2) & (lane < LANES // 2 + 2), follows, value)

    for x in range(ext_x):
        ids = with_ends(ie_ref[x], before_ref[COLS : COLS + ext_y, :], after_ref[COLS : COLS + ext_y, :], x)
        e_ref[x] = modulus_of(levels_ref, ids)
    element_weights(e_ref, above_ref, below_ref, both_ref, 1)
    before, after = before_ref[:COLS, :], after_ref[:COLS, :]
    for x in range(ext_x):
        for y in range(ext_y):
            value = with_ends(ve_ref[x, y], before, after, x * ext_y + y)
            low_ref[x, y] = lowered(value)
            if 0 < x < ext_x - 1 and 0 < y < ext_y - 1:
                v_ref[x - 1, y - 1] = value
    sides = sides_of(above_ref, below_ref, both_ref)
    first_image(v_ref, low_ref, e_ref, sides, q_ref, qlow_ref, 1)
    right = jnp.zeros((3 * COLS, LANES), jnp.float32)
    for n, (_, b, q, w) in enumerate(own_nodes(v_ref, q_ref, qlow_ref, sides, 1)):
        three = jnp.concatenate([b, q, w], axis=0)
        at = lanes_of(three) - 2 * n
        here = ((at >= 0) & (at < 2)) | ((at >= 2 * EDGE - 2) & (at < 2 * EDGE))
        right = jnp.where(here, turn(three, 2 * n), right)
    right = split_terms(right, 3)
    total = products(left_terms(right), right)
    g_ref[...] = pack_moments(total_ref[...] + total)


def pack_moments(total):
    first, second = total[:COLS], total[COLS:]
    row = lax.broadcasted_iota(jnp.int32, (COLS, LANES), 0)
    lane = lax.broadcasted_iota(jnp.int32, (COLS, LANES), 1)
    col = lane % COLS
    upper = jnp.where(lane < COLS, first, second)
    lower = jnp.where(
        lane < COLS,
        0.5 * (pltpu.roll(first, LANES - COLS, 1) + second),
        pltpu.roll(second, LANES - COLS, 1),
    )
    valid = lane < 2 * COLS
    square = jnp.where(valid, jnp.where(row <= col, upper, lower), 0.0)
    diagonal = jnp.sum(jnp.where(valid & (row == col), lower, 0.0), axis=0, keepdims=True)
    out = []
    for half in range(2):
        out.append(square[8 * half : 8 * half + 8])
    spread_rows = jnp.zeros((8, LANES), jnp.float32)
    sub8 = lax.broadcasted_iota(jnp.int32, (8, LANES), 0)
    lane8 = lax.broadcasted_iota(jnp.int32, (8, LANES), 1)
    for quarter in range(4):
        piece = out[quarter // 2]
        if quarter % 2:
            piece = pltpu.roll(piece, 4, 0)
        if quarter:
            piece = pltpu.roll(piece, 2 * COLS * quarter, 1)
        here = (sub8 < 4) & (lane8 // (2 * COLS) == quarter)
        spread_rows = jnp.where(here, piece, spread_rows)
    return jnp.where(sub8 == 4, diagonal, spread_rows)


def unpack_moments(packed):
    sub8 = lax.broadcasted_iota(jnp.int32, (8, LANES), 0)
    halves = []
    for half in range(2):
        a, b = 2 * half, 2 * half + 1
        top = pltpu.roll(packed, LANES - 2 * COLS * a, 1) if a else packed
        bottom = pltpu.roll(pltpu.roll(packed, LANES - 2 * COLS * b, 1), 4, 0)
        halves.append(jnp.where(sub8 < 4, top, bottom))
    square = jnp.concatenate(halves, axis=0)
    row = lax.broadcasted_iota(jnp.int32, (COLS, COLS), 0)
    col = lax.broadcasted_iota(jnp.int32, (COLS, COLS), 1)
    moments = []
    for pair in range(2):
        turned = pltpu.roll(square, LANES - COLS, 1) if pair else square
        mixed = turned[:, :COLS]
        diagonal = (pltpu.roll(packed, LANES - COLS, 1) if pair else packed)[4:5, :COLS]
        flipped = mixed.T
        moments.append(jnp.where(row <= col, mixed, flipped))
        lower = jnp.where(row == col, diagonal, jnp.where(row > col, mixed, flipped))
        moments.append(lower)
    return moments


def dot(left, right, dims=((1,), (0,))):
    return lax.dot_general(left, right, (dims, ((), ())), precision=HIGH, preferred_element_type=jnp.float32)


def replicated(matrix):
    return [jnp.broadcast_to(matrix[:, i : i + 1], (COLS, LANES)) for i in range(COLS)]


def sweeps(rows):
    rows = list(rows)
    sub = lax.broadcasted_iota(jnp.int32, (COLS, LANES), 0)
    for k in range(COLS):
        scale = 1.0 / rows[k][k : k + 1, :]
        pivot_row = rows[k] * scale
        for i in range(COLS):
            if i != k:
                factor = rows[i][k : k + 1, :]
                moved = rows[i] - factor * pivot_row
                rows[i] = jnp.where(sub == k, factor * scale, moved)
        rows[k] = jnp.where(sub == k, -scale, pivot_row)
        yield rows


def times(rows, right):
    parts = [rows[i] * right[i : i + 1, :] for i in range(COLS)]
    while len(parts) > 1:
        parts = [a + b for a, b in zip(parts[::2], parts[1::2])]
    return parts[0]


def mixer(coeffs, count):
    flipped = split_terms(coeffs.T, count)
    return jnp.concatenate([flipped] * count, axis=1)


def mixed(left, block, count):
    out = jnp.dot(left, split_terms(block, count), preferred_element_type=jnp.float32)
    size = out.shape[0] // count
    return sum(out[size * n : size * (n + 1)] for n in range(count))


def finish_kernel(
    g_ref, v_ref, q_ref, above_ref, below_ref, both_ref,
    ve_ref, qe_ref, abovee_ref, belowe_ref, bothe_ref,
    sol_ref, res_ref, d_ref, dlow_ref, w0_ref, w1_ref, w2_ref,
):
    own_x, own_y = v_ref.shape[0], v_ref.shape[1]
    m0, m1, m2, m3 = unpack_moments(g_ref[...])
    first = ((0,), (0,))
    padding = jnp.zeros((COLS, LANES - COLS), jnp.float32)
    *_, minus_inv = sweeps(replicated(m1))
    minus_alpha = times(minus_inv, jnp.concatenate([m0, padding], axis=1))
    minus_m2a = times(replicated(m2), minus_alpha)
    mix = times(minus_inv, minus_m2a)[:, :COLS]
    minus_m3a = times(replicated(m3), minus_alpha)[:, :COLS]
    minus_alpha, minus_m2a = minus_alpha[:, :COLS], minus_m2a[:, :COLS]
    alpha = -minus_alpha
    left = mixer(jnp.concatenate([mix, minus_alpha], axis=0), 3)
    updated = dot(minus_alpha, minus_m2a, first) - m0
    curved = dot(minus_alpha, minus_m3a, first) + dot(minus_m2a, mix, first)
    steps = sweeps(replicated(0.5 * (curved + curved.T)))
    minus_inv = None
    for x in range(own_x):
        for y in range(own_y):
            q0, q1, qe = q_ref[x, y, :, :LANES], q_ref[x, y, :, LANES:], qe_ref[x, y]
            lane = lanes_of(qe)
            q0 = jnp.where(lane == 0, qe, q0)
            q1 = jnp.where(lane == LANES - 1, turn(qe, LANES // 2), q1)
            block = jnp.concatenate(
                [
                    jnp.concatenate([v_ref[x, y], ve_ref[x, y]], axis=1),
                    jnp.concatenate([q0, q1, qe], axis=1),
                ],
                axis=0,
            )
            value = mixed(left, block, 3)
            d_ref[x, y] = value
            dlow_ref[x, y] = lowered(value)
            minus_inv = next(steps, minus_inv)
    gamma = -times(minus_inv, jnp.concatenate([updated, padding], axis=1))[:, :COLS]
    edge, main = (abovee_ref, belowe_ref, bothe_ref), (above_ref, below_ref, both_ref)
    whole = (w0_ref, w1_ref, w2_ref)
    for end_ref, main_ref, whole_ref in zip(edge, main, whole):
        for ex in range(1, own_x):
            end = end_ref[ex]
            lane = lanes_of(end)
            whole_ref[ex, :, :LANES] = jnp.where(lane == 0, end, main_ref[ex, :, :LANES])
            end = turn(end, LANES // 2)
            whole_ref[ex, :, LANES:] = jnp.where(lane == LANES - 1, end, main_ref[ex, :, LANES:])
    main, edge = sides_of(*whole), sides_of(*edge)
    zero = jnp.zeros((COLS, COLS), jnp.float32)
    last = mixer(
        jnp.concatenate(
            [
                jnp.concatenate([alpha, gamma, zero, zero], axis=0),
                jnp.concatenate([zero, zero, -alpha, -gamma], axis=0),
            ],
            axis=1,
        ),
        2,
    )
    for x in range(1, own_x - 1):
        for y in range(1, own_y - 1):
            low = lambda i, j, t: dlow_ref[i, j, :, tile_of(t)]
            at = (x, y, x + 1, y + 1)
            plane, down, up = zip(*[terms(low, main, t, *at) for t in range(2)])
            ends = terms(lambda i, j, t: dlow_ref[i, j, :, tile_of(2)], edge, 0, *at)
            from_above = shifted(down, 1, turn(ends[1], LANES // 2))
            from_below = shifted(up, -1, ends[2])
            image = [
                SIGMA * d_ref[x, y, :, tile_of(t)] + (plane[t] - from_above[t] - from_below[t])
                for t in range(2)
            ]
            q0, q1, qe = q_ref[x, y, :, :LANES], q_ref[x, y, :, LANES:], qe_ref[x, y]
            lane = lanes_of(qe)
            q0 = jnp.where(lane == 0, qe, q0)
            q1 = jnp.where(lane == LANES - 1, turn(qe, LANES // 2), q1)
            b = v_ref[x, y]
            block = jnp.concatenate(
                [
                    b,
                    d_ref[x, y, :, : 2 * LANES],
                    jnp.concatenate([q0, q1], axis=1),
                    jnp.concatenate(image, axis=1),
                ],
                axis=0,
            )
            out = mixed(last, block, 2)
            sol_ref[:, x - 1, y - 1, :] = out[:COLS]
            res_ref[:, x - 1, y - 1, :] = b + out[COLS:]


def both_ways(axis, to_next, to_last, around=False):
    count = lax.axis_size(axis)
    steps = range(count) if around else range(count - 1)
    before = lax.ppermute(to_next, axis, [(i, (i + 1) % count) for i in steps])
    after = lax.ppermute(to_last, axis, [((i + 1) % count, i) for i in steps])
    return before, after


def spread(value, axes, root):
    count = lax.axis_size(axes)
    copies = jnp.broadcast_to(value[None], (count, *value.shape))
    group = [(root + i) % count for i in range(count)]
    return jnp.sum(lax.all_to_all(copies, axes, 0, 0, axis_index_groups=[group]), axis=0)


def near(value):
    return pltpu.with_memory_space_constraint(value, pltpu.VMEM)


def on_device(loads, moduli, material):
    f32, bf16, wide = jnp.float32, jnp.bfloat16, 2 * LANES
    own_x, own_y = material.shape[:2]
    ext_x, ext_y = own_x + 4, own_y + 4
    own, levels = pl.pallas_call(
        front_kernel,
        out_shape=(
            pltpu.VMEM((2, COLS + 1, own_x, own_y, LANES), f32),
            pltpu.VMEM((moduli.shape[0], LANES), f32),
        ),
        in_specs=[
            pl.BlockSpec(memory_space=pltpu.SMEM),
            pl.BlockSpec(memory_space=pltpu.VMEM),
            pl.BlockSpec(memory_space=pltpu.VMEM),
        ],
        name="front",
    )(moduli, loads, material)
    place = lax.axis_index(GY)
    row = lax.broadcasted_iota(jnp.int32, (8, LANES), 0)
    flags = jnp.where(row == 0, place > 0, place < lax.axis_size(GY) - 1).astype(f32)
    before, after = both_ways("gx", own, own)
    part = jnp.concatenate([before, own], axis=2)
    parts = part[:, :, :, 2:], part[:, :, :, :2]
    sides = both_ways(GY, *parts, around=True)
    lasts = both_ways(GY, after[:, :, :, 2:], after[:, :, :, :2], around=True)
    flat = [near(v.reshape(-1, LANES)) for v in (before, own, after, sides[0], lasts[0], sides[1], lasts[1])]
    ends = pltpu.VMEM((COLS + 8, LANES), f32)
    first, last = pl.pallas_call(
        functools.partial(pack_kernel, ext_x=ext_x, ext_y=ext_y), out_shape=(ends, ends), name="pack"
    )(near(flags), *flat)
    before, after = both_ways("gz", last, first)
    nodes = own_x * own_y

    def weights(size):
        return (pltpu.VMEM((ext_x - 1, ext_y, size), f32),) * 3

    def fields(size):
        return (pltpu.VMEM((ext_x - 2, ext_y - 2, COLS, size), f32),) * 2

    def scratch(size):
        return [
            pltpu.VMEM((ext_x, ext_y, COLS, size), f32),
            pltpu.VMEM((ext_x - 2, ext_y - 2, COLS, size), f32),
            pltpu.VMEM((ext_x, ext_y, size), f32),
        ]

    *main, total, edge, ids = pl.pallas_call(
        main_kernel,
        out_shape=(
            *fields(wide),
            *weights(wide),
            pltpu.VMEM((2 * COLS, LANES), f32),
            pltpu.VMEM((ext_x, ext_y, COLS, LANES), f32),
            pltpu.VMEM((ext_x, ext_y, LANES), f32),
        ),
        scratch_shapes=scratch(wide)
        + [pltpu.VMEM((6 * COLS, nodes * wide), bf16), pltpu.VMEM((9 * COLS, nodes * wide), bf16)],
        name="main",
    )(near(levels), near(flags), *flat)
    *edges, moments = pl.pallas_call(
        edge_kernel,
        out_shape=(*fields(LANES), *weights(LANES), pltpu.VMEM((8, LANES), f32)),
        scratch_shapes=scratch(LANES),
        name="edge",
    )(*[near(value) for value in (levels, total, edge, ids, before, after)])
    rows = 5
    length, chips = lax.axis_size("gz"), lax.axis_size("gy_0")
    moments = spread(moments[:rows].reshape(rows, 1, LANES), "gz", 17 * length // 32)
    middle = (lax.axis_size("gx") // 2 * chips + chips // 2) * 2 + 1
    moments = spread(moments, PLANE, middle).reshape(rows, LANES)
    moments = jnp.concatenate([moments, jnp.zeros((8 - rows, LANES), f32)], axis=0)
    out = jax.ShapeDtypeStruct(loads.shape, f32)
    return pl.pallas_call(
        finish_kernel,
        out_shape=(out, out),
        scratch_shapes=[pltpu.VMEM((ext_x - 2, ext_y - 2, COLS, 3 * LANES), f32)] * 2
        + [pltpu.VMEM((ext_x - 1, ext_y, wide), f32)] * 3,
        name="finish",
    )(*[near(value) for value in (moments, *main, *edges)])


def solution(mesh):
    chips, long = mesh.shape["gy"] // 2, mesh.shape["gz"]
    split = Mesh(mesh.devices.reshape(mesh.shape["gx"], chips, 2, long), ("gx", "gy_0", "gy_1", "gz"))
    spec = P(None, "gx", GY, "gz")

    return jax.shard_map(
        on_device,
        mesh=split,
        in_specs=(spec, P(), P("gx", GY, "gz")),
        out_specs=(spec, spec),
        check_vma=False,
    )
```

```python
import functools

import jax
import jax.numpy as jnp
import numpy as np
from jax import lax
from jax.experimental import pallas as pl
from jax.experimental.pallas import tpu as pltpu
from jax.sharding import Mesh
from jax.sharding import PartitionSpec as P

PLANE = ("gx", "gy_0", "gy_1")
GY = ("gy_0", "gy_1")
SIGMA = 0.25
COLS = 16
LANES = 128
EDGE = LANES // 4
HIGH = lax.Precision.HIGHEST
GRANT = pltpu.CompilerParams(vmem_limit_bytes=16 * 2**20)


def stiffness_table():
    line_mass = np.array([[1.0 / 3.0, 1.0 / 6.0], [1.0 / 6.0, 1.0 / 3.0]])
    line_stiff = np.array([[1.0, -1.0], [-1.0, 1.0]])
    table = np.zeros((8, 8))
    for target in range(8):
        for source in range(8):
            target_bits = [target >> 2 & 1, target >> 1 & 1, target & 1]
            source_bits = [source >> 2 & 1, source >> 1 & 1, source & 1]
            total = 0.0
            for stiff_dim in range(3):
                factor = 1.0
                for other in range(3):
                    if other == stiff_dim:
                        factor = factor * line_stiff[target_bits[other], source_bits[other]]
                    else:
                        factor = factor * line_mass[target_bits[other], source_bits[other]]
                total = total + factor
            table[target, source] = total
    return table


def kernel_scale():
    table = np.asarray(jnp.asarray(stiffness_table(), jnp.bfloat16).astype(jnp.float32))
    unit = -float(table[0, 7])
    for target in range(8):
        for source in range(8):
            bits = bin(target ^ source).count("1")
            want = (4.0, 0.0, -1.0, -1.0)[bits] * unit
            assert abs(float(table[target, source]) - want) < 1e-12
    return unit


UNIT = kernel_scale()


def lowered(value):
    return value.astype(jnp.bfloat16).astype(jnp.float32)


MIDDLE = (2, 3, 4, 5)
OUTER = (0, 1, 6, 7)


def tile_of(tile):
    return slice(tile * LANES, (tile + 1) * LANES)


def lanes_of(value):
    return lax.broadcasted_iota(jnp.int32, value.shape, 1)


def turn(value, amount):
    amount %= LANES
    return pltpu.roll(value, amount, 1) if amount else value


def shifted(tiles, step, beyond=None):
    count = len(tiles)
    turned = [turn(t, -step) for t in tiles]
    past = turn(beyond, -step) if beyond is not None else turned[0 if step > 0 else -1]
    lane = lanes_of(tiles[0])
    if step > 0:
        return [jnp.where(lane < LANES - 1, turned[i], turned[i + 1] if i + 1 < count else past) for i in range(count)]
    return [jnp.where(lane > 0, turned[i], turned[i - 1] if i else past) for i in range(count)]


def terms(low, sides, tile, x, y, wx, wy):
    above, below, both = sides
    around = {(i, j): low(x + i, y + j, tile) for i in (-1, 0, 1) for j in (-1, 0, 1)}
    total = None
    for i in (-1, 1):
        for j in (-1, 1):
            ex, ey = wx + (i - 1) // 2, wy + (j - 1) // 2
            others = around[i, 0] + around[0, j] + around[i, j]
            new = (
                both(ex, ey, tile) * around[i, j],
                below(ex, ey, tile) * others,
                above(ex, ey, tile) * others,
            )
            total = new if total is None else tuple(a + b for a, b in zip(total, new))
    rim = [both(wx + i, wy + j, tile) for i in (-1, 0) for j in (-1, 0)]
    centre = (4.0 * ((rim[0] + rim[1]) + (rim[2] + rim[3]))) * around[0, 0]
    return centre - total[0], total[1], total[2]


def operator(field, low, sides, count, x, y, wx, wy):
    plane, down, up = zip(*[terms(low, sides, t, x, y, wx, wy) for t in range(count)])
    from_above, from_below = shifted(down, 1), shifted(up, -1)
    return [SIGMA * field(t) + (plane[t] - from_above[t] - from_below[t]) for t in range(count)]


def split_terms(value, count):
    parts = []
    for n in range(count):
        part = value.astype(jnp.bfloat16)
        parts.append(part)
        if n + 1 < count:
            value = value - part.astype(jnp.float32)
    return jnp.concatenate(parts, axis=0)


def rows_of(refs, flags_ref, tile, x, y, first, count):
    before_x_ref, own_ref, after_x_ref, before_ref, before_last_ref, after_ref, after_last_ref = refs
    flag = None
    if 2 <= y < 6:
        ref, column, wide, tall, at = (before_x_ref, own_ref, after_x_ref)[x // 2], x % 2, 2, 4, y - 2
    else:
        low = y < 2
        flag, at, tall = (0, y, 2) if low else (1, y - 6, 2)
        if x < 4:
            ref, column, wide = before_ref if low else after_ref, x, 4
        else:
            ref, column, wide = before_last_ref if low else after_last_ref, x - 4, 2
    stride = wide * tall
    start = tile * (ref.shape[0] // 2) + first * stride + column * tall + at
    value = ref[pl.ds(start, count, stride=stride), :] if count > 1 else ref[start : start + 1, :]
    if flag is not None:
        value = jnp.where(flags_ref[flag : flag + 1, :] > 0.0, value, 0.0)
    return value


def front_kernel(moduli_ref, loads_ref, material_ref, own_ref, levels_ref):
    for t in range(2):
        own_ref[t, :COLS] = loads_ref[:, :, :, tile_of(t)]
        own_ref[t, COLS] = (material_ref[:, :, tile_of(t)] + 1).astype(jnp.float32)
    for level in range(moduli_ref.shape[0]):
        levels_ref[level : level + 1, :] = jnp.full((1, LANES), moduli_ref[level], jnp.float32)


def pack_rows(starts, out_refs, refs, flags_ref, ext_x, ext_y, ys):
    for tile, (start_ref, out_ref) in enumerate(zip(starts, out_refs)):
        offset = 2 * tile
        lane = lax.broadcasted_iota(jnp.int32, (COLS, LANES), 1)
        packed = jnp.zeros((COLS, LANES), jnp.float32) if start_ref is None else start_ref[:COLS, :]
        for y in range(ext_y):
            row = slice(COLS + y, COLS + y + 1)
            ids = jnp.zeros((1, LANES), jnp.float32) if start_ref is None else start_ref[row, :]
            for x in range(ext_x) if y in ys else ():
                node = x * ext_y + y
                value = rows_of(refs, flags_ref, tile, x, y, 0, COLS)
                packed = jnp.where(lane // 2 == node, turn(value, 2 * node + offset), packed)
                value = rows_of(refs, flags_ref, tile, x, y, COLS, 1)
                ids = jnp.where(lane[:1] // 2 == x, turn(value, 2 * x + offset), ids)
            out_ref[row, :] = ids
        out_ref[:COLS, :] = packed


def pack_kernel(flags_ref, a_ref, b_ref, c_ref, d_ref, lo0_ref, hi0_ref, lo_ref, hi_ref, ext_x, ext_y):
    refs = (None, None, None, a_ref, b_ref, c_ref, d_ref)
    pack_rows((lo0_ref, hi0_ref), (lo_ref, hi_ref), refs, flags_ref, ext_x, ext_y, OUTER)


def modulus_of(levels_ref, ids):
    modulus = jnp.zeros_like(ids)
    for level in range(levels_ref.shape[0]):
        modulus = jnp.where(ids == level + 1.0, levels_ref[level : level + 1, :], modulus)
    return modulus


def element_weights(e_ref, above_ref, below_ref, both_ref, count):
    ext_x, ext_y = e_ref.shape[:2]
    for ex in range(ext_x - 1):
        flat = []
        for t in range(count):
            both_x = e_ref[ex, :, tile_of(t)] + e_ref[ex + 1, :, tile_of(t)]
            flat.append(both_x + pltpu.roll(both_x, ext_y - 1, 0))
        ahead = shifted(flat, 1)
        weights = [(0.125 * UNIT) * (flat[t] + ahead[t]) for t in range(count)]
        behind = shifted(weights, -1)
        for t in range(count):
            above_ref[ex, :, tile_of(t)] = weights[t]
            below_ref[ex, :, tile_of(t)] = behind[t]
            both_ref[ex, :, tile_of(t)] = weights[t] + behind[t]


def sides_of(*refs):
    return tuple(lambda ex, ey, t, ref=ref: ref[ex, ey : ey + 1, tile_of(t)] for ref in refs)


def first_image(v_ref, low_ref, e_ref, sides, q_ref, qlow_ref, count, ys):
    ext_x, ext_y = low_ref.shape[0], low_ref.shape[1]
    for x in range(1, ext_x - 1):
        for y in ys:
            image = operator(
                lambda t: v_ref[x - 1, y - 1, :, tile_of(t)],
                lambda i, j, t: low_ref[i, j, :, tile_of(t)],
                sides, count, x, y, x, y,
            )
            for t in range(count):
                value = image[t]
                if count == 1 or x in (1, ext_x - 2) or y in (1, ext_y - 2):
                    value = jnp.where(e_ref[x, y : y + 1, tile_of(t)] > 0.0, value, 0.0)
                q_ref[x - 1, y - 1, :, tile_of(t)] = value
                qlow_ref[x - 1, y - 1, :, tile_of(t)] = lowered(value)


def own_nodes(v_ref, q_ref, qlow_ref, sides, count):
    own_x, own_y = v_ref.shape[0], v_ref.shape[1]
    for x in range(1, own_x - 1):
        for y in range(1, own_y - 1):
            image = operator(
                lambda t: q_ref[x, y, :, tile_of(t)],
                lambda i, j, t: qlow_ref[i, j, :, tile_of(t)],
                sides, count, x, y, x + 1, y + 1,
            )
            for t in range(count):
                yield t, v_ref[x, y, :, tile_of(t)], q_ref[x, y, :, tile_of(t)], image[t]


def left_terms(right):
    return jnp.concatenate([right[3 * COLS * n : 3 * COLS * n + 2 * COLS] for n in range(3)], axis=0)


def products(left, right):
    product = lax.dot_general(left, right, (((1,), (1,)), ((), ())), preferred_element_type=jnp.float32)
    rows = sum(product[2 * COLS * n : 2 * COLS * (n + 1)] for n in range(3))
    lane = lax.broadcasted_iota(jnp.int32, (2 * COLS, LANES), 1)
    first = rows[:, :LANES]
    rest = jnp.concatenate([rows[:, LANES:], jnp.zeros((2 * COLS, 2 * LANES - 9 * COLS), jnp.float32)], axis=1)
    third = jnp.where(lane < 2 * COLS, turn(first, -6 * COLS), turn(rest, 2 * COLS))
    return first + turn(first, -3 * COLS) + third


def edge_of(tiles):
    lane = lanes_of(tiles[0])
    return jnp.where(lane < EDGE, tiles[0], jnp.where(lane < 2 * EDGE, turn(tiles[1], 2 * EDGE), 0.0))


def middle_kernel(
    levels_ref, before_ref, own_ref, after_ref,
    v_ref, low_ref, q_ref, qlow_ref, ve_ref, ie_ref, e_ref, lo_ref, hi_ref,
    above_ref, below_ref, both_ref,
):
    ext_x, ext_y = low_ref.shape[0], e_ref.shape[1]
    refs = (before_ref, own_ref, after_ref, None, None, None, None)
    e_ref[...] = jnp.zeros_like(e_ref)
    ie_ref[...] = jnp.zeros_like(ie_ref)
    for x in range(ext_x):
        for y in MIDDLE:
            tiles = [rows_of(refs, None, t, x, y, COLS, 1) for t in range(2)]
            ie_ref[x, y - 2 : y - 1, :] = edge_of(tiles)
            for t in range(2):
                e_ref[x, y - 2 : y - 1, tile_of(t)] = tiles[t]
            tiles = [rows_of(refs, None, t, x, y, 0, COLS) for t in range(2)]
            ve_ref[x, y - 2] = edge_of(tiles)
            for t in range(2):
                low_ref[x, y - 2, :, tile_of(t)] = lowered(tiles[t])
                if 0 < x < ext_x - 1:
                    v_ref[x - 1, y - 2, :, tile_of(t)] = tiles[t]
        for t in range(2):
            e_ref[x, :, tile_of(t)] = modulus_of(levels_ref, e_ref[x, :, tile_of(t)])
    pack_rows((None, None), (lo_ref, hi_ref), refs, None, ext_x, ext_y, MIDDLE)
    element_weights(e_ref, above_ref, below_ref, both_ref, 2)
    sides = sides_of(above_ref, below_ref, both_ref)
    for x in range(1, ext_x - 1):
        for y in (1, 2):
            image = operator(
                lambda t: v_ref[x - 1, y, :, tile_of(t)],
                lambda i, j, t: low_ref[i, j, :, tile_of(t)],
                sides, 2, x, y, x, y,
            )
            for t in range(2):
                value = image[t]
                if x in (1, ext_x - 2):
                    value = jnp.where(e_ref[x, y : y + 1, tile_of(t)] > 0.0, value, 0.0)
                q_ref[x - 1, y - 1, :, tile_of(t)] = value
                qlow_ref[x - 1, y - 1, :, tile_of(t)] = lowered(value)


def main_kernel(
    levels_ref, flags_ref, a_ref, b_ref, c_ref, d_ref,
    vm_ref, lowm_ref, qm_ref, qlowm_ref, vem_ref, iem_ref, em_ref,
    v_ref, q_ref, above_ref, below_ref, both_ref, total_ref, ve_ref, ie_ref,
    low_ref, qlow_ref, e_ref, left_ref, right_ref,
):
    ext_x, ext_y = low_ref.shape[0], low_ref.shape[1]
    refs = (None, None, None, a_ref, b_ref, c_ref, d_ref)
    for x in range(ext_x):
        ie_ref[x, 2:6, :] = iem_ref[x, 0:4, :]
        for y in OUTER:
            tiles = [rows_of(refs, flags_ref, t, x, y, COLS, 1) for t in range(2)]
            ie_ref[x, y : y + 1, :] = edge_of(tiles)
            for t in range(2):
                e_ref[x, y : y + 1, tile_of(t)] = tiles[t]
        for t in range(2):
            e_ref[x, 2:6, tile_of(t)] = jnp.zeros((4, LANES), jnp.float32)
            e_ref[x, :, tile_of(t)] = modulus_of(levels_ref, e_ref[x, :, tile_of(t)])
            e_ref[x, 2:6, tile_of(t)] = em_ref[x, 0:4, tile_of(t)]
    element_weights(e_ref, above_ref, below_ref, both_ref, 2)
    for x in range(ext_x):
        for y in range(ext_y):
            inner = 0 < x < ext_x - 1 and 0 < y < ext_y - 1
            if y in MIDDLE:
                ve_ref[x, y] = vem_ref[x, y - 2]
                low_ref[x, y] = lowm_ref[x, y - 2]
                if inner:
                    v_ref[x - 1, y - 1] = vm_ref[x - 1, y - 2]
                if inner and y in (3, 4):
                    q_ref[x - 1, y - 1] = qm_ref[x - 1, y - 3]
                    qlow_ref[x - 1, y - 1] = qlowm_ref[x - 1, y - 3]
                continue
            tiles = [rows_of(refs, flags_ref, t, x, y, 0, COLS) for t in range(2)]
            ve_ref[x, y] = edge_of(tiles)
            for t in range(2):
                low_ref[x, y, :, tile_of(t)] = lowered(tiles[t])
                if inner:
                    v_ref[x - 1, y - 1, :, tile_of(t)] = tiles[t]
    sides = sides_of(above_ref, below_ref, both_ref)
    first_image(v_ref, low_ref, e_ref, sides, q_ref, qlow_ref, 2, (1, 2, 5, 6))
    for n, (t, b, q, w) in enumerate(own_nodes(v_ref, q_ref, qlow_ref, sides, 2)):
        right = split_terms(jnp.concatenate([b, q, w], axis=0), 3)
        left = left_terms(right)
        here = lanes_of(left) >= 2 if t == 0 else lanes_of(left) < LANES - 2
        left_ref[:, tile_of(n)] = jnp.where(here, left, jnp.zeros_like(left))
        right_ref[:, tile_of(n)] = right
    total_ref[...] = products(left_ref[...], right_ref[...])


def edge_kernel(
    levels_ref, total_ref, ve_ref, ie_ref, before_ref, after_ref,
    v_ref, q_ref, above_ref, below_ref, both_ref, g_ref,
    low_ref, qlow_ref, e_ref,
):
    ext_x, ext_y = low_ref.shape[0], low_ref.shape[1]

    def with_ends(own, before, after, index):
        lane = lanes_of(own)
        follows, comes = turn(after, LANES // 2 - 2 * index), turn(before, LANES - 2 - 2 * index)
        value = jnp.where(lane >= LANES - 2, comes, own)
        return jnp.where((lane >= LANES // 2) & (lane < LANES // 2 + 2), follows, value)

    for x in range(ext_x):
        ids = with_ends(ie_ref[x], before_ref[COLS : COLS + ext_y, :], after_ref[COLS : COLS + ext_y, :], x)
        e_ref[x] = modulus_of(levels_ref, ids)
    element_weights(e_ref, above_ref, below_ref, both_ref, 1)
    before, after = before_ref[:COLS, :], after_ref[:COLS, :]
    for x in range(ext_x):
        for y in range(ext_y):
            value = with_ends(ve_ref[x, y], before, after, x * ext_y + y)
            low_ref[x, y] = lowered(value)
            if 0 < x < ext_x - 1 and 0 < y < ext_y - 1:
                v_ref[x - 1, y - 1] = value
    sides = sides_of(above_ref, below_ref, both_ref)
    first_image(v_ref, low_ref, e_ref, sides, q_ref, qlow_ref, 1, range(1, ext_y - 1))
    right = jnp.zeros((3 * COLS, LANES), jnp.float32)
    for n, (_, b, q, w) in enumerate(own_nodes(v_ref, q_ref, qlow_ref, sides, 1)):
        three = jnp.concatenate([b, q, w], axis=0)
        at = lanes_of(three) - 2 * n
        here = ((at >= 0) & (at < 2)) | ((at >= 2 * EDGE - 2) & (at < 2 * EDGE))
        right = jnp.where(here, turn(three, 2 * n), right)
    right = split_terms(right, 3)
    total = products(left_terms(right), right)
    g_ref[...] = pack_moments(total_ref[...] + total)


def pack_moments(total):
    first, second = total[:COLS], total[COLS:]
    row = lax.broadcasted_iota(jnp.int32, (COLS, LANES), 0)
    lane = lax.broadcasted_iota(jnp.int32, (COLS, LANES), 1)
    col = lane % COLS
    upper = jnp.where(lane < COLS, first, second)
    lower = jnp.where(
        lane < COLS,
        0.5 * (pltpu.roll(first, LANES - COLS, 1) + second),
        pltpu.roll(second, LANES - COLS, 1),
    )
    valid = lane < 2 * COLS
    square = jnp.where(valid, jnp.where(row <= col, upper, lower), 0.0)
    diagonal = jnp.sum(jnp.where(valid & (row == col), lower, 0.0), axis=0, keepdims=True)
    out = []
    for half in range(2):
        out.append(square[8 * half : 8 * half + 8])
    spread_rows = jnp.zeros((8, LANES), jnp.float32)
    sub8 = lax.broadcasted_iota(jnp.int32, (8, LANES), 0)
    lane8 = lax.broadcasted_iota(jnp.int32, (8, LANES), 1)
    for quarter in range(4):
        piece = out[quarter // 2]
        if quarter % 2:
            piece = pltpu.roll(piece, 4, 0)
        if quarter:
            piece = pltpu.roll(piece, 2 * COLS * quarter, 1)
        here = (sub8 < 4) & (lane8 // (2 * COLS) == quarter)
        spread_rows = jnp.where(here, piece, spread_rows)
    return jnp.where(sub8 == 4, diagonal, spread_rows)


def unpack_moments(packed):
    sub8 = lax.broadcasted_iota(jnp.int32, (8, LANES), 0)
    halves = []
    for half in range(2):
        a, b = 2 * half, 2 * half + 1
        top = pltpu.roll(packed, LANES - 2 * COLS * a, 1) if a else packed
        bottom = pltpu.roll(pltpu.roll(packed, LANES - 2 * COLS * b, 1), 4, 0)
        halves.append(jnp.where(sub8 < 4, top, bottom))
    square = jnp.concatenate(halves, axis=0)
    row = lax.broadcasted_iota(jnp.int32, (COLS, COLS), 0)
    col = lax.broadcasted_iota(jnp.int32, (COLS, COLS), 1)
    moments = []
    for pair in range(2):
        turned = pltpu.roll(square, LANES - COLS, 1) if pair else square
        mixed = turned[:, :COLS]
        diagonal = (pltpu.roll(packed, LANES - COLS, 1) if pair else packed)[4:5, :COLS]
        flipped = mixed.T
        moments.append(jnp.where(row <= col, mixed, flipped))
        lower = jnp.where(row == col, diagonal, jnp.where(row > col, mixed, flipped))
        moments.append(lower)
    return moments


def dot(left, right, dims=((1,), (0,))):
    return lax.dot_general(left, right, (dims, ((), ())), precision=HIGH, preferred_element_type=jnp.float32)


def replicated(matrix):
    return [jnp.broadcast_to(matrix[:, i : i + 1], (COLS, LANES)) for i in range(COLS)]


def sweeps(rows):
    rows = list(rows)
    sub = lax.broadcasted_iota(jnp.int32, (COLS, LANES), 0)
    for k in range(COLS):
        scale = 1.0 / rows[k][k : k + 1, :]
        pivot_row = rows[k] * scale
        for i in range(COLS):
            if i != k:
                factor = rows[i][k : k + 1, :]
                moved = rows[i] - factor * pivot_row
                rows[i] = jnp.where(sub == k, factor * scale, moved)
        rows[k] = jnp.where(sub == k, -scale, pivot_row)
        yield rows


def times(rows, right):
    parts = [rows[i] * right[i : i + 1, :] for i in range(COLS)]
    while len(parts) > 1:
        parts = [a + b for a, b in zip(parts[::2], parts[1::2])]
    return parts[0]


def mixer(coeffs, count):
    flipped = split_terms(coeffs.T, count)
    return jnp.concatenate([flipped] * count, axis=1)


def mixed(left, block, count):
    out = jnp.dot(left, split_terms(block, count), preferred_element_type=jnp.float32)
    size = out.shape[0] // count
    return sum(out[size * n : size * (n + 1)] for n in range(count))


def finish_kernel(
    g_ref, v_ref, q_ref, above_ref, below_ref, both_ref,
    ve_ref, qe_ref, abovee_ref, belowe_ref, bothe_ref,
    sol_ref, res_ref, d_ref, dlow_ref, w0_ref, w1_ref, w2_ref,
):
    own_x, own_y = v_ref.shape[0], v_ref.shape[1]
    m0, m1, m2, m3 = unpack_moments(g_ref[...])
    first = ((0,), (0,))
    padding = jnp.zeros((COLS, LANES - COLS), jnp.float32)
    *_, minus_inv = sweeps(replicated(m1))
    minus_alpha = times(minus_inv, jnp.concatenate([m0, padding], axis=1))
    minus_m2a = times(replicated(m2), minus_alpha)
    mix = times(minus_inv, minus_m2a)[:, :COLS]
    minus_m3a = times(replicated(m3), minus_alpha)[:, :COLS]
    minus_alpha, minus_m2a = minus_alpha[:, :COLS], minus_m2a[:, :COLS]
    alpha = -minus_alpha
    left = mixer(jnp.concatenate([mix, minus_alpha], axis=0), 3)
    updated = dot(minus_alpha, minus_m2a, first) - m0
    curved = dot(minus_alpha, minus_m3a, first) + dot(minus_m2a, mix, first)
    steps = sweeps(replicated(0.5 * (curved + curved.T)))
    minus_inv = None
    for x in range(own_x):
        for y in range(own_y):
            q0, q1, qe = q_ref[x, y, :, :LANES], q_ref[x, y, :, LANES:], qe_ref[x, y]
            lane = lanes_of(qe)
            q0 = jnp.where(lane == 0, qe, q0)
            q1 = jnp.where(lane == LANES - 1, turn(qe, LANES // 2), q1)
            block = jnp.concatenate(
                [
                    jnp.concatenate([v_ref[x, y], ve_ref[x, y]], axis=1),
                    jnp.concatenate([q0, q1, qe], axis=1),
                ],
                axis=0,
            )
            value = mixed(left, block, 3)
            d_ref[x, y] = value
            dlow_ref[x, y] = lowered(value)
            minus_inv = next(steps, minus_inv)
    gamma = -times(minus_inv, jnp.concatenate([updated, padding], axis=1))[:, :COLS]
    edge, main = (abovee_ref, belowe_ref, bothe_ref), (above_ref, below_ref, both_ref)
    whole = (w0_ref, w1_ref, w2_ref)
    for end_ref, main_ref, whole_ref in zip(edge, main, whole):
        for ex in range(1, own_x):
            end = end_ref[ex]
            lane = lanes_of(end)
            whole_ref[ex, :, :LANES] = jnp.where(lane == 0, end, main_ref[ex, :, :LANES])
            end = turn(end, LANES // 2)
            whole_ref[ex, :, LANES:] = jnp.where(lane == LANES - 1, end, main_ref[ex, :, LANES:])
    main, edge = sides_of(*whole), sides_of(*edge)
    zero = jnp.zeros((COLS, COLS), jnp.float32)
    last = mixer(
        jnp.concatenate(
            [
                jnp.concatenate([alpha, gamma, zero, zero], axis=0),
                jnp.concatenate([zero, zero, -alpha, -gamma], axis=0),
            ],
            axis=1,
        ),
        3,
    )
    for x in range(1, own_x - 1):
        for y in range(1, own_y - 1):
            low = lambda i, j, t: dlow_ref[i, j, :, tile_of(t)]
            at = (x, y, x + 1, y + 1)
            plane, down, up = zip(*[terms(low, main, t, *at) for t in range(2)])
            ends = terms(lambda i, j, t: dlow_ref[i, j, :, tile_of(2)], edge, 0, *at)
            from_above = shifted(down, 1, turn(ends[1], LANES // 2))
            from_below = shifted(up, -1, ends[2])
            image = [
                SIGMA * d_ref[x, y, :, tile_of(t)] + (plane[t] - from_above[t] - from_below[t])
                for t in range(2)
            ]
            q0, q1, qe = q_ref[x, y, :, :LANES], q_ref[x, y, :, LANES:], qe_ref[x, y]
            lane = lanes_of(qe)
            q0 = jnp.where(lane == 0, qe, q0)
            q1 = jnp.where(lane == LANES - 1, turn(qe, LANES // 2), q1)
            b = v_ref[x, y]
            block = jnp.concatenate(
                [
                    b,
                    d_ref[x, y, :, : 2 * LANES],
                    jnp.concatenate([q0, q1], axis=1),
                    jnp.concatenate(image, axis=1),
                ],
                axis=0,
            )
            out = mixed(last, block, 3)
            sol_ref[:, x - 1, y - 1, :] = out[:COLS]
            res_ref[:, x - 1, y - 1, :] = b + out[COLS:]


def both_ways(axis, to_next, to_last, around=False):
    count = lax.axis_size(axis)
    steps = range(count) if around else range(count - 1)
    before = lax.ppermute(to_next, axis, [(i, (i + 1) % count) for i in steps])
    after = lax.ppermute(to_last, axis, [((i + 1) % count, i) for i in steps])
    return before, after


def spread(value, axes, root):
    count = lax.axis_size(axes)
    copies = jnp.broadcast_to(value[None], (count, *value.shape))
    group = [(root + i) % count for i in range(count)]
    return jnp.sum(lax.all_to_all(copies, axes, 0, 0, axis_index_groups=[group]), axis=0)


def near(value):
    return pltpu.with_memory_space_constraint(value, pltpu.VMEM)


def on_device(loads, moduli, material):
    f32, bf16, wide = jnp.float32, jnp.bfloat16, 2 * LANES
    own_x, own_y = material.shape[:2]
    ext_x, ext_y = own_x + 4, own_y + 4
    own, levels = pl.pallas_call(
        front_kernel,
        out_shape=(
            pltpu.VMEM((2, COLS + 1, own_x, own_y, LANES), f32),
            pltpu.VMEM((moduli.shape[0], LANES), f32),
        ),
        in_specs=[
            pl.BlockSpec(memory_space=pltpu.SMEM),
            pl.BlockSpec(memory_space=pltpu.VMEM),
            pl.BlockSpec(memory_space=pltpu.VMEM),
        ],
        name="front",
    )(moduli, loads, material)
    place = lax.axis_index(GY)
    row = lax.broadcasted_iota(jnp.int32, (8, LANES), 0)
    flags = jnp.where(row == 0, place > 0, place < lax.axis_size(GY) - 1).astype(f32)
    before, after = both_ways("gx", own, own)
    part = jnp.concatenate([before, own], axis=2)
    parts = part[:, :, :, 2:], part[:, :, :, :2]
    sides = both_ways(GY, *parts, around=True)
    lasts = both_ways(GY, after[:, :, :, 2:], after[:, :, :, :2], around=True)
    line = [near(v.reshape(-1, LANES)) for v in (before, own, after)]
    flat = [near(v.reshape(-1, LANES)) for v in (sides[0], lasts[0], sides[1], lasts[1])]
    levels, flags = near(levels), near(flags)
    ends = (pltpu.VMEM((COLS + 8, LANES), f32),) * 2

    def block(xs, ys, size):
        return pltpu.VMEM((xs, ys, COLS, size), f32)

    *mid, lo, hi = pl.pallas_call(
        middle_kernel,
        out_shape=(
            block(ext_x - 2, own_y, wide),
            block(ext_x, own_y, wide),
            block(ext_x - 2, own_y - 2, wide),
            block(ext_x - 2, own_y - 2, wide),
            block(ext_x, own_y, LANES),
            pltpu.VMEM((ext_x, ext_y, LANES), f32),
            pltpu.VMEM((ext_x, ext_y, wide), f32),
            *ends,
        ),
        scratch_shapes=[pltpu.VMEM((ext_x - 1, ext_y, wide), f32)] * 3,
        compiler_params=GRANT,
        name="middle",
    )(levels, *line)
    first, last = pl.pallas_call(
        functools.partial(pack_kernel, ext_x=ext_x, ext_y=ext_y), out_shape=ends, compiler_params=GRANT, name="pack"
    )(flags, *flat, near(lo), near(hi))
    before, after = both_ways("gz", last, first)
    nodes = own_x * own_y

    def weights(size):
        return (pltpu.VMEM((ext_x - 1, ext_y, size), f32),) * 3

    def fields(size):
        return (pltpu.VMEM((ext_x - 2, ext_y - 2, COLS, size), f32),) * 2

    def scratch(size):
        return [
            pltpu.VMEM((ext_x, ext_y, COLS, size), f32),
            pltpu.VMEM((ext_x - 2, ext_y - 2, COLS, size), f32),
            pltpu.VMEM((ext_x, ext_y, size), f32),
        ]

    *main, total, edge, ids = pl.pallas_call(
        main_kernel,
        out_shape=(
            *fields(wide),
            *weights(wide),
            pltpu.VMEM((2 * COLS, LANES), f32),
            pltpu.VMEM((ext_x, ext_y, COLS, LANES), f32),
            pltpu.VMEM((ext_x, ext_y, LANES), f32),
        ),
        scratch_shapes=scratch(wide)
        + [pltpu.VMEM((6 * COLS, nodes * wide), bf16), pltpu.VMEM((9 * COLS, nodes * wide), bf16)],
        compiler_params=GRANT,
        name="main",
    )(levels, flags, *flat, *[near(v) for v in mid])
    *edges, moments = pl.pallas_call(
        edge_kernel,
        out_shape=(*fields(LANES), *weights(LANES), pltpu.VMEM((8, LANES), f32)),
        scratch_shapes=scratch(LANES),
        compiler_params=GRANT,
        name="edge",
    )(*[near(value) for value in (levels, total, edge, ids, before, after)])
    rows = 5
    length, chips = lax.axis_size("gz"), lax.axis_size("gy_0")
    moments = spread(moments[:rows].reshape(rows, 1, LANES), "gz", 17 * length // 32)
    middle = (lax.axis_size("gx") // 2 * chips + chips // 2) * 2 + 1
    moments = spread(moments, PLANE, middle).reshape(rows, LANES)
    moments = jnp.concatenate([moments, jnp.zeros((8 - rows, LANES), f32)], axis=0)
    out = jax.ShapeDtypeStruct(loads.shape, f32)
    return pl.pallas_call(
        finish_kernel,
        out_shape=(out, out),
        scratch_shapes=[pltpu.VMEM((ext_x - 2, ext_y - 2, COLS, 3 * LANES), f32)] * 2
        + [pltpu.VMEM((ext_x - 1, ext_y, wide), f32)] * 3,
        compiler_params=GRANT,
        name="finish",
    )(*[near(value) for value in (moments, *main, *edges)])


def solution(mesh):
    chips, long = mesh.shape["gy"] // 2, mesh.shape["gz"]
    split = Mesh(mesh.devices.reshape(mesh.shape["gx"], chips, 2, long), ("gx", "gy_0", "gy_1", "gz"))
    spec = P(None, "gx", GY, "gz")

    return jax.shard_map(
        on_device,
        mesh=split,
        in_specs=(spec, P(), P("gx", GY, "gz")),
        out_specs=(spec, spec),
        check_vma=False,
    )
```

```python
import functools

import jax
import jax.numpy as jnp
import numpy as np
from jax import lax
from jax.experimental import pallas as pl
from jax.experimental.pallas import tpu as pltpu
from jax.sharding import Mesh
from jax.sharding import PartitionSpec as P

PLANE = ("gx", "gy_0", "gy_1")
GY = ("gy_0", "gy_1")
SIGMA = 0.25
COLS = 16
LANES = 128
EDGE = LANES // 4
HIGH = lax.Precision.HIGHEST
GRANT = pltpu.CompilerParams(vmem_limit_bytes=16 * 2**20)


def stiffness_table():
    line_mass = np.array([[1.0 / 3.0, 1.0 / 6.0], [1.0 / 6.0, 1.0 / 3.0]])
    line_stiff = np.array([[1.0, -1.0], [-1.0, 1.0]])
    table = np.zeros((8, 8))
    for target in range(8):
        for source in range(8):
            target_bits = [target >> 2 & 1, target >> 1 & 1, target & 1]
            source_bits = [source >> 2 & 1, source >> 1 & 1, source & 1]
            total = 0.0
            for stiff_dim in range(3):
                factor = 1.0
                for other in range(3):
                    if other == stiff_dim:
                        factor = factor * line_stiff[target_bits[other], source_bits[other]]
                    else:
                        factor = factor * line_mass[target_bits[other], source_bits[other]]
                total = total + factor
            table[target, source] = total
    return table


def kernel_scale():
    table = np.asarray(jnp.asarray(stiffness_table(), jnp.bfloat16).astype(jnp.float32))
    unit = -float(table[0, 7])
    for target in range(8):
        for source in range(8):
            bits = bin(target ^ source).count("1")
            want = (4.0, 0.0, -1.0, -1.0)[bits] * unit
            assert abs(float(table[target, source]) - want) < 1e-12
    return unit


UNIT = kernel_scale()


def lowered(value):
    return value.astype(jnp.bfloat16).astype(jnp.float32)


MIDDLE = (2, 3, 4, 5)
OUTER = (0, 1, 6, 7)


def tile_of(tile):
    return slice(tile * LANES, (tile + 1) * LANES)


def lanes_of(value):
    return lax.broadcasted_iota(jnp.int32, value.shape, 1)


def turn(value, amount):
    amount %= LANES
    return pltpu.roll(value, amount, 1) if amount else value


def shifted(tiles, step, beyond=None):
    count = len(tiles)
    turned = [turn(t, -step) for t in tiles]
    past = turn(beyond, -step) if beyond is not None else turned[0 if step > 0 else -1]
    lane = lanes_of(tiles[0])
    if step > 0:
        return [jnp.where(lane < LANES - 1, turned[i], turned[i + 1] if i + 1 < count else past) for i in range(count)]
    return [jnp.where(lane > 0, turned[i], turned[i - 1] if i else past) for i in range(count)]


def terms(low, sides, tile, x, y, wx, wy):
    above, below, both = sides
    around = {(i, j): low(x + i, y + j, tile) for i in (-1, 0, 1) for j in (-1, 0, 1)}
    total = None
    for i in (-1, 1):
        for j in (-1, 1):
            ex, ey = wx + (i - 1) // 2, wy + (j - 1) // 2
            others = around[i, 0] + around[0, j] + around[i, j]
            new = (
                both(ex, ey, tile) * around[i, j],
                below(ex, ey, tile) * others,
                above(ex, ey, tile) * others,
            )
            total = new if total is None else tuple(a + b for a, b in zip(total, new))
    rim = [both(wx + i, wy + j, tile) for i in (-1, 0) for j in (-1, 0)]
    centre = (4.0 * ((rim[0] + rim[1]) + (rim[2] + rim[3]))) * around[0, 0]
    return centre - total[0], total[1], total[2]


def operator(field, low, sides, count, x, y, wx, wy):
    plane, down, up = zip(*[terms(low, sides, t, x, y, wx, wy) for t in range(count)])
    from_above, from_below = shifted(down, 1), shifted(up, -1)
    return [SIGMA * field(t) + (plane[t] - from_above[t] - from_below[t]) for t in range(count)]


def split_terms(value, count):
    parts = []
    for n in range(count):
        part = value.astype(jnp.bfloat16)
        parts.append(part)
        if n + 1 < count:
            value = value - part.astype(jnp.float32)
    return jnp.concatenate(parts, axis=0)


def rows_of(refs, flags_ref, tile, x, y, first, count):
    before_x_ref, own_ref, after_x_ref, before_ref, before_last_ref, after_ref, after_last_ref = refs
    flag = None
    if 2 <= y < 6:
        ref, column, wide, tall, at = (before_x_ref, own_ref, after_x_ref)[x // 2], x % 2, 2, 4, y - 2
    else:
        low = y < 2
        flag, at, tall = (0, y, 2) if low else (1, y - 6, 2)
        if x < 4:
            ref, column, wide = before_ref if low else after_ref, x, 4
        else:
            ref, column, wide = before_last_ref if low else after_last_ref, x - 4, 2
    stride = wide * tall
    start = tile * (ref.shape[0] // 2) + first * stride + column * tall + at
    value = ref[pl.ds(start, count, stride=stride), :] if count > 1 else ref[start : start + 1, :]
    if flag is not None:
        value = jnp.where(flags_ref[flag : flag + 1, :] > 0.0, value, 0.0)
    return value


def front_kernel(moduli_ref, loads_ref, material_ref, own_ref, levels_ref):
    for t in range(2):
        own_ref[t, :COLS] = loads_ref[:, :, :, tile_of(t)]
        own_ref[t, COLS] = (material_ref[:, :, tile_of(t)] + 1).astype(jnp.float32)
    for level in range(moduli_ref.shape[0]):
        levels_ref[level : level + 1, :] = jnp.full((1, LANES), moduli_ref[level], jnp.float32)


def pack_rows(starts, out_refs, refs, flags_ref, ext_x, ext_y, ys):
    for tile, (start_ref, out_ref) in enumerate(zip(starts, out_refs)):
        offset = 2 * tile
        lane = lax.broadcasted_iota(jnp.int32, (COLS, LANES), 1)
        packed = jnp.zeros((COLS, LANES), jnp.float32) if start_ref is None else start_ref[:COLS, :]
        for y in range(ext_y):
            row = slice(COLS + y, COLS + y + 1)
            ids = jnp.zeros((1, LANES), jnp.float32) if start_ref is None else start_ref[row, :]
            for x in range(ext_x) if y in ys else ():
                node = x * ext_y + y
                value = rows_of(refs, flags_ref, tile, x, y, 0, COLS)
                packed = jnp.where(lane // 2 == node, turn(value, 2 * node + offset), packed)
                value = rows_of(refs, flags_ref, tile, x, y, COLS, 1)
                ids = jnp.where(lane[:1] // 2 == x, turn(value, 2 * x + offset), ids)
            out_ref[row, :] = ids
        out_ref[:COLS, :] = packed


def pack_kernel(flags_ref, a_ref, b_ref, c_ref, d_ref, lo0_ref, hi0_ref, lo_ref, hi_ref, ext_x, ext_y):
    refs = (None, None, None, a_ref, b_ref, c_ref, d_ref)
    pack_rows((lo0_ref, hi0_ref), (lo_ref, hi_ref), refs, flags_ref, ext_x, ext_y, OUTER)


def total_kernel(flags_ref, parts_ref, out_ref, count):
    rows = parts_ref.shape[0] // count
    sub = lax.broadcasted_iota(jnp.int32, (8, LANES), 0)
    out = jnp.zeros((8, LANES), jnp.float32)
    for row in range(rows):
        part = jnp.sum(parts_ref[pl.ds(row, count, stride=rows), :], axis=0, keepdims=True)
        out = jnp.where(sub == row, part, out)
    out_ref[...] = jnp.where(flags_ref[2:3, :] > 0.0, out, 0.0)


def modulus_of(levels_ref, ids):
    modulus = jnp.zeros_like(ids)
    for level in range(levels_ref.shape[0]):
        modulus = jnp.where(ids == level + 1.0, levels_ref[level : level + 1, :], modulus)
    return modulus


def element_weights(e_ref, above_ref, below_ref, both_ref, count):
    ext_x, ext_y = e_ref.shape[:2]
    for ex in range(ext_x - 1):
        flat = []
        for t in range(count):
            both_x = e_ref[ex, :, tile_of(t)] + e_ref[ex + 1, :, tile_of(t)]
            flat.append(both_x + pltpu.roll(both_x, ext_y - 1, 0))
        ahead = shifted(flat, 1)
        weights = [(0.125 * UNIT) * (flat[t] + ahead[t]) for t in range(count)]
        behind = shifted(weights, -1)
        for t in range(count):
            above_ref[ex, :, tile_of(t)] = weights[t]
            below_ref[ex, :, tile_of(t)] = behind[t]
            both_ref[ex, :, tile_of(t)] = weights[t] + behind[t]


def sides_of(*refs):
    return tuple(lambda ex, ey, t, ref=ref: ref[ex, ey : ey + 1, tile_of(t)] for ref in refs)


def first_image(v_ref, low_ref, e_ref, sides, q_ref, qlow_ref, count, ys):
    ext_x, ext_y = low_ref.shape[0], low_ref.shape[1]
    for x in range(1, ext_x - 1):
        for y in ys:
            image = operator(
                lambda t: v_ref[x - 1, y - 1, :, tile_of(t)],
                lambda i, j, t: low_ref[i, j, :, tile_of(t)],
                sides, count, x, y, x, y,
            )
            for t in range(count):
                value = image[t]
                if count == 1 or x in (1, ext_x - 2) or y in (1, ext_y - 2):
                    value = jnp.where(e_ref[x, y : y + 1, tile_of(t)] > 0.0, value, 0.0)
                q_ref[x - 1, y - 1, :, tile_of(t)] = value
                qlow_ref[x - 1, y - 1, :, tile_of(t)] = lowered(value)


def own_nodes(v_ref, q_ref, qlow_ref, sides, count):
    own_x, own_y = v_ref.shape[0], v_ref.shape[1]
    for x in range(1, own_x - 1):
        for y in range(1, own_y - 1):
            image = operator(
                lambda t: q_ref[x, y, :, tile_of(t)],
                lambda i, j, t: qlow_ref[i, j, :, tile_of(t)],
                sides, count, x, y, x + 1, y + 1,
            )
            for t in range(count):
                yield t, v_ref[x, y, :, tile_of(t)], q_ref[x, y, :, tile_of(t)], image[t]


def left_terms(right):
    return jnp.concatenate([right[3 * COLS * n : 3 * COLS * n + 2 * COLS] for n in range(3)], axis=0)


def products(left, right):
    product = lax.dot_general(left, right, (((1,), (1,)), ((), ())), preferred_element_type=jnp.float32)
    rows = sum(product[2 * COLS * n : 2 * COLS * (n + 1)] for n in range(3))
    lane = lax.broadcasted_iota(jnp.int32, (2 * COLS, LANES), 1)
    first = rows[:, :LANES]
    rest = jnp.concatenate([rows[:, LANES:], jnp.zeros((2 * COLS, 2 * LANES - 9 * COLS), jnp.float32)], axis=1)
    third = jnp.where(lane < 2 * COLS, turn(first, -6 * COLS), turn(rest, 2 * COLS))
    return first + turn(first, -3 * COLS) + third


def edge_of(tiles):
    lane = lanes_of(tiles[0])
    return jnp.where(lane < EDGE, tiles[0], jnp.where(lane < 2 * EDGE, turn(tiles[1], 2 * EDGE), 0.0))


def middle_kernel(
    levels_ref, before_ref, own_ref, after_ref,
    v_ref, low_ref, q_ref, qlow_ref, ve_ref, ie_ref, e_ref, lo_ref, hi_ref,
    above_ref, below_ref, both_ref,
):
    ext_x, ext_y = low_ref.shape[0], e_ref.shape[1]
    refs = (before_ref, own_ref, after_ref, None, None, None, None)
    e_ref[...] = jnp.zeros_like(e_ref)
    ie_ref[...] = jnp.zeros_like(ie_ref)
    for x in range(ext_x):
        for y in MIDDLE:
            tiles = [rows_of(refs, None, t, x, y, COLS, 1) for t in range(2)]
            ie_ref[x, y - 2 : y - 1, :] = edge_of(tiles)
            for t in range(2):
                e_ref[x, y - 2 : y - 1, tile_of(t)] = tiles[t]
            tiles = [rows_of(refs, None, t, x, y, 0, COLS) for t in range(2)]
            ve_ref[x, y - 2] = edge_of(tiles)
            for t in range(2):
                low_ref[x, y - 2, :, tile_of(t)] = lowered(tiles[t])
                if 0 < x < ext_x - 1:
                    v_ref[x - 1, y - 2, :, tile_of(t)] = tiles[t]
        for t in range(2):
            e_ref[x, :, tile_of(t)] = modulus_of(levels_ref, e_ref[x, :, tile_of(t)])
    pack_rows((None, None), (lo_ref, hi_ref), refs, None, ext_x, ext_y, MIDDLE)
    element_weights(e_ref, above_ref, below_ref, both_ref, 2)
    sides = sides_of(above_ref, below_ref, both_ref)
    for x in range(1, ext_x - 1):
        for y in (1, 2):
            image = operator(
                lambda t: v_ref[x - 1, y, :, tile_of(t)],
                lambda i, j, t: low_ref[i, j, :, tile_of(t)],
                sides, 2, x, y, x, y,
            )
            for t in range(2):
                value = image[t]
                if x in (1, ext_x - 2):
                    value = jnp.where(e_ref[x, y : y + 1, tile_of(t)] > 0.0, value, 0.0)
                q_ref[x - 1, y - 1, :, tile_of(t)] = value
                qlow_ref[x - 1, y - 1, :, tile_of(t)] = lowered(value)


def main_kernel(
    levels_ref, flags_ref, a_ref, b_ref, c_ref, d_ref,
    vm_ref, lowm_ref, qm_ref, qlowm_ref, vem_ref, iem_ref, em_ref,
    v_ref, q_ref, above_ref, below_ref, both_ref, total_ref, ve_ref, ie_ref,
    low_ref, qlow_ref, e_ref, left_ref, right_ref,
):
    ext_x, ext_y = low_ref.shape[0], low_ref.shape[1]
    refs = (None, None, None, a_ref, b_ref, c_ref, d_ref)
    for x in range(ext_x):
        ie_ref[x, 2:6, :] = iem_ref[x, 0:4, :]
        for y in OUTER:
            tiles = [rows_of(refs, flags_ref, t, x, y, COLS, 1) for t in range(2)]
            ie_ref[x, y : y + 1, :] = edge_of(tiles)
            for t in range(2):
                e_ref[x, y : y + 1, tile_of(t)] = tiles[t]
        for t in range(2):
            e_ref[x, 2:6, tile_of(t)] = jnp.zeros((4, LANES), jnp.float32)
            e_ref[x, :, tile_of(t)] = modulus_of(levels_ref, e_ref[x, :, tile_of(t)])
            e_ref[x, 2:6, tile_of(t)] = em_ref[x, 0:4, tile_of(t)]
    element_weights(e_ref, above_ref, below_ref, both_ref, 2)
    for x in range(ext_x):
        for y in range(ext_y):
            inner = 0 < x < ext_x - 1 and 0 < y < ext_y - 1
            if y in MIDDLE:
                ve_ref[x, y] = vem_ref[x, y - 2]
                low_ref[x, y] = lowm_ref[x, y - 2]
                if inner:
                    v_ref[x - 1, y - 1] = vm_ref[x - 1, y - 2]
                if inner and y in (3, 4):
                    q_ref[x - 1, y - 1] = qm_ref[x - 1, y - 3]
                    qlow_ref[x - 1, y - 1] = qlowm_ref[x - 1, y - 3]
                continue
            tiles = [rows_of(refs, flags_ref, t, x, y, 0, COLS) for t in range(2)]
            ve_ref[x, y] = edge_of(tiles)
            for t in range(2):
                low_ref[x, y, :, tile_of(t)] = lowered(tiles[t])
                if inner:
                    v_ref[x - 1, y - 1, :, tile_of(t)] = tiles[t]
    sides = sides_of(above_ref, below_ref, both_ref)
    first_image(v_ref, low_ref, e_ref, sides, q_ref, qlow_ref, 2, (1, 2, 5, 6))
    for n, (t, b, q, w) in enumerate(own_nodes(v_ref, q_ref, qlow_ref, sides, 2)):
        right = split_terms(jnp.concatenate([b, q, w], axis=0), 3)
        left = left_terms(right)
        here = lanes_of(left) >= 2 if t == 0 else lanes_of(left) < LANES - 2
        left_ref[:, tile_of(n)] = jnp.where(here, left, jnp.zeros_like(left))
        right_ref[:, tile_of(n)] = right
    total_ref[...] = products(left_ref[...], right_ref[...])


def edge_kernel(
    levels_ref, total_ref, ve_ref, ie_ref, before_ref, after_ref,
    v_ref, q_ref, above_ref, below_ref, both_ref, g_ref,
    low_ref, qlow_ref, e_ref,
):
    ext_x, ext_y = low_ref.shape[0], low_ref.shape[1]

    def with_ends(own, before, after, index):
        lane = lanes_of(own)
        follows, comes = turn(after, LANES // 2 - 2 * index), turn(before, LANES - 2 - 2 * index)
        value = jnp.where(lane >= LANES - 2, comes, own)
        return jnp.where((lane >= LANES // 2) & (lane < LANES // 2 + 2), follows, value)

    for x in range(ext_x):
        ids = with_ends(ie_ref[x], before_ref[COLS : COLS + ext_y, :], after_ref[COLS : COLS + ext_y, :], x)
        e_ref[x] = modulus_of(levels_ref, ids)
    element_weights(e_ref, above_ref, below_ref, both_ref, 1)
    before, after = before_ref[:COLS, :], after_ref[:COLS, :]
    for x in range(ext_x):
        for y in range(ext_y):
            value = with_ends(ve_ref[x, y], before, after, x * ext_y + y)
            low_ref[x, y] = lowered(value)
            if 0 < x < ext_x - 1 and 0 < y < ext_y - 1:
                v_ref[x - 1, y - 1] = value
    sides = sides_of(above_ref, below_ref, both_ref)
    first_image(v_ref, low_ref, e_ref, sides, q_ref, qlow_ref, 1, range(1, ext_y - 1))
    right = jnp.zeros((3 * COLS, LANES), jnp.float32)
    for n, (_, b, q, w) in enumerate(own_nodes(v_ref, q_ref, qlow_ref, sides, 1)):
        three = jnp.concatenate([b, q, w], axis=0)
        at = lanes_of(three) - 2 * n
        here = ((at >= 0) & (at < 2)) | ((at >= 2 * EDGE - 2) & (at < 2 * EDGE))
        right = jnp.where(here, turn(three, 2 * n), right)
    right = split_terms(right, 3)
    total = products(left_terms(right), right)
    g_ref[...] = pack_moments(total_ref[...] + total)


def pack_moments(total):
    first, second = total[:COLS], total[COLS:]
    row = lax.broadcasted_iota(jnp.int32, (COLS, LANES), 0)
    lane = lax.broadcasted_iota(jnp.int32, (COLS, LANES), 1)
    col = lane % COLS
    upper = jnp.where(lane < COLS, first, second)
    lower = jnp.where(
        lane < COLS,
        0.5 * (pltpu.roll(first, LANES - COLS, 1) + second),
        pltpu.roll(second, LANES - COLS, 1),
    )
    valid = lane < 2 * COLS
    square = jnp.where(valid, jnp.where(row <= col, upper, lower), 0.0)
    diagonal = jnp.sum(jnp.where(valid & (row == col), lower, 0.0), axis=0, keepdims=True)
    out = []
    for half in range(2):
        out.append(square[8 * half : 8 * half + 8])
    spread_rows = jnp.zeros((8, LANES), jnp.float32)
    sub8 = lax.broadcasted_iota(jnp.int32, (8, LANES), 0)
    lane8 = lax.broadcasted_iota(jnp.int32, (8, LANES), 1)
    for quarter in range(4):
        piece = out[quarter // 2]
        if quarter % 2:
            piece = pltpu.roll(piece, 4, 0)
        if quarter:
            piece = pltpu.roll(piece, 2 * COLS * quarter, 1)
        here = (sub8 < 4) & (lane8 // (2 * COLS) == quarter)
        spread_rows = jnp.where(here, piece, spread_rows)
    return jnp.where(sub8 == 4, diagonal, spread_rows)


def unpack_moments(packed):
    sub8 = lax.broadcasted_iota(jnp.int32, (8, LANES), 0)
    halves = []
    for half in range(2):
        a, b = 2 * half, 2 * half + 1
        top = pltpu.roll(packed, LANES - 2 * COLS * a, 1) if a else packed
        bottom = pltpu.roll(pltpu.roll(packed, LANES - 2 * COLS * b, 1), 4, 0)
        halves.append(jnp.where(sub8 < 4, top, bottom))
    square = jnp.concatenate(halves, axis=0)
    row = lax.broadcasted_iota(jnp.int32, (COLS, COLS), 0)
    col = lax.broadcasted_iota(jnp.int32, (COLS, COLS), 1)
    moments = []
    for pair in range(2):
        turned = pltpu.roll(square, LANES - COLS, 1) if pair else square
        mixed = turned[:, :COLS]
        diagonal = (pltpu.roll(packed, LANES - COLS, 1) if pair else packed)[4:5, :COLS]
        flipped = mixed.T
        moments.append(jnp.where(row <= col, mixed, flipped))
        lower = jnp.where(row == col, diagonal, jnp.where(row > col, mixed, flipped))
        moments.append(lower)
    return moments


def dot(left, right, dims=((1,), (0,))):
    return lax.dot_general(left, right, (dims, ((), ())), precision=HIGH, preferred_element_type=jnp.float32)


def replicated(matrix):
    return [jnp.broadcast_to(matrix[:, i : i + 1], (COLS, LANES)) for i in range(COLS)]


def sweeps(rows):
    rows = list(rows)
    sub = lax.broadcasted_iota(jnp.int32, (COLS, LANES), 0)
    for k in range(COLS):
        scale = 1.0 / rows[k][k : k + 1, :]
        pivot_row = rows[k] * scale
        for i in range(COLS):
            if i != k:
                factor = rows[i][k : k + 1, :]
                moved = rows[i] - factor * pivot_row
                rows[i] = jnp.where(sub == k, factor * scale, moved)
        rows[k] = jnp.where(sub == k, -scale, pivot_row)
        yield rows


def times(rows, right):
    parts = [rows[i] * right[i : i + 1, :] for i in range(COLS)]
    while len(parts) > 1:
        parts = [a + b for a, b in zip(parts[::2], parts[1::2])]
    return parts[0]


def mixer(coeffs, count):
    flipped = split_terms(coeffs.T, count)
    return jnp.concatenate([flipped] * count, axis=1)


def mixed(left, block, count):
    out = jnp.dot(left, split_terms(block, count), preferred_element_type=jnp.float32)
    size = out.shape[0] // count
    return sum(out[size * n : size * (n + 1)] for n in range(count))


def finish_kernel(
    g_ref, v_ref, q_ref, above_ref, below_ref, both_ref,
    ve_ref, qe_ref, abovee_ref, belowe_ref, bothe_ref,
    sol_ref, res_ref, d_ref, dlow_ref, w0_ref, w1_ref, w2_ref,
):
    own_x, own_y = v_ref.shape[0], v_ref.shape[1]
    m0, m1, m2, m3 = unpack_moments(g_ref[...])
    first = ((0,), (0,))
    padding = jnp.zeros((COLS, LANES - COLS), jnp.float32)
    *_, minus_inv = sweeps(replicated(m1))
    minus_alpha = times(minus_inv, jnp.concatenate([m0, padding], axis=1))
    minus_m2a = times(replicated(m2), minus_alpha)
    mix = times(minus_inv, minus_m2a)[:, :COLS]
    minus_m3a = times(replicated(m3), minus_alpha)[:, :COLS]
    minus_alpha, minus_m2a = minus_alpha[:, :COLS], minus_m2a[:, :COLS]
    alpha = -minus_alpha
    left = mixer(jnp.concatenate([mix, minus_alpha], axis=0), 3)
    updated = dot(minus_alpha, minus_m2a, first) - m0
    curved = dot(minus_alpha, minus_m3a, first) + dot(minus_m2a, mix, first)
    steps = sweeps(replicated(0.5 * (curved + curved.T)))
    minus_inv = None
    for x in range(own_x):
        for y in range(own_y):
            q0, q1, qe = q_ref[x, y, :, :LANES], q_ref[x, y, :, LANES:], qe_ref[x, y]
            lane = lanes_of(qe)
            q0 = jnp.where(lane == 0, qe, q0)
            q1 = jnp.where(lane == LANES - 1, turn(qe, LANES // 2), q1)
            block = jnp.concatenate(
                [
                    jnp.concatenate([v_ref[x, y], ve_ref[x, y]], axis=1),
                    jnp.concatenate([q0, q1, qe], axis=1),
                ],
                axis=0,
            )
            value = mixed(left, block, 3)
            d_ref[x, y] = value
            dlow_ref[x, y] = lowered(value)
            minus_inv = next(steps, minus_inv)
    gamma = -times(minus_inv, jnp.concatenate([updated, padding], axis=1))[:, :COLS]
    edge, main = (abovee_ref, belowe_ref, bothe_ref), (above_ref, below_ref, both_ref)
    whole = (w0_ref, w1_ref, w2_ref)
    for end_ref, main_ref, whole_ref in zip(edge, main, whole):
        for ex in range(1, own_x):
            end = end_ref[ex]
            lane = lanes_of(end)
            whole_ref[ex, :, :LANES] = jnp.where(lane == 0, end, main_ref[ex, :, :LANES])
            end = turn(end, LANES // 2)
            whole_ref[ex, :, LANES:] = jnp.where(lane == LANES - 1, end, main_ref[ex, :, LANES:])
    main, edge = sides_of(*whole), sides_of(*edge)
    zero = jnp.zeros((COLS, COLS), jnp.float32)
    last = mixer(
        jnp.concatenate(
            [
                jnp.concatenate([alpha, gamma, zero, zero], axis=0),
                jnp.concatenate([zero, zero, -alpha, -gamma], axis=0),
            ],
            axis=1,
        ),
        3,
    )
    for x in range(1, own_x - 1):
        for y in range(1, own_y - 1):
            low = lambda i, j, t: dlow_ref[i, j, :, tile_of(t)]
            at = (x, y, x + 1, y + 1)
            plane, down, up = zip(*[terms(low, main, t, *at) for t in range(2)])
            ends = terms(lambda i, j, t: dlow_ref[i, j, :, tile_of(2)], edge, 0, *at)
            from_above = shifted(down, 1, turn(ends[1], LANES // 2))
            from_below = shifted(up, -1, ends[2])
            image = [
                SIGMA * d_ref[x, y, :, tile_of(t)] + (plane[t] - from_above[t] - from_below[t])
                for t in range(2)
            ]
            q0, q1, qe = q_ref[x, y, :, :LANES], q_ref[x, y, :, LANES:], qe_ref[x, y]
            lane = lanes_of(qe)
            q0 = jnp.where(lane == 0, qe, q0)
            q1 = jnp.where(lane == LANES - 1, turn(qe, LANES // 2), q1)
            b = v_ref[x, y]
            block = jnp.concatenate(
                [
                    b,
                    d_ref[x, y, :, : 2 * LANES],
                    jnp.concatenate([q0, q1], axis=1),
                    jnp.concatenate(image, axis=1),
                ],
                axis=0,
            )
            out = mixed(last, block, 3)
            sol_ref[:, x - 1, y - 1, :] = out[:COLS]
            res_ref[:, x - 1, y - 1, :] = b + out[COLS:]


def both_ways(axis, to_next, to_last, around=False):
    count = lax.axis_size(axis)
    steps = range(count) if around else range(count - 1)
    before = lax.ppermute(to_next, axis, [(i, (i + 1) % count) for i in steps])
    after = lax.ppermute(to_last, axis, [((i + 1) % count, i) for i in steps])
    return before, after


def spread(value, axes, root):
    count = lax.axis_size(axes)
    copies = jnp.broadcast_to(value[None], (count, *value.shape))
    group = [(root + i) % count for i in range(count)]
    return jnp.sum(lax.all_to_all(copies, axes, 0, 0, axis_index_groups=[group]), axis=0)


def line_groups(root):
    wide_x, wide_y, _, long = (lax.axis_size(axis) for axis in (*PLANE, "gz"))
    at = np.arange(wide_x * wide_y * 2 * long).reshape(wide_x * wide_y, 2, long)
    order = [(root + i) % long for i in range(long)]
    lines = [[int(v) for v in at[place, 1, order]] for place in range(wide_x * wide_y)]
    others = at[:, 0, :].T.reshape(-1, long)
    return lines + [[int(v) for v in group] for group in others]


def near(value):
    return pltpu.with_memory_space_constraint(value, pltpu.VMEM)


def on_device(loads, moduli, material):
    f32, bf16, wide = jnp.float32, jnp.bfloat16, 2 * LANES
    own_x, own_y = material.shape[:2]
    ext_x, ext_y = own_x + 4, own_y + 4
    own, levels = pl.pallas_call(
        front_kernel,
        out_shape=(
            pltpu.VMEM((2, COLS + 1, own_x, own_y, LANES), f32),
            pltpu.VMEM((moduli.shape[0], LANES), f32),
        ),
        in_specs=[
            pl.BlockSpec(memory_space=pltpu.SMEM),
            pl.BlockSpec(memory_space=pltpu.VMEM),
            pl.BlockSpec(memory_space=pltpu.VMEM),
        ],
        name="front",
    )(moduli, loads, material)
    place = lax.axis_index(GY)
    row = lax.broadcasted_iota(jnp.int32, (8, LANES), 0)
    flags = jnp.where(row == 0, place > 0, place < lax.axis_size(GY) - 1)
    flags = jnp.where(row == 2, lax.axis_index("gy_1") == 1, flags).astype(f32)
    before, after = both_ways("gx", own, own)
    part = jnp.concatenate([before, own], axis=2)
    parts = part[:, :, :, 2:], part[:, :, :, :2]
    sides = both_ways(GY, *parts, around=True)
    lasts = both_ways(GY, after[:, :, :, 2:], after[:, :, :, :2], around=True)
    line = [near(v.reshape(-1, LANES)) for v in (before, own, after)]
    flat = [near(v.reshape(-1, LANES)) for v in (sides[0], lasts[0], sides[1], lasts[1])]
    levels, flags = near(levels), near(flags)
    ends = (pltpu.VMEM((COLS + 8, LANES), f32),) * 2

    def block(xs, ys, size):
        return pltpu.VMEM((xs, ys, COLS, size), f32)

    *mid, lo, hi = pl.pallas_call(
        middle_kernel,
        out_shape=(
            block(ext_x - 2, own_y, wide),
            block(ext_x, own_y, wide),
            block(ext_x - 2, own_y - 2, wide),
            block(ext_x - 2, own_y - 2, wide),
            block(ext_x, own_y, LANES),
            pltpu.VMEM((ext_x, ext_y, LANES), f32),
            pltpu.VMEM((ext_x, ext_y, wide), f32),
            *ends,
        ),
        scratch_shapes=[pltpu.VMEM((ext_x - 1, ext_y, wide), f32)] * 3,
        compiler_params=GRANT,
        name="middle",
    )(levels, *line)
    first, last = pl.pallas_call(
        functools.partial(pack_kernel, ext_x=ext_x, ext_y=ext_y), out_shape=ends, compiler_params=GRANT, name="pack"
    )(flags, *flat, near(lo), near(hi))
    before, after = both_ways("gz", last, first)
    nodes = own_x * own_y

    def weights(size):
        return (pltpu.VMEM((ext_x - 1, ext_y, size), f32),) * 3

    def fields(size):
        return (pltpu.VMEM((ext_x - 2, ext_y - 2, COLS, size), f32),) * 2

    def scratch(size):
        return [
            pltpu.VMEM((ext_x, ext_y, COLS, size), f32),
            pltpu.VMEM((ext_x - 2, ext_y - 2, COLS, size), f32),
            pltpu.VMEM((ext_x, ext_y, size), f32),
        ]

    *main, total, edge, ids = pl.pallas_call(
        main_kernel,
        out_shape=(
            *fields(wide),
            *weights(wide),
            pltpu.VMEM((2 * COLS, LANES), f32),
            pltpu.VMEM((ext_x, ext_y, COLS, LANES), f32),
            pltpu.VMEM((ext_x, ext_y, LANES), f32),
        ),
        scratch_shapes=scratch(wide)
        + [pltpu.VMEM((6 * COLS, nodes * wide), bf16), pltpu.VMEM((9 * COLS, nodes * wide), bf16)],
        compiler_params=GRANT,
        name="main",
    )(levels, flags, *flat, *[near(v) for v in mid])
    *edges, moments = pl.pallas_call(
        edge_kernel,
        out_shape=(*fields(LANES), *weights(LANES), pltpu.VMEM((8, LANES), f32)),
        scratch_shapes=scratch(LANES),
        compiler_params=GRANT,
        name="edge",
    )(*[near(value) for value in (levels, total, edge, ids, before, after)])
    rows = 5
    length, chips = lax.axis_size("gz"), lax.axis_size("gy_0")
    moments = jnp.sum(lax.all_gather(moments[:rows], "gy_1"), axis=0).reshape(rows, 1, LANES)
    copies = jnp.broadcast_to(moments[None], (length, *moments.shape))
    moments = lax.all_to_all(copies, (*PLANE, "gz"), 0, 0, axis_index_groups=line_groups(18 * length // 32))
    moments = pl.pallas_call(
        functools.partial(total_kernel, count=length),
        out_shape=pltpu.VMEM((8, LANES), f32),
        compiler_params=GRANT,
        name="total",
    )(flags, near(moments.reshape(length * rows, LANES)))
    moments = moments[:rows].reshape(rows, 1, LANES)
    middle = (lax.axis_size("gx") // 2 * chips + chips // 2) * 2 + 1
    moments = spread(moments, PLANE, middle).reshape(rows, LANES)
    moments = jnp.concatenate([moments, jnp.zeros((8 - rows, LANES), f32)], axis=0)
    out = jax.ShapeDtypeStruct(loads.shape, f32)
    return pl.pallas_call(
        finish_kernel,
        out_shape=(out, out),
        scratch_shapes=[pltpu.VMEM((ext_x - 2, ext_y - 2, COLS, 3 * LANES), f32)] * 2
        + [pltpu.VMEM((ext_x - 1, ext_y, wide), f32)] * 3,
        compiler_params=GRANT,
        name="finish",
    )(*[near(value) for value in (moments, *main, *edges)])


def solution(mesh):
    chips, long = mesh.shape["gy"] // 2, mesh.shape["gz"]
    split = Mesh(mesh.devices.reshape(mesh.shape["gx"], chips, 2, long), ("gx", "gy_0", "gy_1", "gz"))
    spec = P(None, "gx", GY, "gz")

    return jax.shard_map(
        on_device,
        mesh=split,
        in_specs=(spec, P(), P("gx", GY, "gz")),
        out_specs=(spec, spec),
        check_vma=False,
    )
```

```python
import functools

import jax
import jax.numpy as jnp
import numpy as np
from jax import lax
from jax.experimental import pallas as pl
from jax.experimental.pallas import tpu as pltpu
from jax.sharding import Mesh
from jax.sharding import PartitionSpec as P

PLANE = ("gx", "gy_0", "gy_1")
GY = ("gy_0", "gy_1")
SIGMA = 0.25
COLS = 16
LANES = 128
EDGE = LANES // 4
HIGH = lax.Precision.HIGHEST
GRANT = pltpu.CompilerParams(vmem_limit_bytes=16 * 2**20)


def stiffness_table():
    line_mass = np.array([[1.0 / 3.0, 1.0 / 6.0], [1.0 / 6.0, 1.0 / 3.0]])
    line_stiff = np.array([[1.0, -1.0], [-1.0, 1.0]])
    table = np.zeros((8, 8))
    for target in range(8):
        for source in range(8):
            target_bits = [target >> 2 & 1, target >> 1 & 1, target & 1]
            source_bits = [source >> 2 & 1, source >> 1 & 1, source & 1]
            total = 0.0
            for stiff_dim in range(3):
                factor = 1.0
                for other in range(3):
                    if other == stiff_dim:
                        factor = factor * line_stiff[target_bits[other], source_bits[other]]
                    else:
                        factor = factor * line_mass[target_bits[other], source_bits[other]]
                total = total + factor
            table[target, source] = total
    return table


def kernel_scale():
    table = np.asarray(jnp.asarray(stiffness_table(), jnp.bfloat16).astype(jnp.float32))
    unit = -float(table[0, 7])
    for target in range(8):
        for source in range(8):
            bits = bin(target ^ source).count("1")
            want = (4.0, 0.0, -1.0, -1.0)[bits] * unit
            assert abs(float(table[target, source]) - want) < 1e-12
    return unit


UNIT = kernel_scale()


def lowered(value):
    return value.astype(jnp.bfloat16).astype(jnp.float32)


MIDDLE = (2, 3, 4, 5)
OUTER = (0, 1, 6, 7)


def tile_of(tile):
    return slice(tile * LANES, (tile + 1) * LANES)


def lanes_of(value):
    return lax.broadcasted_iota(jnp.int32, value.shape, 1)


def turn(value, amount):
    amount %= LANES
    return pltpu.roll(value, amount, 1) if amount else value


def shifted(tiles, step, beyond=None):
    count = len(tiles)
    turned = [turn(t, -step) for t in tiles]
    past = turn(beyond, -step) if beyond is not None else turned[0 if step > 0 else -1]
    lane = lanes_of(tiles[0])
    if step > 0:
        return [jnp.where(lane < LANES - 1, turned[i], turned[i + 1] if i + 1 < count else past) for i in range(count)]
    return [jnp.where(lane > 0, turned[i], turned[i - 1] if i else past) for i in range(count)]


def terms(low, sides, tile, x, y, wx, wy):
    above, below, both = sides
    around = {(i, j): low(x + i, y + j, tile) for i in (-1, 0, 1) for j in (-1, 0, 1)}
    total = None
    for i in (-1, 1):
        for j in (-1, 1):
            ex, ey = wx + (i - 1) // 2, wy + (j - 1) // 2
            others = around[i, 0] + around[0, j] + around[i, j]
            new = (
                both(ex, ey, tile) * around[i, j],
                below(ex, ey, tile) * others,
                above(ex, ey, tile) * others,
            )
            total = new if total is None else tuple(a + b for a, b in zip(total, new))
    rim = [both(wx + i, wy + j, tile) for i in (-1, 0) for j in (-1, 0)]
    centre = (4.0 * ((rim[0] + rim[1]) + (rim[2] + rim[3]))) * around[0, 0]
    return centre - total[0], total[1], total[2]


def operator(field, low, sides, count, x, y, wx, wy):
    plane, down, up = zip(*[terms(low, sides, t, x, y, wx, wy) for t in range(count)])
    from_above, from_below = shifted(down, 1), shifted(up, -1)
    return [SIGMA * field(t) + (plane[t] - from_above[t] - from_below[t]) for t in range(count)]


def split_terms(value, count):
    parts = []
    for n in range(count):
        part = value.astype(jnp.bfloat16)
        parts.append(part)
        if n + 1 < count:
            value = value - part.astype(jnp.float32)
    return jnp.concatenate(parts, axis=0)


def rows_of(refs, flags_ref, tile, x, y, first, count):
    before_x_ref, own_ref, after_x_ref, before_ref, before_last_ref, after_ref, after_last_ref = refs
    flag = None
    if 2 <= y < 6:
        ref, column, wide, tall, at = (before_x_ref, own_ref, after_x_ref)[x // 2], x % 2, 2, 4, y - 2
    else:
        low = y < 2
        flag, at, tall = (0, y, 2) if low else (1, y - 6, 2)
        if x < 4:
            ref, column, wide = before_ref if low else after_ref, x, 4
        else:
            ref, column, wide = before_last_ref if low else after_last_ref, x - 4, 2
    stride = wide * tall
    start = tile * (ref.shape[0] // 2) + first * stride + column * tall + at
    value = ref[pl.ds(start, count, stride=stride), :] if count > 1 else ref[start : start + 1, :]
    if flag is not None:
        value = jnp.where(flags_ref[flag : flag + 1, :] > 0.0, value, 0.0)
    return value


def front_kernel(moduli_ref, loads_ref, material_ref, own_ref, levels_ref):
    for t in range(2):
        own_ref[t, :COLS] = loads_ref[:, :, :, tile_of(t)]
        own_ref[t, COLS] = (material_ref[:, :, tile_of(t)] + 1).astype(jnp.float32)
    for level in range(moduli_ref.shape[0]):
        levels_ref[level : level + 1, :] = jnp.full((1, LANES), moduli_ref[level], jnp.float32)


def pack_rows(starts, out_refs, refs, flags_ref, ext_x, ext_y, ys):
    for tile, (start_ref, out_ref) in enumerate(zip(starts, out_refs)):
        offset = 2 * tile
        lane = lax.broadcasted_iota(jnp.int32, (COLS, LANES), 1)
        packed = jnp.zeros((COLS, LANES), jnp.float32) if start_ref is None else start_ref[:COLS, :]
        for y in range(ext_y):
            row = slice(COLS + y, COLS + y + 1)
            ids = jnp.zeros((1, LANES), jnp.float32) if start_ref is None else start_ref[row, :]
            for x in range(ext_x) if y in ys else ():
                node = x * ext_y + y
                value = rows_of(refs, flags_ref, tile, x, y, 0, COLS)
                packed = jnp.where(lane // 2 == node, turn(value, 2 * node + offset), packed)
                value = rows_of(refs, flags_ref, tile, x, y, COLS, 1)
                ids = jnp.where(lane[:1] // 2 == x, turn(value, 2 * x + offset), ids)
            out_ref[row, :] = ids
        out_ref[:COLS, :] = packed


def pack_kernel(flags_ref, a_ref, b_ref, c_ref, d_ref, lo0_ref, hi0_ref, lo_ref, hi_ref, ext_x, ext_y):
    refs = (None, None, None, a_ref, b_ref, c_ref, d_ref)
    pack_rows((lo0_ref, hi0_ref), (lo_ref, hi_ref), refs, flags_ref, ext_x, ext_y, OUTER)


def sums_of(parts_ref, count):
    rows = parts_ref.shape[0] // count
    sub = lax.broadcasted_iota(jnp.int32, (8, LANES), 0)
    out = jnp.zeros((8, LANES), jnp.float32)
    for row in range(rows):
        part = jnp.sum(parts_ref[pl.ds(row, count, stride=rows), :], axis=0, keepdims=True)
        out = jnp.where(sub == row, part, out)
    return out


def total_kernel(flags_ref, parts_ref, out_ref, count, copies):
    rows = parts_ref.shape[0] // count
    out = jnp.where(flags_ref[2:3, :] > 0.0, sums_of(parts_ref, count), 0.0)
    for row in range(rows):
        out_ref[pl.ds(row, copies, stride=rows), :] = jnp.broadcast_to(out[row : row + 1, :], (copies, LANES))


def modulus_of(levels_ref, ids):
    modulus = jnp.zeros_like(ids)
    for level in range(levels_ref.shape[0]):
        modulus = jnp.where(ids == level + 1.0, levels_ref[level : level + 1, :], modulus)
    return modulus


def element_weights(e_ref, above_ref, below_ref, both_ref, count):
    ext_x, ext_y = e_ref.shape[:2]
    for ex in range(ext_x - 1):
        flat = []
        for t in range(count):
            both_x = e_ref[ex, :, tile_of(t)] + e_ref[ex + 1, :, tile_of(t)]
            flat.append(both_x + pltpu.roll(both_x, ext_y - 1, 0))
        ahead = shifted(flat, 1)
        weights = [(0.125 * UNIT) * (flat[t] + ahead[t]) for t in range(count)]
        behind = shifted(weights, -1)
        for t in range(count):
            above_ref[ex, :, tile_of(t)] = weights[t]
            below_ref[ex, :, tile_of(t)] = behind[t]
            both_ref[ex, :, tile_of(t)] = weights[t] + behind[t]


def sides_of(*refs):
    return tuple(lambda ex, ey, t, ref=ref: ref[ex, ey : ey + 1, tile_of(t)] for ref in refs)


def first_image(v_ref, low_ref, e_ref, sides, q_ref, qlow_ref, count, ys):
    ext_x, ext_y = low_ref.shape[0], low_ref.shape[1]
    for x in range(1, ext_x - 1):
        for y in ys:
            image = operator(
                lambda t: v_ref[x - 1, y - 1, :, tile_of(t)],
                lambda i, j, t: low_ref[i, j, :, tile_of(t)],
                sides, count, x, y, x, y,
            )
            for t in range(count):
                value = image[t]
                if count == 1 or x in (1, ext_x - 2) or y in (1, ext_y - 2):
                    value = jnp.where(e_ref[x, y : y + 1, tile_of(t)] > 0.0, value, 0.0)
                q_ref[x - 1, y - 1, :, tile_of(t)] = value
                qlow_ref[x - 1, y - 1, :, tile_of(t)] = lowered(value)


def own_nodes(v_ref, q_ref, qlow_ref, sides, count):
    own_x, own_y = v_ref.shape[0], v_ref.shape[1]
    for x in range(1, own_x - 1):
        for y in range(1, own_y - 1):
            image = operator(
                lambda t: q_ref[x, y, :, tile_of(t)],
                lambda i, j, t: qlow_ref[i, j, :, tile_of(t)],
                sides, count, x, y, x + 1, y + 1,
            )
            for t in range(count):
                yield t, v_ref[x, y, :, tile_of(t)], q_ref[x, y, :, tile_of(t)], image[t]


def left_terms(right):
    return jnp.concatenate([right[3 * COLS * n : 3 * COLS * n + 2 * COLS] for n in range(3)], axis=0)


def products(left, right):
    product = lax.dot_general(left, right, (((1,), (1,)), ((), ())), preferred_element_type=jnp.float32)
    rows = sum(product[2 * COLS * n : 2 * COLS * (n + 1)] for n in range(3))
    lane = lax.broadcasted_iota(jnp.int32, (2 * COLS, LANES), 1)
    first = rows[:, :LANES]
    rest = jnp.concatenate([rows[:, LANES:], jnp.zeros((2 * COLS, 2 * LANES - 9 * COLS), jnp.float32)], axis=1)
    third = jnp.where(lane < 2 * COLS, turn(first, -6 * COLS), turn(rest, 2 * COLS))
    return first + turn(first, -3 * COLS) + third


def edge_of(tiles):
    lane = lanes_of(tiles[0])
    return jnp.where(lane < EDGE, tiles[0], jnp.where(lane < 2 * EDGE, turn(tiles[1], 2 * EDGE), 0.0))


def middle_kernel(
    levels_ref, before_ref, own_ref, after_ref,
    v_ref, low_ref, q_ref, qlow_ref, ve_ref, ie_ref, e_ref, lo_ref, hi_ref,
    above_ref, below_ref, both_ref,
):
    ext_x, ext_y = low_ref.shape[0], e_ref.shape[1]
    refs = (before_ref, own_ref, after_ref, None, None, None, None)
    e_ref[...] = jnp.zeros_like(e_ref)
    ie_ref[...] = jnp.zeros_like(ie_ref)
    for x in range(ext_x):
        for y in MIDDLE:
            tiles = [rows_of(refs, None, t, x, y, COLS, 1) for t in range(2)]
            ie_ref[x, y - 2 : y - 1, :] = edge_of(tiles)
            for t in range(2):
                e_ref[x, y - 2 : y - 1, tile_of(t)] = tiles[t]
            tiles = [rows_of(refs, None, t, x, y, 0, COLS) for t in range(2)]
            ve_ref[x, y - 2] = edge_of(tiles)
            for t in range(2):
                low_ref[x, y - 2, :, tile_of(t)] = lowered(tiles[t])
                if 0 < x < ext_x - 1:
                    v_ref[x - 1, y - 2, :, tile_of(t)] = tiles[t]
        for t in range(2):
            e_ref[x, :, tile_of(t)] = modulus_of(levels_ref, e_ref[x, :, tile_of(t)])
    pack_rows((None, None), (lo_ref, hi_ref), refs, None, ext_x, ext_y, MIDDLE)
    element_weights(e_ref, above_ref, below_ref, both_ref, 2)
    sides = sides_of(above_ref, below_ref, both_ref)
    for x in range(1, ext_x - 1):
        for y in (1, 2):
            image = operator(
                lambda t: v_ref[x - 1, y, :, tile_of(t)],
                lambda i, j, t: low_ref[i, j, :, tile_of(t)],
                sides, 2, x, y, x, y,
            )
            for t in range(2):
                value = image[t]
                if x in (1, ext_x - 2):
                    value = jnp.where(e_ref[x, y : y + 1, tile_of(t)] > 0.0, value, 0.0)
                q_ref[x - 1, y - 1, :, tile_of(t)] = value
                qlow_ref[x - 1, y - 1, :, tile_of(t)] = lowered(value)


def main_kernel(
    levels_ref, flags_ref, a_ref, b_ref, c_ref, d_ref,
    vm_ref, lowm_ref, qm_ref, qlowm_ref, vem_ref, iem_ref, em_ref,
    v_ref, q_ref, above_ref, below_ref, both_ref, total_ref, ve_ref, ie_ref,
    low_ref, qlow_ref, e_ref, left_ref, right_ref,
):
    ext_x, ext_y = low_ref.shape[0], low_ref.shape[1]
    refs = (None, None, None, a_ref, b_ref, c_ref, d_ref)
    for x in range(ext_x):
        ie_ref[x, 2:6, :] = iem_ref[x, 0:4, :]
        for y in OUTER:
            tiles = [rows_of(refs, flags_ref, t, x, y, COLS, 1) for t in range(2)]
            ie_ref[x, y : y + 1, :] = edge_of(tiles)
            for t in range(2):
                e_ref[x, y : y + 1, tile_of(t)] = tiles[t]
        for t in range(2):
            e_ref[x, 2:6, tile_of(t)] = jnp.zeros((4, LANES), jnp.float32)
            e_ref[x, :, tile_of(t)] = modulus_of(levels_ref, e_ref[x, :, tile_of(t)])
            e_ref[x, 2:6, tile_of(t)] = em_ref[x, 0:4, tile_of(t)]
    element_weights(e_ref, above_ref, below_ref, both_ref, 2)
    for x in range(ext_x):
        for y in range(ext_y):
            inner = 0 < x < ext_x - 1 and 0 < y < ext_y - 1
            if y in MIDDLE:
                ve_ref[x, y] = vem_ref[x, y - 2]
                low_ref[x, y] = lowm_ref[x, y - 2]
                if inner:
                    v_ref[x - 1, y - 1] = vm_ref[x - 1, y - 2]
                if inner and y in (3, 4):
                    q_ref[x - 1, y - 1] = qm_ref[x - 1, y - 3]
                    qlow_ref[x - 1, y - 1] = qlowm_ref[x - 1, y - 3]
                continue
            tiles = [rows_of(refs, flags_ref, t, x, y, 0, COLS) for t in range(2)]
            ve_ref[x, y] = edge_of(tiles)
            for t in range(2):
                low_ref[x, y, :, tile_of(t)] = lowered(tiles[t])
                if inner:
                    v_ref[x - 1, y - 1, :, tile_of(t)] = tiles[t]
    sides = sides_of(above_ref, below_ref, both_ref)
    first_image(v_ref, low_ref, e_ref, sides, q_ref, qlow_ref, 2, (1, 2, 5, 6))
    for n, (t, b, q, w) in enumerate(own_nodes(v_ref, q_ref, qlow_ref, sides, 2)):
        right = split_terms(jnp.concatenate([b, q, w], axis=0), 3)
        left = left_terms(right)
        here = lanes_of(left) >= 2 if t == 0 else lanes_of(left) < LANES - 2
        left_ref[:, tile_of(n)] = jnp.where(here, left, jnp.zeros_like(left))
        right_ref[:, tile_of(n)] = right
    total_ref[...] = products(left_ref[...], right_ref[...])


def edge_kernel(
    levels_ref, total_ref, ve_ref, ie_ref, before_ref, after_ref,
    v_ref, q_ref, above_ref, below_ref, both_ref, g_ref,
    low_ref, qlow_ref, e_ref,
):
    ext_x, ext_y = low_ref.shape[0], low_ref.shape[1]

    def with_ends(own, before, after, index):
        lane = lanes_of(own)
        follows, comes = turn(after, LANES // 2 - 2 * index), turn(before, LANES - 2 - 2 * index)
        value = jnp.where(lane >= LANES - 2, comes, own)
        return jnp.where((lane >= LANES // 2) & (lane < LANES // 2 + 2), follows, value)

    for x in range(ext_x):
        ids = with_ends(ie_ref[x], before_ref[COLS : COLS + ext_y, :], after_ref[COLS : COLS + ext_y, :], x)
        e_ref[x] = modulus_of(levels_ref, ids)
    element_weights(e_ref, above_ref, below_ref, both_ref, 1)
    before, after = before_ref[:COLS, :], after_ref[:COLS, :]
    for x in range(ext_x):
        for y in range(ext_y):
            value = with_ends(ve_ref[x, y], before, after, x * ext_y + y)
            low_ref[x, y] = lowered(value)
            if 0 < x < ext_x - 1 and 0 < y < ext_y - 1:
                v_ref[x - 1, y - 1] = value
    sides = sides_of(above_ref, below_ref, both_ref)
    first_image(v_ref, low_ref, e_ref, sides, q_ref, qlow_ref, 1, range(1, ext_y - 1))
    right = jnp.zeros((3 * COLS, LANES), jnp.float32)
    for n, (_, b, q, w) in enumerate(own_nodes(v_ref, q_ref, qlow_ref, sides, 1)):
        three = jnp.concatenate([b, q, w], axis=0)
        at = lanes_of(three) - 2 * n
        here = ((at >= 0) & (at < 2)) | ((at >= 2 * EDGE - 2) & (at < 2 * EDGE))
        right = jnp.where(here, turn(three, 2 * n), right)
    right = split_terms(right, 3)
    total = products(left_terms(right), right)
    g_ref[...] = pack_moments(total_ref[...] + total)


def pack_moments(total):
    first, second = total[:COLS], total[COLS:]
    row = lax.broadcasted_iota(jnp.int32, (COLS, LANES), 0)
    lane = lax.broadcasted_iota(jnp.int32, (COLS, LANES), 1)
    col = lane % COLS
    upper = jnp.where(lane < COLS, first, second)
    lower = jnp.where(
        lane < COLS,
        0.5 * (pltpu.roll(first, LANES - COLS, 1) + second),
        pltpu.roll(second, LANES - COLS, 1),
    )
    valid = lane < 2 * COLS
    square = jnp.where(valid, jnp.where(row <= col, upper, lower), 0.0)
    diagonal = jnp.sum(jnp.where(valid & (row == col), lower, 0.0), axis=0, keepdims=True)
    out = []
    for half in range(2):
        out.append(square[8 * half : 8 * half + 8])
    spread_rows = jnp.zeros((8, LANES), jnp.float32)
    sub8 = lax.broadcasted_iota(jnp.int32, (8, LANES), 0)
    lane8 = lax.broadcasted_iota(jnp.int32, (8, LANES), 1)
    for quarter in range(4):
        piece = out[quarter // 2]
        if quarter % 2:
            piece = pltpu.roll(piece, 4, 0)
        if quarter:
            piece = pltpu.roll(piece, 2 * COLS * quarter, 1)
        here = (sub8 < 4) & (lane8 // (2 * COLS) == quarter)
        spread_rows = jnp.where(here, piece, spread_rows)
    return jnp.where(sub8 == 4, diagonal, spread_rows)


def unpack_moments(packed):
    sub8 = lax.broadcasted_iota(jnp.int32, (8, LANES), 0)
    halves = []
    for half in range(2):
        a, b = 2 * half, 2 * half + 1
        top = pltpu.roll(packed, LANES - 2 * COLS * a, 1) if a else packed
        bottom = pltpu.roll(pltpu.roll(packed, LANES - 2 * COLS * b, 1), 4, 0)
        halves.append(jnp.where(sub8 < 4, top, bottom))
    square = jnp.concatenate(halves, axis=0)
    row = lax.broadcasted_iota(jnp.int32, (COLS, COLS), 0)
    col = lax.broadcasted_iota(jnp.int32, (COLS, COLS), 1)
    moments = []
    for pair in range(2):
        turned = pltpu.roll(square, LANES - COLS, 1) if pair else square
        mixed = turned[:, :COLS]
        diagonal = (pltpu.roll(packed, LANES - COLS, 1) if pair else packed)[4:5, :COLS]
        flipped = mixed.T
        moments.append(jnp.where(row <= col, mixed, flipped))
        lower = jnp.where(row == col, diagonal, jnp.where(row > col, mixed, flipped))
        moments.append(lower)
    return moments


def dot(left, right, dims=((1,), (0,))):
    return lax.dot_general(left, right, (dims, ((), ())), precision=HIGH, preferred_element_type=jnp.float32)


def replicated(matrix):
    return [jnp.broadcast_to(matrix[:, i : i + 1], (COLS, LANES)) for i in range(COLS)]


def sweeps(rows):
    rows = list(rows)
    sub = lax.broadcasted_iota(jnp.int32, (COLS, LANES), 0)
    for k in range(COLS):
        scale = 1.0 / rows[k][k : k + 1, :]
        pivot_row = rows[k] * scale
        for i in range(COLS):
            if i != k:
                factor = rows[i][k : k + 1, :]
                moved = rows[i] - factor * pivot_row
                rows[i] = jnp.where(sub == k, factor * scale, moved)
        rows[k] = jnp.where(sub == k, -scale, pivot_row)
        yield rows


def times(rows, right):
    parts = [rows[i] * right[i : i + 1, :] for i in range(COLS)]
    while len(parts) > 1:
        parts = [a + b for a, b in zip(parts[::2], parts[1::2])]
    return parts[0]


def mixer(coeffs, count):
    flipped = split_terms(coeffs.T, count)
    return jnp.concatenate([flipped] * count, axis=1)


def mixed(left, block, count):
    out = jnp.dot(left, split_terms(block, count), preferred_element_type=jnp.float32)
    size = out.shape[0] // count
    return sum(out[size * n : size * (n + 1)] for n in range(count))


def finish_kernel(
    g_ref, v_ref, q_ref, above_ref, below_ref, both_ref,
    ve_ref, qe_ref, abovee_ref, belowe_ref, bothe_ref,
    sol_ref, res_ref, d_ref, dlow_ref, w0_ref, w1_ref, w2_ref,
):
    own_x, own_y = v_ref.shape[0], v_ref.shape[1]
    m0, m1, m2, m3 = unpack_moments(sums_of(g_ref, g_ref.shape[0] // 5))
    first = ((0,), (0,))
    padding = jnp.zeros((COLS, LANES - COLS), jnp.float32)
    *_, minus_inv = sweeps(replicated(m1))
    minus_alpha = times(minus_inv, jnp.concatenate([m0, padding], axis=1))
    minus_m2a = times(replicated(m2), minus_alpha)
    mix = times(minus_inv, minus_m2a)[:, :COLS]
    minus_m3a = times(replicated(m3), minus_alpha)[:, :COLS]
    minus_alpha, minus_m2a = minus_alpha[:, :COLS], minus_m2a[:, :COLS]
    alpha = -minus_alpha
    left = mixer(jnp.concatenate([mix, minus_alpha], axis=0), 3)
    updated = dot(minus_alpha, minus_m2a, first) - m0
    curved = dot(minus_alpha, minus_m3a, first) + dot(minus_m2a, mix, first)
    steps = sweeps(replicated(0.5 * (curved + curved.T)))
    minus_inv = None
    for x in range(own_x):
        for y in range(own_y):
            q0, q1, qe = q_ref[x, y, :, :LANES], q_ref[x, y, :, LANES:], qe_ref[x, y]
            lane = lanes_of(qe)
            q0 = jnp.where(lane == 0, qe, q0)
            q1 = jnp.where(lane == LANES - 1, turn(qe, LANES // 2), q1)
            block = jnp.concatenate(
                [
                    jnp.concatenate([v_ref[x, y], ve_ref[x, y]], axis=1),
                    jnp.concatenate([q0, q1, qe], axis=1),
                ],
                axis=0,
            )
            value = mixed(left, block, 3)
            d_ref[x, y] = value
            dlow_ref[x, y] = lowered(value)
            minus_inv = next(steps, minus_inv)
    gamma = -times(minus_inv, jnp.concatenate([updated, padding], axis=1))[:, :COLS]
    edge, main = (abovee_ref, belowe_ref, bothe_ref), (above_ref, below_ref, both_ref)
    whole = (w0_ref, w1_ref, w2_ref)
    for end_ref, main_ref, whole_ref in zip(edge, main, whole):
        for ex in range(1, own_x):
            end = end_ref[ex]
            lane = lanes_of(end)
            whole_ref[ex, :, :LANES] = jnp.where(lane == 0, end, main_ref[ex, :, :LANES])
            end = turn(end, LANES // 2)
            whole_ref[ex, :, LANES:] = jnp.where(lane == LANES - 1, end, main_ref[ex, :, LANES:])
    main, edge = sides_of(*whole), sides_of(*edge)
    zero = jnp.zeros((COLS, COLS), jnp.float32)
    last = mixer(
        jnp.concatenate(
            [
                jnp.concatenate([alpha, gamma, zero, zero], axis=0),
                jnp.concatenate([zero, zero, -alpha, -gamma], axis=0),
            ],
            axis=1,
        ),
        3,
    )
    for x in range(1, own_x - 1):
        for y in range(1, own_y - 1):
            low = lambda i, j, t: dlow_ref[i, j, :, tile_of(t)]
            at = (x, y, x + 1, y + 1)
            plane, down, up = zip(*[terms(low, main, t, *at) for t in range(2)])
            ends = terms(lambda i, j, t: dlow_ref[i, j, :, tile_of(2)], edge, 0, *at)
            from_above = shifted(down, 1, turn(ends[1], LANES // 2))
            from_below = shifted(up, -1, ends[2])
            image = [
                SIGMA * d_ref[x, y, :, tile_of(t)] + (plane[t] - from_above[t] - from_below[t])
                for t in range(2)
            ]
            q0, q1, qe = q_ref[x, y, :, :LANES], q_ref[x, y, :, LANES:], qe_ref[x, y]
            lane = lanes_of(qe)
            q0 = jnp.where(lane == 0, qe, q0)
            q1 = jnp.where(lane == LANES - 1, turn(qe, LANES // 2), q1)
            b = v_ref[x, y]
            block = jnp.concatenate(
                [
                    b,
                    d_ref[x, y, :, : 2 * LANES],
                    jnp.concatenate([q0, q1], axis=1),
                    jnp.concatenate(image, axis=1),
                ],
                axis=0,
            )
            out = mixed(last, block, 3)
            sol_ref[:, x - 1, y - 1, :] = out[:COLS]
            res_ref[:, x - 1, y - 1, :] = b + out[COLS:]


def both_ways(axis, to_next, to_last, around=False):
    count = lax.axis_size(axis)
    steps = range(count) if around else range(count - 1)
    before = lax.ppermute(to_next, axis, [(i, (i + 1) % count) for i in steps])
    after = lax.ppermute(to_last, axis, [((i + 1) % count, i) for i in steps])
    return before, after


def line_groups(root):
    wide_x, wide_y, _, long = (lax.axis_size(axis) for axis in (*PLANE, "gz"))
    at = np.arange(wide_x * wide_y * 2 * long).reshape(wide_x * wide_y, 2, long)
    order = [(root + i) % long for i in range(long)]
    lines = [[int(v) for v in at[place, 1, order]] for place in range(wide_x * wide_y)]
    others = at[:, 0, :].T.reshape(-1, long)
    return lines + [[int(v) for v in group] for group in others]


def near(value):
    return pltpu.with_memory_space_constraint(value, pltpu.VMEM)


def on_device(loads, moduli, material):
    f32, bf16, wide = jnp.float32, jnp.bfloat16, 2 * LANES
    own_x, own_y = material.shape[:2]
    ext_x, ext_y = own_x + 4, own_y + 4
    own, levels = pl.pallas_call(
        front_kernel,
        out_shape=(
            pltpu.VMEM((2, COLS + 1, own_x, own_y, LANES), f32),
            pltpu.VMEM((moduli.shape[0], LANES), f32),
        ),
        in_specs=[
            pl.BlockSpec(memory_space=pltpu.SMEM),
            pl.BlockSpec(memory_space=pltpu.VMEM),
            pl.BlockSpec(memory_space=pltpu.VMEM),
        ],
        name="front",
    )(moduli, loads, material)
    place = lax.axis_index(GY)
    row = lax.broadcasted_iota(jnp.int32, (8, LANES), 0)
    flags = jnp.where(row == 0, place > 0, place < lax.axis_size(GY) - 1)
    flags = jnp.where(row == 2, lax.axis_index("gy_1") == 1, flags).astype(f32)
    before, after = both_ways("gx", own, own)
    part = jnp.concatenate([before, own], axis=2)
    parts = part[:, :, :, 2:], part[:, :, :, :2]
    sides = both_ways(GY, *parts, around=True)
    lasts = both_ways(GY, after[:, :, :, 2:], after[:, :, :, :2], around=True)
    line = [near(v.reshape(-1, LANES)) for v in (before, own, after)]
    flat = [near(v.reshape(-1, LANES)) for v in (sides[0], lasts[0], sides[1], lasts[1])]
    levels, flags = near(levels), near(flags)
    ends = (pltpu.VMEM((COLS + 8, LANES), f32),) * 2

    def block(xs, ys, size):
        return pltpu.VMEM((xs, ys, COLS, size), f32)

    *mid, lo, hi = pl.pallas_call(
        middle_kernel,
        out_shape=(
            block(ext_x - 2, own_y, wide),
            block(ext_x, own_y, wide),
            block(ext_x - 2, own_y - 2, wide),
            block(ext_x - 2, own_y - 2, wide),
            block(ext_x, own_y, LANES),
            pltpu.VMEM((ext_x, ext_y, LANES), f32),
            pltpu.VMEM((ext_x, ext_y, wide), f32),
            *ends,
        ),
        scratch_shapes=[pltpu.VMEM((ext_x - 1, ext_y, wide), f32)] * 3,
        compiler_params=GRANT,
        name="middle",
    )(levels, *line)
    first, last = pl.pallas_call(
        functools.partial(pack_kernel, ext_x=ext_x, ext_y=ext_y), out_shape=ends, compiler_params=GRANT, name="pack"
    )(flags, *flat, near(lo), near(hi))
    before, after = both_ways("gz", last, first)
    nodes = own_x * own_y

    def weights(size):
        return (pltpu.VMEM((ext_x - 1, ext_y, size), f32),) * 3

    def fields(size):
        return (pltpu.VMEM((ext_x - 2, ext_y - 2, COLS, size), f32),) * 2

    def scratch(size):
        return [
            pltpu.VMEM((ext_x, ext_y, COLS, size), f32),
            pltpu.VMEM((ext_x - 2, ext_y - 2, COLS, size), f32),
            pltpu.VMEM((ext_x, ext_y, size), f32),
        ]

    *main, total, edge, ids = pl.pallas_call(
        main_kernel,
        out_shape=(
            *fields(wide),
            *weights(wide),
            pltpu.VMEM((2 * COLS, LANES), f32),
            pltpu.VMEM((ext_x, ext_y, COLS, LANES), f32),
            pltpu.VMEM((ext_x, ext_y, LANES), f32),
        ),
        scratch_shapes=scratch(wide)
        + [pltpu.VMEM((6 * COLS, nodes * wide), bf16), pltpu.VMEM((9 * COLS, nodes * wide), bf16)],
        compiler_params=GRANT,
        name="main",
    )(levels, flags, *flat, *[near(v) for v in mid])
    *edges, moments = pl.pallas_call(
        edge_kernel,
        out_shape=(*fields(LANES), *weights(LANES), pltpu.VMEM((8, LANES), f32)),
        scratch_shapes=scratch(LANES),
        compiler_params=GRANT,
        name="edge",
    )(*[near(value) for value in (levels, total, edge, ids, before, after)])
    rows = 5
    length, chips = lax.axis_size("gz"), lax.axis_size("gy_0")
    moments = jnp.sum(lax.all_gather(moments[:rows], "gy_1"), axis=0).reshape(rows, 1, LANES)
    copies = jnp.broadcast_to(moments[None], (length, *moments.shape))
    moments = lax.all_to_all(copies, (*PLANE, "gz"), 0, 0, axis_index_groups=line_groups(19 * length // 32))
    places = lax.axis_size(PLANE)
    copies = pl.pallas_call(
        functools.partial(total_kernel, count=length, copies=places),
        out_shape=pltpu.VMEM((places * rows, LANES), f32),
        compiler_params=GRANT,
        name="total",
    )(flags, near(moments.reshape(length * rows, LANES)))
    middle = (lax.axis_size("gx") // 2 * chips + chips // 2) * 2 + 1
    group = [(middle + i) % places for i in range(places)]
    copies = copies.reshape(places, rows, 1, LANES)
    moments = lax.all_to_all(copies, PLANE, 0, 0, axis_index_groups=[group]).reshape(places * rows, LANES)
    out = jax.ShapeDtypeStruct(loads.shape, f32)
    return pl.pallas_call(
        finish_kernel,
        out_shape=(out, out),
        scratch_shapes=[pltpu.VMEM((ext_x - 2, ext_y - 2, COLS, 3 * LANES), f32)] * 2
        + [pltpu.VMEM((ext_x - 1, ext_y, wide), f32)] * 3,
        compiler_params=GRANT,
        name="finish",
    )(*[near(value) for value in (moments, *main, *edges)])


def solution(mesh):
    chips, long = mesh.shape["gy"] // 2, mesh.shape["gz"]
    split = Mesh(mesh.devices.reshape(mesh.shape["gx"], chips, 2, long), ("gx", "gy_0", "gy_1", "gz"))
    spec = P(None, "gx", GY, "gz")

    return jax.shard_map(
        on_device,
        mesh=split,
        in_specs=(spec, P(), P("gx", GY, "gz")),
        out_specs=(spec, spec),
        check_vma=False,
    )
```

```python
import functools

import jax
import jax.numpy as jnp
import numpy as np
from jax import lax
from jax.experimental import pallas as pl
from jax.experimental.pallas import tpu as pltpu
from jax.sharding import Mesh
from jax.sharding import PartitionSpec as P

PLANE = ("gx", "gy_0", "gy_1")
GY = ("gy_0", "gy_1")
SIGMA = 0.25
COLS = 16
LANES = 128
EDGE = LANES // 4
HIGH = lax.Precision.HIGHEST
GRANT = pltpu.CompilerParams(vmem_limit_bytes=16 * 2**20)


def stiffness_table():
    line_mass = np.array([[1.0 / 3.0, 1.0 / 6.0], [1.0 / 6.0, 1.0 / 3.0]])
    line_stiff = np.array([[1.0, -1.0], [-1.0, 1.0]])
    table = np.zeros((8, 8))
    for target in range(8):
        for source in range(8):
            target_bits = [target >> 2 & 1, target >> 1 & 1, target & 1]
            source_bits = [source >> 2 & 1, source >> 1 & 1, source & 1]
            total = 0.0
            for stiff_dim in range(3):
                factor = 1.0
                for other in range(3):
                    if other == stiff_dim:
                        factor = factor * line_stiff[target_bits[other], source_bits[other]]
                    else:
                        factor = factor * line_mass[target_bits[other], source_bits[other]]
                total = total + factor
            table[target, source] = total
    return table


def kernel_scale():
    table = np.asarray(jnp.asarray(stiffness_table(), jnp.bfloat16).astype(jnp.float32))
    unit = -float(table[0, 7])
    for target in range(8):
        for source in range(8):
            bits = bin(target ^ source).count("1")
            want = (4.0, 0.0, -1.0, -1.0)[bits] * unit
            assert abs(float(table[target, source]) - want) < 1e-12
    return unit


UNIT = kernel_scale()


def lowered(value):
    return value.astype(jnp.bfloat16).astype(jnp.float32)


MIDDLE = (2, 3, 4, 5)
OUTER = (0, 1, 6, 7)


def tile_of(tile):
    return slice(tile * LANES, (tile + 1) * LANES)


def lanes_of(value):
    return lax.broadcasted_iota(jnp.int32, value.shape, 1)


def turn(value, amount):
    amount %= LANES
    return pltpu.roll(value, amount, 1) if amount else value


def shifted(tiles, step, beyond=None):
    count = len(tiles)
    turned = [turn(t, -step) for t in tiles]
    past = turn(beyond, -step) if beyond is not None else turned[0 if step > 0 else -1]
    lane = lanes_of(tiles[0])
    if step > 0:
        return [jnp.where(lane < LANES - 1, turned[i], turned[i + 1] if i + 1 < count else past) for i in range(count)]
    return [jnp.where(lane > 0, turned[i], turned[i - 1] if i else past) for i in range(count)]


def terms(low, sides, tile, x, y, wx, wy):
    above, below, both = sides
    around = {(i, j): low(x + i, y + j, tile) for i in (-1, 0, 1) for j in (-1, 0, 1)}
    total = None
    for i in (-1, 1):
        for j in (-1, 1):
            ex, ey = wx + (i - 1) // 2, wy + (j - 1) // 2
            others = around[i, 0] + around[0, j] + around[i, j]
            new = (
                both(ex, ey, tile) * around[i, j],
                below(ex, ey, tile) * others,
                above(ex, ey, tile) * others,
            )
            total = new if total is None else tuple(a + b for a, b in zip(total, new))
    rim = [both(wx + i, wy + j, tile) for i in (-1, 0) for j in (-1, 0)]
    centre = (4.0 * ((rim[0] + rim[1]) + (rim[2] + rim[3]))) * around[0, 0]
    return centre - total[0], total[1], total[2]


def operator(field, low, sides, count, x, y, wx, wy):
    plane, down, up = zip(*[terms(low, sides, t, x, y, wx, wy) for t in range(count)])
    from_above, from_below = shifted(down, 1), shifted(up, -1)
    return [SIGMA * field(t) + (plane[t] - from_above[t] - from_below[t]) for t in range(count)]


def split_terms(value, count):
    parts = []
    for n in range(count):
        part = value.astype(jnp.bfloat16)
        parts.append(part)
        if n + 1 < count:
            value = value - part.astype(jnp.float32)
    return jnp.concatenate(parts, axis=0)


def rows_of(refs, flags_ref, tile, x, y, first, count):
    before_x_ref, own_ref, after_x_ref, before_ref, before_last_ref, after_ref, after_last_ref = refs
    flag = None
    if 2 <= y < 6:
        ref, column, wide, tall, at = (before_x_ref, own_ref, after_x_ref)[x // 2], x % 2, 2, 4, y - 2
    else:
        low = y < 2
        flag, at, tall = (0, y, 2) if low else (1, y - 6, 2)
        if x < 4:
            ref, column, wide = before_ref if low else after_ref, x, 4
        else:
            ref, column, wide = before_last_ref if low else after_last_ref, x - 4, 2
    stride = wide * tall
    start = tile * (ref.shape[0] // 2) + first * stride + column * tall + at
    value = ref[pl.ds(start, count, stride=stride), :] if count > 1 else ref[start : start + 1, :]
    if flag is not None:
        value = jnp.where(flags_ref[flag : flag + 1, :] > 0.0, value, 0.0)
    return value


def front_kernel(moduli_ref, loads_ref, material_ref, own_ref, levels_ref):
    for t in range(2):
        own_ref[t, :COLS] = loads_ref[:, :, :, tile_of(t)]
        own_ref[t, COLS] = (material_ref[:, :, tile_of(t)] + 1).astype(jnp.float32)
    for level in range(moduli_ref.shape[0]):
        levels_ref[level : level + 1, :] = jnp.full((1, LANES), moduli_ref[level], jnp.float32)


def pack_rows(starts, out_refs, refs, flags_ref, ext_x, ext_y, ys):
    for tile, (start_ref, out_ref) in enumerate(zip(starts, out_refs)):
        offset = 2 * tile
        lane = lax.broadcasted_iota(jnp.int32, (COLS, LANES), 1)
        packed = jnp.zeros((COLS, LANES), jnp.float32) if start_ref is None else start_ref[:COLS, :]
        for y in range(ext_y):
            row = slice(COLS + y, COLS + y + 1)
            ids = jnp.zeros((1, LANES), jnp.float32) if start_ref is None else start_ref[row, :]
            for x in range(ext_x) if y in ys else ():
                node = x * ext_y + y
                value = rows_of(refs, flags_ref, tile, x, y, 0, COLS)
                packed = jnp.where(lane // 2 == node, turn(value, 2 * node + offset), packed)
                value = rows_of(refs, flags_ref, tile, x, y, COLS, 1)
                ids = jnp.where(lane[:1] // 2 == x, turn(value, 2 * x + offset), ids)
            out_ref[row, :] = ids
        out_ref[:COLS, :] = packed


def pack_kernel(flags_ref, a_ref, b_ref, c_ref, d_ref, lo0_ref, hi0_ref, lo_ref, hi_ref, ext_x, ext_y):
    refs = (None, None, None, a_ref, b_ref, c_ref, d_ref)
    pack_rows((lo0_ref, hi0_ref), (lo_ref, hi_ref), refs, flags_ref, ext_x, ext_y, OUTER)


def sums_of(parts_ref, count):
    rows = parts_ref.shape[0] // count
    sub = lax.broadcasted_iota(jnp.int32, (8, LANES), 0)
    out = jnp.zeros((8, LANES), jnp.float32)
    for row in range(rows):
        part = jnp.sum(parts_ref[pl.ds(row, count, stride=rows), :], axis=0, keepdims=True)
        out = jnp.where(sub == row, part, out)
    return out


def pair_kernel(both_ref, out_ref, rows):
    copies = out_ref.shape[0] // rows
    half = both_ref.shape[0] // 2
    total = both_ref[:half, :] + both_ref[half:, :]
    for row in range(rows):
        out_ref[pl.ds(row, copies, stride=rows), :] = jnp.broadcast_to(total[row : row + 1, :], (copies, LANES))


def total_kernel(flags_ref, parts_ref, out_ref, count, copies):
    rows = parts_ref.shape[0] // count
    out = jnp.where(flags_ref[2:3, :] > 0.0, sums_of(parts_ref, count), 0.0)
    for row in range(rows):
        out_ref[pl.ds(row, copies, stride=rows), :] = jnp.broadcast_to(out[row : row + 1, :], (copies, LANES))


def modulus_of(levels_ref, ids):
    modulus = jnp.zeros_like(ids)
    for level in range(levels_ref.shape[0]):
        modulus = jnp.where(ids == level + 1.0, levels_ref[level : level + 1, :], modulus)
    return modulus


def element_weights(e_ref, above_ref, below_ref, both_ref, count):
    ext_x, ext_y = e_ref.shape[:2]
    for ex in range(ext_x - 1):
        flat = []
        for t in range(count):
            both_x = e_ref[ex, :, tile_of(t)] + e_ref[ex + 1, :, tile_of(t)]
            flat.append(both_x + pltpu.roll(both_x, ext_y - 1, 0))
        ahead = shifted(flat, 1)
        weights = [(0.125 * UNIT) * (flat[t] + ahead[t]) for t in range(count)]
        behind = shifted(weights, -1)
        for t in range(count):
            above_ref[ex, :, tile_of(t)] = weights[t]
            below_ref[ex, :, tile_of(t)] = behind[t]
            both_ref[ex, :, tile_of(t)] = weights[t] + behind[t]


def sides_of(*refs):
    return tuple(lambda ex, ey, t, ref=ref: ref[ex, ey : ey + 1, tile_of(t)] for ref in refs)


def first_image(v_ref, low_ref, e_ref, sides, q_ref, qlow_ref, count, ys):
    ext_x, ext_y = low_ref.shape[0], low_ref.shape[1]
    for x in range(1, ext_x - 1):
        for y in ys:
            image = operator(
                lambda t: v_ref[x - 1, y - 1, :, tile_of(t)],
                lambda i, j, t: low_ref[i, j, :, tile_of(t)],
                sides, count, x, y, x, y,
            )
            for t in range(count):
                value = image[t]
                if count == 1 or x in (1, ext_x - 2) or y in (1, ext_y - 2):
                    value = jnp.where(e_ref[x, y : y + 1, tile_of(t)] > 0.0, value, 0.0)
                q_ref[x - 1, y - 1, :, tile_of(t)] = value
                qlow_ref[x - 1, y - 1, :, tile_of(t)] = lowered(value)


def own_nodes(v_ref, q_ref, qlow_ref, sides, count):
    own_x, own_y = v_ref.shape[0], v_ref.shape[1]
    for x in range(1, own_x - 1):
        for y in range(1, own_y - 1):
            image = operator(
                lambda t: q_ref[x, y, :, tile_of(t)],
                lambda i, j, t: qlow_ref[i, j, :, tile_of(t)],
                sides, count, x, y, x + 1, y + 1,
            )
            for t in range(count):
                yield t, v_ref[x, y, :, tile_of(t)], q_ref[x, y, :, tile_of(t)], image[t]


def left_terms(right):
    return jnp.concatenate([right[3 * COLS * n : 3 * COLS * n + 2 * COLS] for n in range(3)], axis=0)


def products(left, right):
    product = lax.dot_general(left, right, (((1,), (1,)), ((), ())), preferred_element_type=jnp.float32)
    rows = sum(product[2 * COLS * n : 2 * COLS * (n + 1)] for n in range(3))
    lane = lax.broadcasted_iota(jnp.int32, (2 * COLS, LANES), 1)
    first = rows[:, :LANES]
    rest = jnp.concatenate([rows[:, LANES:], jnp.zeros((2 * COLS, 2 * LANES - 9 * COLS), jnp.float32)], axis=1)
    third = jnp.where(lane < 2 * COLS, turn(first, -6 * COLS), turn(rest, 2 * COLS))
    return first + turn(first, -3 * COLS) + third


def edge_of(tiles):
    lane = lanes_of(tiles[0])
    return jnp.where(lane < EDGE, tiles[0], jnp.where(lane < 2 * EDGE, turn(tiles[1], 2 * EDGE), 0.0))


def middle_kernel(
    levels_ref, before_ref, own_ref, after_ref,
    v_ref, low_ref, q_ref, qlow_ref, ve_ref, ie_ref, e_ref, lo_ref, hi_ref,
    above_ref, below_ref, both_ref,
):
    ext_x, ext_y = low_ref.shape[0], e_ref.shape[1]
    refs = (before_ref, own_ref, after_ref, None, None, None, None)
    e_ref[...] = jnp.zeros_like(e_ref)
    ie_ref[...] = jnp.zeros_like(ie_ref)
    for x in range(ext_x):
        for y in MIDDLE:
            tiles = [rows_of(refs, None, t, x, y, COLS, 1) for t in range(2)]
            ie_ref[x, y - 2 : y - 1, :] = edge_of(tiles)
            for t in range(2):
                e_ref[x, y - 2 : y - 1, tile_of(t)] = tiles[t]
            tiles = [rows_of(refs, None, t, x, y, 0, COLS) for t in range(2)]
            ve_ref[x, y - 2] = edge_of(tiles)
            for t in range(2):
                low_ref[x, y - 2, :, tile_of(t)] = lowered(tiles[t])
                if 0 < x < ext_x - 1:
                    v_ref[x - 1, y - 2, :, tile_of(t)] = tiles[t]
        for t in range(2):
            e_ref[x, :, tile_of(t)] = modulus_of(levels_ref, e_ref[x, :, tile_of(t)])
    pack_rows((None, None), (lo_ref, hi_ref), refs, None, ext_x, ext_y, MIDDLE)
    element_weights(e_ref, above_ref, below_ref, both_ref, 2)
    sides = sides_of(above_ref, below_ref, both_ref)
    for x in range(1, ext_x - 1):
        for y in (1, 2):
            image = operator(
                lambda t: v_ref[x - 1, y, :, tile_of(t)],
                lambda i, j, t: low_ref[i, j, :, tile_of(t)],
                sides, 2, x, y, x, y,
            )
            for t in range(2):
                value = image[t]
                if x in (1, ext_x - 2):
                    value = jnp.where(e_ref[x, y : y + 1, tile_of(t)] > 0.0, value, 0.0)
                q_ref[x - 1, y - 1, :, tile_of(t)] = value
                qlow_ref[x - 1, y - 1, :, tile_of(t)] = lowered(value)


def main_kernel(
    levels_ref, flags_ref, a_ref, b_ref, c_ref, d_ref,
    vm_ref, lowm_ref, qm_ref, qlowm_ref, vem_ref, iem_ref, em_ref,
    v_ref, q_ref, above_ref, below_ref, both_ref, total_ref, ve_ref, ie_ref,
    low_ref, qlow_ref, e_ref, left_ref, right_ref,
):
    ext_x, ext_y = low_ref.shape[0], low_ref.shape[1]
    refs = (None, None, None, a_ref, b_ref, c_ref, d_ref)
    for x in range(ext_x):
        ie_ref[x, 2:6, :] = iem_ref[x, 0:4, :]
        for y in OUTER:
            tiles = [rows_of(refs, flags_ref, t, x, y, COLS, 1) for t in range(2)]
            ie_ref[x, y : y + 1, :] = edge_of(tiles)
            for t in range(2):
                e_ref[x, y : y + 1, tile_of(t)] = tiles[t]
        for t in range(2):
            e_ref[x, 2:6, tile_of(t)] = jnp.zeros((4, LANES), jnp.float32)
            e_ref[x, :, tile_of(t)] = modulus_of(levels_ref, e_ref[x, :, tile_of(t)])
            e_ref[x, 2:6, tile_of(t)] = em_ref[x, 0:4, tile_of(t)]
    element_weights(e_ref, above_ref, below_ref, both_ref, 2)
    for x in range(ext_x):
        for y in range(ext_y):
            inner = 0 < x < ext_x - 1 and 0 < y < ext_y - 1
            if y in MIDDLE:
                ve_ref[x, y] = vem_ref[x, y - 2]
                low_ref[x, y] = lowm_ref[x, y - 2]
                if inner:
                    v_ref[x - 1, y - 1] = vm_ref[x - 1, y - 2]
                if inner and y in (3, 4):
                    q_ref[x - 1, y - 1] = qm_ref[x - 1, y - 3]
                    qlow_ref[x - 1, y - 1] = qlowm_ref[x - 1, y - 3]
                continue
            tiles = [rows_of(refs, flags_ref, t, x, y, 0, COLS) for t in range(2)]
            ve_ref[x, y] = edge_of(tiles)
            for t in range(2):
                low_ref[x, y, :, tile_of(t)] = lowered(tiles[t])
                if inner:
                    v_ref[x - 1, y - 1, :, tile_of(t)] = tiles[t]
    sides = sides_of(above_ref, below_ref, both_ref)
    first_image(v_ref, low_ref, e_ref, sides, q_ref, qlow_ref, 2, (1, 2, 5, 6))
    for n, (t, b, q, w) in enumerate(own_nodes(v_ref, q_ref, qlow_ref, sides, 2)):
        right = split_terms(jnp.concatenate([b, q, w], axis=0), 3)
        left = left_terms(right)
        here = lanes_of(left) >= 2 if t == 0 else lanes_of(left) < LANES - 2
        left_ref[:, tile_of(n)] = jnp.where(here, left, jnp.zeros_like(left))
        right_ref[:, tile_of(n)] = right
    total_ref[...] = products(left_ref[...], right_ref[...])


def edge_kernel(
    levels_ref, total_ref, ve_ref, ie_ref, before_ref, after_ref,
    v_ref, q_ref, above_ref, below_ref, both_ref, g_ref,
    low_ref, qlow_ref, e_ref,
):
    ext_x, ext_y = low_ref.shape[0], low_ref.shape[1]

    def with_ends(own, before, after, index):
        lane = lanes_of(own)
        follows, comes = turn(after, LANES // 2 - 2 * index), turn(before, LANES - 2 - 2 * index)
        value = jnp.where(lane >= LANES - 2, comes, own)
        return jnp.where((lane >= LANES // 2) & (lane < LANES // 2 + 2), follows, value)

    for x in range(ext_x):
        ids = with_ends(ie_ref[x], before_ref[COLS : COLS + ext_y, :], after_ref[COLS : COLS + ext_y, :], x)
        e_ref[x] = modulus_of(levels_ref, ids)
    element_weights(e_ref, above_ref, below_ref, both_ref, 1)
    before, after = before_ref[:COLS, :], after_ref[:COLS, :]
    for x in range(ext_x):
        for y in range(ext_y):
            value = with_ends(ve_ref[x, y], before, after, x * ext_y + y)
            low_ref[x, y] = lowered(value)
            if 0 < x < ext_x - 1 and 0 < y < ext_y - 1:
                v_ref[x - 1, y - 1] = value
    sides = sides_of(above_ref, below_ref, both_ref)
    first_image(v_ref, low_ref, e_ref, sides, q_ref, qlow_ref, 1, range(1, ext_y - 1))
    right = jnp.zeros((3 * COLS, LANES), jnp.float32)
    for n, (_, b, q, w) in enumerate(own_nodes(v_ref, q_ref, qlow_ref, sides, 1)):
        three = jnp.concatenate([b, q, w], axis=0)
        at = lanes_of(three) - 2 * n
        here = ((at >= 0) & (at < 2)) | ((at >= 2 * EDGE - 2) & (at < 2 * EDGE))
        right = jnp.where(here, turn(three, 2 * n), right)
    right = split_terms(right, 3)
    total = products(left_terms(right), right)
    g_ref[...] = pack_moments(total_ref[...] + total)


def pack_moments(total):
    first, second = total[:COLS], total[COLS:]
    row = lax.broadcasted_iota(jnp.int32, (COLS, LANES), 0)
    lane = lax.broadcasted_iota(jnp.int32, (COLS, LANES), 1)
    col = lane % COLS
    upper = jnp.where(lane < COLS, first, second)
    lower = jnp.where(
        lane < COLS,
        0.5 * (pltpu.roll(first, LANES - COLS, 1) + second),
        pltpu.roll(second, LANES - COLS, 1),
    )
    valid = lane < 2 * COLS
    square = jnp.where(valid, jnp.where(row <= col, upper, lower), 0.0)
    diagonal = jnp.sum(jnp.where(valid & (row == col), lower, 0.0), axis=0, keepdims=True)
    out = []
    for half in range(2):
        out.append(square[8 * half : 8 * half + 8])
    spread_rows = jnp.zeros((8, LANES), jnp.float32)
    sub8 = lax.broadcasted_iota(jnp.int32, (8, LANES), 0)
    lane8 = lax.broadcasted_iota(jnp.int32, (8, LANES), 1)
    for quarter in range(4):
        piece = out[quarter // 2]
        if quarter % 2:
            piece = pltpu.roll(piece, 4, 0)
        if quarter:
            piece = pltpu.roll(piece, 2 * COLS * quarter, 1)
        here = (sub8 < 4) & (lane8 // (2 * COLS) == quarter)
        spread_rows = jnp.where(here, piece, spread_rows)
    return jnp.where(sub8 == 4, diagonal, spread_rows)


def unpack_moments(packed):
    sub8 = lax.broadcasted_iota(jnp.int32, (8, LANES), 0)
    halves = []
    for half in range(2):
        a, b = 2 * half, 2 * half + 1
        top = pltpu.roll(packed, LANES - 2 * COLS * a, 1) if a else packed
        bottom = pltpu.roll(pltpu.roll(packed, LANES - 2 * COLS * b, 1), 4, 0)
        halves.append(jnp.where(sub8 < 4, top, bottom))
    square = jnp.concatenate(halves, axis=0)
    row = lax.broadcasted_iota(jnp.int32, (COLS, COLS), 0)
    col = lax.broadcasted_iota(jnp.int32, (COLS, COLS), 1)
    moments = []
    for pair in range(2):
        turned = pltpu.roll(square, LANES - COLS, 1) if pair else square
        mixed = turned[:, :COLS]
        diagonal = (pltpu.roll(packed, LANES - COLS, 1) if pair else packed)[4:5, :COLS]
        flipped = mixed.T
        moments.append(jnp.where(row <= col, mixed, flipped))
        lower = jnp.where(row == col, diagonal, jnp.where(row > col, mixed, flipped))
        moments.append(lower)
    return moments


def dot(left, right, dims=((1,), (0,))):
    return lax.dot_general(left, right, (dims, ((), ())), precision=HIGH, preferred_element_type=jnp.float32)


def replicated(matrix):
    return [jnp.broadcast_to(matrix[:, i : i + 1], (COLS, LANES)) for i in range(COLS)]


def sweeps(rows):
    rows = list(rows)
    sub = lax.broadcasted_iota(jnp.int32, (COLS, LANES), 0)
    for k in range(COLS):
        scale = 1.0 / rows[k][k : k + 1, :]
        pivot_row = rows[k] * scale
        for i in range(COLS):
            if i != k:
                factor = rows[i][k : k + 1, :]
                moved = rows[i] - factor * pivot_row
                rows[i] = jnp.where(sub == k, factor * scale, moved)
        rows[k] = jnp.where(sub == k, -scale, pivot_row)
        yield rows


def times(rows, right):
    parts = [rows[i] * right[i : i + 1, :] for i in range(COLS)]
    while len(parts) > 1:
        parts = [a + b for a, b in zip(parts[::2], parts[1::2])]
    return parts[0]


def mixer(coeffs, count):
    flipped = split_terms(coeffs.T, count)
    return jnp.concatenate([flipped] * count, axis=1)


def mixed(left, block, count):
    out = jnp.dot(left, split_terms(block, count), preferred_element_type=jnp.float32)
    size = out.shape[0] // count
    return sum(out[size * n : size * (n + 1)] for n in range(count))


def finish_kernel(
    g_ref, v_ref, q_ref, above_ref, below_ref, both_ref,
    ve_ref, qe_ref, abovee_ref, belowe_ref, bothe_ref,
    sol_ref, res_ref, d_ref, dlow_ref, w0_ref, w1_ref, w2_ref,
):
    own_x, own_y = v_ref.shape[0], v_ref.shape[1]
    m0, m1, m2, m3 = unpack_moments(sums_of(g_ref, g_ref.shape[0] // 5))
    first = ((0,), (0,))
    padding = jnp.zeros((COLS, LANES - COLS), jnp.float32)
    *_, minus_inv = sweeps(replicated(m1))
    minus_alpha = times(minus_inv, jnp.concatenate([m0, padding], axis=1))
    minus_m2a = times(replicated(m2), minus_alpha)
    mix = times(minus_inv, minus_m2a)[:, :COLS]
    minus_m3a = times(replicated(m3), minus_alpha)[:, :COLS]
    minus_alpha, minus_m2a = minus_alpha[:, :COLS], minus_m2a[:, :COLS]
    alpha = -minus_alpha
    left = mixer(jnp.concatenate([mix, minus_alpha], axis=0), 3)
    updated = dot(minus_alpha, minus_m2a, first) - m0
    curved = dot(minus_alpha, minus_m3a, first) + dot(minus_m2a, mix, first)
    steps = sweeps(replicated(0.5 * (curved + curved.T)))
    minus_inv = None
    for x in range(own_x):
        for y in range(own_y):
            q0, q1, qe = q_ref[x, y, :, :LANES], q_ref[x, y, :, LANES:], qe_ref[x, y]
            lane = lanes_of(qe)
            q0 = jnp.where(lane == 0, qe, q0)
            q1 = jnp.where(lane == LANES - 1, turn(qe, LANES // 2), q1)
            block = jnp.concatenate(
                [
                    jnp.concatenate([v_ref[x, y], ve_ref[x, y]], axis=1),
                    jnp.concatenate([q0, q1, qe], axis=1),
                ],
                axis=0,
            )
            value = mixed(left, block, 3)
            d_ref[x, y] = value
            dlow_ref[x, y] = lowered(value)
            minus_inv = next(steps, minus_inv)
    gamma = -times(minus_inv, jnp.concatenate([updated, padding], axis=1))[:, :COLS]
    edge, main = (abovee_ref, belowe_ref, bothe_ref), (above_ref, below_ref, both_ref)
    whole = (w0_ref, w1_ref, w2_ref)
    for end_ref, main_ref, whole_ref in zip(edge, main, whole):
        for ex in range(1, own_x):
            end = end_ref[ex]
            lane = lanes_of(end)
            whole_ref[ex, :, :LANES] = jnp.where(lane == 0, end, main_ref[ex, :, :LANES])
            end = turn(end, LANES // 2)
            whole_ref[ex, :, LANES:] = jnp.where(lane == LANES - 1, end, main_ref[ex, :, LANES:])
    main, edge = sides_of(*whole), sides_of(*edge)
    zero = jnp.zeros((COLS, COLS), jnp.float32)
    last = mixer(
        jnp.concatenate(
            [
                jnp.concatenate([alpha, gamma, zero, zero], axis=0),
                jnp.concatenate([zero, zero, -alpha, -gamma], axis=0),
            ],
            axis=1,
        ),
        3,
    )
    for x in range(1, own_x - 1):
        for y in range(1, own_y - 1):
            low = lambda i, j, t: dlow_ref[i, j, :, tile_of(t)]
            at = (x, y, x + 1, y + 1)
            plane, down, up = zip(*[terms(low, main, t, *at) for t in range(2)])
            ends = terms(lambda i, j, t: dlow_ref[i, j, :, tile_of(2)], edge, 0, *at)
            from_above = shifted(down, 1, turn(ends[1], LANES // 2))
            from_below = shifted(up, -1, ends[2])
            image = [
                SIGMA * d_ref[x, y, :, tile_of(t)] + (plane[t] - from_above[t] - from_below[t])
                for t in range(2)
            ]
            q0, q1, qe = q_ref[x, y, :, :LANES], q_ref[x, y, :, LANES:], qe_ref[x, y]
            lane = lanes_of(qe)
            q0 = jnp.where(lane == 0, qe, q0)
            q1 = jnp.where(lane == LANES - 1, turn(qe, LANES // 2), q1)
            b = v_ref[x, y]
            block = jnp.concatenate(
                [
                    b,
                    d_ref[x, y, :, : 2 * LANES],
                    jnp.concatenate([q0, q1], axis=1),
                    jnp.concatenate(image, axis=1),
                ],
                axis=0,
            )
            out = mixed(last, block, 3)
            sol_ref[:, x - 1, y - 1, :] = out[:COLS]
            res_ref[:, x - 1, y - 1, :] = b + out[COLS:]


def both_ways(axis, to_next, to_last, around=False):
    count = lax.axis_size(axis)
    steps = range(count) if around else range(count - 1)
    before = lax.ppermute(to_next, axis, [(i, (i + 1) % count) for i in steps])
    after = lax.ppermute(to_last, axis, [((i + 1) % count, i) for i in steps])
    return before, after


def line_groups(root):
    wide_x, wide_y, _, long = (lax.axis_size(axis) for axis in (*PLANE, "gz"))
    at = np.arange(wide_x * wide_y * 2 * long).reshape(wide_x * wide_y, 2, long)
    order = [(root + i) % long for i in range(long)]
    lines = [[int(v) for v in at[place, 1, order]] for place in range(wide_x * wide_y)]
    others = at[:, 0, :].T.reshape(-1, long)
    return lines + [[int(v) for v in group] for group in others]


def near(value):
    return pltpu.with_memory_space_constraint(value, pltpu.VMEM)


def on_device(loads, moduli, material):
    f32, bf16, wide = jnp.float32, jnp.bfloat16, 2 * LANES
    own_x, own_y = material.shape[:2]
    ext_x, ext_y = own_x + 4, own_y + 4
    own, levels = pl.pallas_call(
        front_kernel,
        out_shape=(
            pltpu.VMEM((2, COLS + 1, own_x, own_y, LANES), f32),
            pltpu.VMEM((moduli.shape[0], LANES), f32),
        ),
        in_specs=[
            pl.BlockSpec(memory_space=pltpu.SMEM),
            pl.BlockSpec(memory_space=pltpu.VMEM),
            pl.BlockSpec(memory_space=pltpu.VMEM),
        ],
        name="front",
    )(moduli, loads, material)
    place = lax.axis_index(GY)
    row = lax.broadcasted_iota(jnp.int32, (8, LANES), 0)
    flags = jnp.where(row == 0, place > 0, place < lax.axis_size(GY) - 1)
    flags = jnp.where(row == 2, lax.axis_index("gy_1") == 1, flags).astype(f32)
    before, after = both_ways("gx", own, own)
    part = jnp.concatenate([before, own], axis=2)
    parts = part[:, :, :, 2:], part[:, :, :, :2]
    sides = both_ways(GY, *parts, around=True)
    lasts = both_ways(GY, after[:, :, :, 2:], after[:, :, :, :2], around=True)
    line = [near(v.reshape(-1, LANES)) for v in (before, own, after)]
    flat = [near(v.reshape(-1, LANES)) for v in (sides[0], lasts[0], sides[1], lasts[1])]
    levels, flags = near(levels), near(flags)
    ends = (pltpu.VMEM((COLS + 8, LANES), f32),) * 2

    def block(xs, ys, size):
        return pltpu.VMEM((xs, ys, COLS, size), f32)

    *mid, lo, hi = pl.pallas_call(
        middle_kernel,
        out_shape=(
            block(ext_x - 2, own_y, wide),
            block(ext_x, own_y, wide),
            block(ext_x - 2, own_y - 2, wide),
            block(ext_x - 2, own_y - 2, wide),
            block(ext_x, own_y, LANES),
            pltpu.VMEM((ext_x, ext_y, LANES), f32),
            pltpu.VMEM((ext_x, ext_y, wide), f32),
            *ends,
        ),
        scratch_shapes=[pltpu.VMEM((ext_x - 1, ext_y, wide), f32)] * 3,
        compiler_params=GRANT,
        name="middle",
    )(levels, *line)
    first, last = pl.pallas_call(
        functools.partial(pack_kernel, ext_x=ext_x, ext_y=ext_y), out_shape=ends, compiler_params=GRANT, name="pack"
    )(flags, *flat, near(lo), near(hi))
    before, after = both_ways("gz", last, first)
    nodes = own_x * own_y

    def weights(size):
        return (pltpu.VMEM((ext_x - 1, ext_y, size), f32),) * 3

    def fields(size):
        return (pltpu.VMEM((ext_x - 2, ext_y - 2, COLS, size), f32),) * 2

    def scratch(size):
        return [
            pltpu.VMEM((ext_x, ext_y, COLS, size), f32),
            pltpu.VMEM((ext_x - 2, ext_y - 2, COLS, size), f32),
            pltpu.VMEM((ext_x, ext_y, size), f32),
        ]

    *main, total, edge, ids = pl.pallas_call(
        main_kernel,
        out_shape=(
            *fields(wide),
            *weights(wide),
            pltpu.VMEM((2 * COLS, LANES), f32),
            pltpu.VMEM((ext_x, ext_y, COLS, LANES), f32),
            pltpu.VMEM((ext_x, ext_y, LANES), f32),
        ),
        scratch_shapes=scratch(wide)
        + [pltpu.VMEM((6 * COLS, nodes * wide), bf16), pltpu.VMEM((9 * COLS, nodes * wide), bf16)],
        compiler_params=GRANT,
        name="main",
    )(levels, flags, *flat, *[near(v) for v in mid])
    *edges, moments = pl.pallas_call(
        edge_kernel,
        out_shape=(*fields(LANES), *weights(LANES), pltpu.VMEM((8, LANES), f32)),
        scratch_shapes=scratch(LANES),
        compiler_params=GRANT,
        name="edge",
    )(*[near(value) for value in (levels, total, edge, ids, before, after)])
    rows = 5
    length, chips = lax.axis_size("gz"), lax.axis_size("gy_0")
    both = near(lax.all_gather(moments, "gy_1").reshape(-1, LANES))
    copies = pl.pallas_call(
        functools.partial(pair_kernel, rows=rows),
        out_shape=pltpu.VMEM((length * rows, LANES), f32),
        compiler_params=GRANT,
        name="pair",
    )(both).reshape(length, rows, 1, LANES)
    moments = lax.all_to_all(copies, (*PLANE, "gz"), 0, 0, axis_index_groups=line_groups(19 * length // 32))
    places = lax.axis_size(PLANE)
    copies = pl.pallas_call(
        functools.partial(total_kernel, count=length, copies=places),
        out_shape=pltpu.VMEM((places * rows, LANES), f32),
        compiler_params=GRANT,
        name="total",
    )(flags, near(moments.reshape(length * rows, LANES)))
    middle = (lax.axis_size("gx") // 2 * chips + chips // 2) * 2 + 1
    group = [(middle + i) % places for i in range(places)]
    copies = copies.reshape(places, rows, 1, LANES)
    moments = lax.all_to_all(copies, PLANE, 0, 0, axis_index_groups=[group]).reshape(places * rows, LANES)
    out = jax.ShapeDtypeStruct(loads.shape, f32)
    return pl.pallas_call(
        finish_kernel,
        out_shape=(out, out),
        scratch_shapes=[pltpu.VMEM((ext_x - 2, ext_y - 2, COLS, 3 * LANES), f32)] * 2
        + [pltpu.VMEM((ext_x - 1, ext_y, wide), f32)] * 3,
        compiler_params=GRANT,
        name="finish",
    )(*[near(value) for value in (moments, *main, *edges)])


def solution(mesh):
    chips, long = mesh.shape["gy"] // 2, mesh.shape["gz"]
    split = Mesh(mesh.devices.reshape(mesh.shape["gx"], chips, 2, long), ("gx", "gy_0", "gy_1", "gz"))
    spec = P(None, "gx", GY, "gz")

    return jax.shard_map(
        on_device,
        mesh=split,
        in_specs=(spec, P(), P("gx", GY, "gz")),
        out_specs=(spec, spec),
        check_vma=False,
    )
```
